512 devices in a mesh: blk: 32 (over z, core), sub: 16 (over x, y).
Axes of the slice: x: 4, y: 4, z: 16, core: 2. Of those that a mesh axis runs over, the one named last changes fastest.
Arguments:
- rhs: float32 [4096, 16, 256], P(('blk', 'sub')), may hold values from -6 to 6
- leaf_neighbors: int32 [4096, 6], P(('blk', 'sub')), may hold values from -1 to 4095, as said below
- parent_neighbors: int32 [512, 6], replicated, may hold values from -1 to 511, as said below
- children: int32 [512, 8], replicated, may hold values from 0 to 4095, as said below
- owners: int32 [512], replicated, may hold values from 0 to 15, as said below
- parent_places: int32 [512], replicated, may hold values from 0 to 511, as said below
Outputs:
- leaf_solution: float32 [4096, 16, 256], P(('blk', 'sub'))
- parent_solution: float32 [1536, 16, 256], P(('blk', 'sub'))
The draws below stay inside these ranges and needn't reach their ends.
Inputs may be any that keep to these rules, and one draw needn't show every extreme that they name: `leaf_neighbors`: entry f of block b is the leaf block across face f of b, or -1 on the domain's boundary; the relation is mutual. Leaves d * 8 onward are the blocks of device d in order of blk then sub; a range is the 128 leaves of one index of blk. The -x and +x neighbours of a leaf belong to the devices one index lower and one index higher along sub with the same blk index; its -y and +y neighbours belong to its own device; its -z and +z neighbours belong to its own device or to the device one index lower or higher along blk with the same sub index. `parent_neighbors`: entry f of parent p is the parent block across face f of p, or -1; mutual. Range r holds the parents r * 16 onward; x and y neighbours lie in the same range, -z and +z neighbours in the range just below or above. Entry o = 4 oz + 2 oy + ox names the child in octant (oz, oy, ox); every leaf is the child of one parent, and a parent's children lie in the leaf range with the same index as the parent's range; its four children with ox = 0 belong to one device of even index 2k along sub and its four with ox = 1 to the device 2k + 1 with the same blk index. `owners`: within each range no index owns more than 3 parents, and some index owns exactly 3. `parent_places`: A permutation; parents of range r have places r * 16 onward.
All inputs are finite; a program needn't handle non-finite values.
Results may differ from the reference program's by a relative error of at most 0.0003.
Values sent between devices are 32-bit elements; how exact they have to be, the bound alone decides.
A program may use at most 64 MiB of HBM per device.

```python
import jax
import jax.numpy as jnp

BLK_DEV = 8
ROOT_SWEEPS = 8
LEAVES = 4096
PARENTS = 512
PMOST = 3
PSLOTS = 1536
N_BLK = 32
N_SUB = 16


def neighbours(grid):
    padded = jnp.pad(grid, 1, constant_values=-1)
    lists = jnp.stack([padded[1:-1, 1:-1, :-2], padded[1:-1, 1:-1, 2:], padded[1:-1, :-2, 1:-1], padded[1:-1, 2:, 1:-1], padded[:-2, 1:-1, 1:-1], padded[2:, 1:-1, 1:-1]], axis=-1).reshape(-1, 6)
    return jnp.zeros((grid.size, 6), jnp.int32).at[grid.reshape(-1)].set(lists.astype(jnp.int32))


def one_range(range_key):
    parent_len = BLK_DEV * N_SUB // 8
    first_key, second_key = jax.random.split(range_key)
    shuffled = jax.random.permutation(first_key, parent_len)
    heavy = jax.random.randint(second_key, (), 0, N_SUB)
    slot_number = jnp.arange(parent_len, dtype=jnp.int32)
    assigned = jnp.where(slot_number < PMOST, heavy, (heavy + 1 + (slot_number - PMOST) % (N_SUB - 1)) % N_SUB)
    return jnp.zeros((parent_len,), jnp.int32).at[shuffled].set(assigned.astype(jnp.int32))


def layout(key):
    width_x = N_SUB
    width_y = BLK_DEV // 2
    depth_z = 2 * N_BLK
    range_len = BLK_DEV * N_SUB
    parent_len = range_len // 8
    device_keys = jax.random.split(jax.random.fold_in(key, 11), N_BLK * N_SUB)
    device_order = jax.vmap(lambda device_key: jax.random.permutation(device_key, BLK_DEV))(device_keys).astype(jnp.int32)
    level_z = jnp.arange(depth_z, dtype=jnp.int32)[:, None, None]
    level_y = jnp.arange(width_y, dtype=jnp.int32)[None, :, None]
    level_x = jnp.arange(width_x, dtype=jnp.int32)[None, None, :]
    device_id = level_z // 2 * N_SUB + level_x + 0 * level_y
    slot_id = level_z % 2 * width_y + level_y + 0 * level_x
    leaf_ids = (device_id * BLK_DEV + device_order[device_id, slot_id]).astype(jnp.int32)
    parent_keys = jax.random.split(jax.random.fold_in(key, 12), N_BLK)
    parent_order = jax.vmap(lambda range_key: jax.random.permutation(range_key, parent_len))(parent_keys).astype(jnp.int32)
    parent_ids = (jnp.arange(N_BLK, dtype=jnp.int32)[:, None] * parent_len + parent_order).reshape(N_BLK, width_y // 2, width_x // 2)
    leaf_lists = neighbours(leaf_ids)
    parent_lists = neighbours(parent_ids)
    kids = leaf_ids.reshape(N_BLK, 2, width_y // 2, 2, width_x // 2, 2).transpose(0, 2, 4, 1, 3, 5).reshape(-1, 8)
    child_lists = jnp.zeros((PARENTS, 8), jnp.int32).at[parent_ids.reshape(-1)].set(kids)
    place_list = jnp.zeros((PARENTS,), jnp.int32).at[parent_ids.reshape(-1)].set(jnp.arange(PARENTS, dtype=jnp.int32))
    owner_keys = jax.random.split(jax.random.fold_in(key, 13), N_BLK)
    owner_list = jax.vmap(one_range)(owner_keys).reshape(-1)
    return (leaf_lists, parent_lists, child_lists, owner_list, place_list)


def draw_leaf_neighbors(key, part):
    return layout(key)[0]


def draw_parent_neighbors(key, part):
    return layout(key)[1]


def draw_children(key, part):
    return layout(key)[2]


def draw_owners(key, part):
    return layout(key)[3]


def draw_parent_places(key, part):
    return layout(key)[4]


def draw_rhs(key, part):
    shape = (LEAVES, 16, 256)
    return jnp.clip(jax.random.normal(key, shape, jnp.float32), -6.0, 6.0)


def setup_inputs(seed: int = 0) -> dict:
    splits = jax.random.split(jax.random.key(seed), 7)
    rhs = draw_rhs(jax.random.fold_in(splits[6], 71), 0)
    leaf_neighbors = draw_leaf_neighbors(jax.random.fold_in(splits[6], 71), 0)
    parent_neighbors = draw_parent_neighbors(jax.random.fold_in(splits[6], 71), 0)
    children = draw_children(jax.random.fold_in(splits[6], 71), 0)
    owners = draw_owners(jax.random.fold_in(splits[6], 71), 0)
    parent_places = draw_parent_places(jax.random.fold_in(splits[6], 71), 0)
    return dict(rhs=rhs, leaf_neighbors=leaf_neighbors, parent_neighbors=parent_neighbors, children=children, owners=owners, parent_places=parent_places)


relax_weight = 0.8


def block_faces(values):
    blocks = values.shape[0]
    cube_cells = values.reshape(blocks, 16, 16, 16)
    stacked = jnp.stack([cube_cells[:, :, :, 0], cube_cells[:, :, :, 15], cube_cells[:, :, 0, :], cube_cells[:, :, 15, :], cube_cells[:, 0], cube_cells[:, 15]], axis=1)
    return stacked.reshape(blocks, 6, 256)


def apply_operator(values, ghosts):
    blocks = values.shape[0]
    cube_cells = values.reshape(blocks, 16, 16, 16)
    shell_faces = ghosts.reshape(blocks, 6, 16, 16)
    beside_all = jnp.concatenate([shell_faces[:, 0][:, :, :, None], cube_cells[:, :, :, :-1]], axis=3)
    beside_all = beside_all + jnp.concatenate([cube_cells[:, :, :, 1:], shell_faces[:, 1][:, :, :, None]], axis=3)
    beside_all = beside_all + jnp.concatenate([shell_faces[:, 2][:, :, None, :], cube_cells[:, :, :-1, :]], axis=2)
    beside_all = beside_all + jnp.concatenate([cube_cells[:, :, 1:, :], shell_faces[:, 3][:, :, None, :]], axis=2)
    beside_all = beside_all + jnp.concatenate([shell_faces[:, 4][:, None], cube_cells[:, :-1]], axis=1)
    beside_all = beside_all + jnp.concatenate([cube_cells[:, 1:], shell_faces[:, 5][:, None]], axis=1)
    return (6.0 * cube_cells - beside_all).reshape(blocks, 16, 256)


def jacobi_sweep(values, forcing, ghosts):
    return values + (relax_weight / 6.0) * (forcing - apply_operator(values, ghosts))


def global_ghosts(values, neighbours):
    face_rows = block_faces(values)
    opposite = jnp.array([1, 0, 3, 2, 5, 4], dtype=jnp.int32)
    picked = face_rows[jnp.maximum(neighbours, 0), opposite[None, :]]
    return jnp.where((neighbours >= 0)[:, :, None], picked, 0.0)


def restrict_octants(values):
    blocks = values.shape[0]
    return (values.reshape(blocks, 8, 2, 8, 2, 8, 2).mean(axis=(2, 4, 6)) * 4.0).reshape(blocks, 512)


def assemble(octant_rows):
    blocks = octant_rows.shape[0]
    return octant_rows.reshape(blocks, 2, 2, 2, 8, 8, 8).transpose(0, 1, 4, 2, 5, 3, 6).reshape(blocks, 16, 256)


def coarsen(values):
    blocks = values.shape[0]
    return (values.reshape(blocks, 4, 4, 4, 4, 4, 4).mean(axis=(2, 4, 6)) * 16.0).reshape(blocks, 64)


def widen_root(coarse):
    blocks = coarse.shape[0]
    return jnp.broadcast_to(coarse.reshape(blocks, 4, 1, 4, 1, 4, 1), (blocks, 4, 4, 4, 4, 4, 4)).reshape(blocks, 16, 256)


def octant_split(values):
    blocks = values.shape[0]
    return values.reshape(blocks, 2, 8, 2, 8, 2, 8).transpose(0, 1, 3, 5, 2, 4, 6).reshape(blocks, 8, 512)


def widen_leaf(octant):
    blocks = octant.shape[0]
    return jnp.broadcast_to(octant.reshape(blocks, 8, 1, 8, 1, 8, 1), (blocks, 8, 2, 8, 2, 8, 2)).reshape(blocks, 16, 256)


def slot_ranks(range_owners):
    width = range_owners.shape[1]
    same_owner = range_owners[:, :, None] == range_owners[:, None, :]
    earlier = jnp.arange(width, dtype=jnp.int32)[:, None] > jnp.arange(width, dtype=jnp.int32)[None, :]
    return jnp.sum(same_owner & earlier[None], axis=2).astype(jnp.int32)


def root_relax(root_values, root_source):
    padded = jnp.pad(root_values, 1)
    beside_all = padded[2:, 1:-1, 1:-1] + padded[:-2, 1:-1, 1:-1]
    beside_all = beside_all + padded[1:-1, 2:, 1:-1] + padded[1:-1, :-2, 1:-1]
    beside_all = beside_all + padded[1:-1, 1:-1, 2:] + padded[1:-1, 1:-1, :-2]
    return root_values + (relax_weight / 6.0) * (root_source - (6.0 * root_values - beside_all))


def reference(rhs, leaf_neighbors, parent_neighbors, children, owners, parent_places):
    factor = relax_weight / 6.0
    sweep_one = factor * rhs
    second = jacobi_sweep(sweep_one, rhs, global_ghosts(sweep_one, leaf_neighbors))
    residual = rhs - apply_operator(second, global_ghosts(second, leaf_neighbors))
    source = assemble(restrict_octants(residual)[children])
    parent_one = factor * source
    parent_two = jacobi_sweep(parent_one, source, global_ghosts(parent_one, parent_neighbors))
    parent_rest = source - apply_operator(parent_two, global_ghosts(parent_two, parent_neighbors))
    ordered = jnp.zeros((PARENTS, 64), jnp.float32).at[parent_places].set(coarsen(parent_rest))
    side_y = BLK_DEV // 4
    side_x = N_SUB // 2
    root_source = ordered.reshape(N_BLK, side_y, side_x, 4, 4, 4).transpose(0, 3, 1, 4, 2, 5).reshape(4 * N_BLK, 4 * side_y, 4 * side_x)
    root_source = root_source - jnp.mean(root_source)
    root_values = jnp.zeros_like(root_source)
    for repeat in range(ROOT_SWEEPS):
        root_values = root_relax(root_values, root_source)
    root_back = root_values.reshape(N_BLK, 4, side_y, 4, side_x, 4).transpose(0, 2, 4, 1, 3, 5).reshape(PARENTS, 64)[parent_places]
    parent_three = parent_two + widen_root(root_back)
    parent_four = jacobi_sweep(parent_three, source, global_ghosts(parent_three, parent_neighbors))
    lifted = jnp.zeros((LEAVES, 512), jnp.float32).at[children.reshape(-1)].set(octant_split(parent_four).reshape(PARENTS * 8, 512))
    leaf_three = second + widen_leaf(lifted)
    leaf_solution = jacobi_sweep(leaf_three, rhs, global_ghosts(leaf_three, leaf_neighbors))
    parent_len = PARENTS // N_BLK
    range_owners = owners.reshape(N_BLK, parent_len)
    slot_row = ((jnp.arange(N_BLK, dtype=jnp.int32)[:, None] * N_SUB + range_owners) * PMOST + slot_ranks(range_owners)).reshape(-1)
    parent_solution = jnp.zeros((PSLOTS, 16, 256), jnp.float32).at[slot_row].set(parent_four)
    return leaf_solution, parent_solution
```

```python
import jax
import jax.numpy as jnp
from jax import lax
from jax.experimental import pallas as pl
from jax.experimental.pallas import tpu as pltpu
from jax.sharding import PartitionSpec as P

FACTOR = 0.8 / 6.0
SWEEPS = 8
MESH = pl.DeviceIdType.MESH
LEAVES_HERE = 8
PARENTS_HERE = 16


def lane_roll(half, shift):
    return pltpu.roll(half, shift % 128, 1)


def row_roll(half, shift):
    return pltpu.roll(half, shift % half.shape[0], 0)


def both(ref, index):
    return [ref[0, index], ref[1, index]]


def lanes_of(ref, index):
    return [ref[index, :, 0:128], ref[index, :, 128:256]]


def flat_pair(ref, rows):
    return [ref[rows, 0:128], ref[rows, 128:256]]


def row_pair(ref, index):
    return [ref[index, :, 0:128], ref[index, :, 128:256]]


def put_row(ref, index, pair):
    ref[index, :, 0:128] = pair[0]
    ref[index, :, 128:256] = pair[1]


def put(ref, index, pair):
    ref[0, index] = pair[0]
    ref[1, index] = pair[1]


def put_flat(ref, rows, pair):
    ref[rows, 0:128] = pair[0]
    ref[rows, 128:256] = pair[1]


def split_dot(left, table):
    high = left.astype(jnp.bfloat16)
    low = (left - high.astype(jnp.float32)).astype(jnp.bfloat16)
    return jnp.dot(high, table, preferred_element_type=jnp.float32) + jnp.dot(
        low, table, preferred_element_type=jnp.float32
    )


def y_sum(lane, h, below, above):
    up = [lane_roll(h[0], 16), lane_roll(h[1], 16)]
    down = [lane_roll(h[0], -16), lane_roll(h[1], -16)]
    first = jnp.where(lane < 16, lane_roll(below, 16), up[0]) + jnp.where(
        lane >= 112, down[1], down[0]
    )
    second = jnp.where(lane < 16, up[0], up[1]) + jnp.where(
        lane >= 112, lane_roll(above, -16), down[1]
    )
    return [first, second]


def x_sum(lane, h, low, high):
    column = lane % 16
    return [
        jnp.where(column == 0, low[i], lane_roll(h[i], 1))
        + jnp.where(column == 15, high[i], lane_roll(h[i], -1))
        for i in range(2)
    ]


def z_sum(row, h, low, high):
    return [
        jnp.where(row == 0, low[i], row_roll(h[i], 1))
        + jnp.where(row == 15, high[i], row_roll(h[i], -1))
        for i in range(2)
    ]


def kernel(
    rhs,
    ln,
    pn,
    ch,
    ow,
    places,
    chv,
    leaf_out,
    parent_out,
    lv1,
    lv2,
    lv3,
    xs1,
    xs2,
    xs3,
    xr1,
    xr2,
    xr3,
    xt,
    zb1,
    zb2,
    zb3,
    res,
    oct_rows,
    src,
    pv1,
    pv2,
    pv3,
    pv4,
    geo,
    hsend,
    hrecv,
    hv,
    h2,
    own_rows,
    halo_two,
    rows_tmp,
    zq,
    slab,
    rbuf,
    rw,
    wm,
    we,
    msend,
    mrecv,
    lw,
    a_send,
    a_recv,
    c_send,
    c_recv,
    d_send,
    d_recv,
    f_send,
    f_recv,
    m_send,
    m_recv,
    tok,
):
    ranges = lax.axis_size("blk")
    subs = lax.axis_size("sub")
    r = lax.axis_index("blk")
    s = lax.axis_index("sub")
    barrier = pltpu.get_barrier_semaphore()
    for k in range(1, 16):
        pl.semaphore_signal(barrier, inc=1, device_id=(r, (s + k) % subs), device_id_type=MESH)
    for d in (1, -1, 2, -2):
        pl.semaphore_signal(
            barrier, inc=1, device_id=((r + d + ranges) % ranges, s), device_id_type=MESH
        )

    lane = lax.broadcasted_iota(jnp.int32, (16, 128), 1)
    row = lax.broadcasted_iota(jnp.int32, (16, 128), 0)
    column = lane % 16
    column8 = column[0:8]
    zero_half = jnp.zeros((16, 128), jnp.float32)
    zeros = [zero_half, zero_half]

    here = r * subs + s
    leaf_y = [[None, None] for _ in range(LEAVES_HERE)]
    leaf_x = [[None, None] for _ in range(LEAVES_HERE)]
    leaf_z = [[None, None] for _ in range(LEAVES_HERE)]
    for b in range(LEAVES_HERE):
        for f in range(6):
            n = ln[b, f]
            local = jnp.where(n >= 0, n & 7, 8)
            if f < 2:
                leaf_x[b][f] = local
            elif f < 4:
                leaf_y[b][f - 2] = local
            else:
                remote = (n >> 3) != here
                own_base, far_base = (8, 16) if f == 4 else (0, 24)
                leaf_z[b][f - 4] = jnp.where(
                    n >= 0, (n & 7) + jnp.where(remote, far_base, own_base), 32
                )

    def pack_faces(values, xs, zb):
        for h in range(2):
            low = jnp.zeros((8, 128), jnp.float32)
            high = jnp.zeros((8, 128), jnp.float32)
            for b in range(LEAVES_HERE):
                for part in range(2):
                    v = values[h, b, part * 8 : part * 8 + 8, :]
                    k = part * 8 + b
                    low = jnp.where(column8 == k, lane_roll(v, k), low)
                    high = jnp.where(column8 == k, lane_roll(v, k - 15), high)
            xs[0, :, h * 128 : h * 128 + 128] = low
            xs[1, :, h * 128 : h * 128 + 128] = high
        for b in range(LEAVES_HERE):
            put_row(zb, b, [values[i, b, 0:1, :] for i in range(2)])
            put_row(zb, 8 + b, [values[i, b, 15:16, :] for i in range(2)])
        zb[32] = jnp.zeros((1, 256), jnp.float32)

    def exchange(step, xs, xr, zb):
        def remote(source, target, slot, device):
            return pltpu.make_async_remote_copy(
                src_ref=source,
                dst_ref=target,
                send_sem=a_send.at[step, slot],
                recv_sem=a_recv.at[step, slot],
                device_id=device,
                device_id_type=MESH,
            )

        return (
            (s > 0, s < subs - 1, remote(xs.at[0], xr.at[1], 0, (r, (s + subs - 1) % subs))),
            (s < subs - 1, s > 0, remote(xs.at[1], xr.at[0], 1, (r, (s + 1) % subs))),
            (
                r > 0,
                r < ranges - 1,
                remote(zb.at[0:8], zb.at[24:32], 2, ((r + ranges - 1) % ranges, s)),
            ),
            (
                r < ranges - 1,
                r > 0,
                remote(zb.at[8:16], zb.at[16:24], 3, ((r + 1) % ranges, s)),
            ),
        )

    def start_all(copies):
        for sends, _, copy in copies:

            @pl.when(sends)
            def _():
                copy.start()

    def wait_arrivals(copies):
        for _, arrives, copy in copies:

            @pl.when(arrives)
            def _():
                copy.wait_recv()

    def wait_departures(copies):
        for sends, _, copy in copies:

            @pl.when(sends)
            def _():
                copy.wait_send()

    def unpack_x(xr):
        for h in range(2):
            lanes = slice(h * 128, h * 128 + 128)
            below = xr[0, :, lanes]
            above = xr[1, :, lanes]
            for j in range(LEAVES_HERE):
                for part in range(2):
                    k = part * 8 + j
                    rows = slice(part * 8, part * 8 + 8)
                    xt[0, h, j, rows, :] = lane_roll(below, -k)
                    xt[1, h, j, rows, :] = lane_roll(above, 15 - k)

    def leaf_beside(values, zb, b):
        h = both(values, b)
        low = [xt[0, i, leaf_x[b][0]] for i in range(2)]
        high = [xt[1, i, leaf_x[b][1]] for i in range(2)]
        xsum = x_sum(lane, h, low, high)
        ysum = y_sum(
            lane,
            h,
            values[1, leaf_y[b][0]],
            values[0, leaf_y[b][1]],
        )
        zsum = z_sum(
            row,
            h,
            row_pair(zb, leaf_z[b][0]),
            row_pair(zb, leaf_z[b][1]),
        )
        return h, [xsum[i] + ysum[i] + zsum[i] for i in range(2)]

    def relaxed(h, beside, forcing):
        return [h[i] + FACTOR * (forcing[i] - (6.0 * h[i] - beside[i])) for i in range(2)]

    def rest(h, beside, forcing):
        return [forcing[i] - (6.0 * h[i] - beside[i]) for i in range(2)]

    for ref in (lv1, lv2, lv3):
        put(ref, 8, zeros)
    for ref in (pv1, pv2, pv3):
        put(ref, 16, zeros)
    for side in range(2):
        xt[side, 0, 8] = zero_half
        xt[side, 1, 8] = zero_half
    for side in range(2):
        for ref in (hv, h2, own_rows):
            ref[side * 17 + 16] = jnp.zeros((1, 256), jnp.float32)

    for b in range(LEAVES_HERE):
        put(lv1, b, [FACTOR * v for v in lanes_of(rhs, b)])
    pack_faces(lv1, xs1, zb1)
    pl.semaphore_wait(barrier, 19)
    first = exchange(0, xs1, xr1, zb1)
    start_all(first)

    def greet(step, distance):
        for d in (distance, -distance):
            pl.semaphore_signal(
                tok.at[step],
                inc=1,
                device_id=((r + d + ranges) % ranges, s),
                device_id_type=MESH,
            )

    greet(0, 2)

    def numbers(shape, dim):
        return lax.broadcasted_iota(jnp.int32, shape, dim)

    def table(hit):
        return jnp.where(hit, 1.0, 0.0).astype(jnp.bfloat16)

    source_id = numbers((512, 128), 0)
    target_id = numbers((512, 128), 1)
    restrict = table(
        ((source_id % 256) // 32 == target_id // 16)
        & ((source_id % 16) // 2 + (source_id // 256) * 8 == target_id % 16)
    )
    fine = numbers((256, 256), 0)
    grid = numbers((256, 256), 1)
    coarse_table = table(
        (fine // 64 == (grid // 32) % 4) & ((fine % 16) // 4 == grid % 4)
    )
    grid_in = numbers((256, 256), 0)
    fine_out = numbers((256, 256), 1)
    widen_table = table(
        (fine_out // 64 == (grid_in // 32) % 4) & ((fine_out % 16) // 4 == grid_in % 4)
    )
    octant_in = numbers((128, 256), 0)
    leaf_cell = numbers((128, 256), 1)
    leaf_table = table(
        (octant_in // 16 == leaf_cell // 32)
        & (octant_in % 16 == (leaf_cell % 16) // 2 + (s % 2) * 8)
    )

    def inside(n, base):
        return jnp.where(n >= 0, jnp.clip(n - base, 0, 15), 16)

    mine = r * 16
    lower = jnp.maximum(r - 1, 0) * 16
    upper = jnp.minimum(r + 1, ranges - 1) * 16
    own_ghost = [
        [
            inside(pn[f, mine + p], mine if f < 4 else (lower if f == 4 else upper))
            for f in range(6)
        ]
        for p in range(PARENTS_HERE)
    ]
    halo_base = (lower, upper)
    halo_ghost = [
        [[inside(pn[f, base + q], base) for f in range(4)] for q in range(PARENTS_HERE)]
        for base in halo_base
    ]
    halo_own = [
        [
            inside(pn[5 - side, halo_base[side] + q], mine)
            for q in range(PARENTS_HERE)
        ]
        for side in range(2)
    ]

    wait_arrivals(first)
    unpack_x(xr1)
    for b in range(LEAVES_HERE):
        h, beside = leaf_beside(lv1, zb1, b)
        put(lv2, b, relaxed(h, beside, lanes_of(rhs, b)))
    pack_faces(lv2, xs2, zb2)
    second = exchange(1, xs2, xr2, zb2)
    start_all(second)
    pl.semaphore_wait(tok.at[0], 2)
    greet(1, 4)

    def missing(base, p, f):
        return jnp.where(pn[f, base + p] < 0, FACTOR, 0.0).astype(jnp.float32)

    def edge_weight(base, p, shape, with_z):
        lanes = lax.broadcasted_iota(jnp.int32, shape, 1)
        rows = lax.broadcasted_iota(jnp.int32, shape, 0)
        pair = []
        for i in range(2):
            w = jnp.ones(shape, jnp.float32)
            w = w - jnp.where(lanes % 16 == 0, missing(base, p, 0), 0.0)
            w = w - jnp.where(lanes % 16 == 15, missing(base, p, 1), 0.0)
            if i == 0:
                w = w - jnp.where(lanes < 16, missing(base, p, 2), 0.0)
            else:
                w = w - jnp.where(lanes >= 112, missing(base, p, 3), 0.0)
            if with_z is None:
                w = w - jnp.where(rows == 0, missing(base, p, 4), 0.0)
                w = w - jnp.where(rows == 15, missing(base, p, 5), 0.0)
            else:
                w = w - missing(base, p, with_z)
            pair.append(w)
        return pair

    def parent_beside(values, halo, p):
        h = both(values, p)
        g = own_ghost[p]
        low = [lane_roll(v, -15) for v in both(values, g[0])]
        high = [lane_roll(v, 15) for v in both(values, g[1])]
        xsum = x_sum(lane, h, low, high)
        ysum = y_sum(lane, h, values[1, g[2]], values[0, g[3]])
        zsum = z_sum(
            row,
            h,
            row_pair(halo, g[4]),
            row_pair(halo, g[5] + 17),
        )
        return h, [xsum[i] + ysum[i] + zsum[i] for i in range(2)]

    for p in range(PARENTS_HERE):
        put(pv1, p, edge_weight(mine, p, (16, 128), None))
        for side in range(2):
            pair = edge_weight(halo_base[side], p, (1, 128), 5 - side)
            hv[side * 17 + p, :, 0:128] = pair[0]
            hv[side * 17 + p, :, 128:256] = pair[1]
    for p in range(PARENTS_HERE):
        h, beside = parent_beside(pv1, hv, p)
        put(geo, p, relaxed(h, beside, [0.0, 0.0]))

    wait_arrivals(second)
    unpack_x(xr2)
    for b in range(LEAVES_HERE):
        h, beside = leaf_beside(lv2, zb2, b)
        put(res, b, rest(h, beside, lanes_of(rhs, b)))
    pieces = []
    for b in range(LEAVES_HERE):
        pieces.append(
            jnp.concatenate(
                [
                    res[i, b, pl.ds(0, 8, stride=2), :] + res[i, b, pl.ds(1, 8, stride=2), :]
                    for i in range(2)
                ],
                axis=1,
            )
        )
    stacked = jnp.concatenate(
        [jnp.concatenate(pieces[0:4], axis=0), jnp.concatenate(pieces[4:8], axis=0)], axis=1
    )
    oct_rows[s] = split_dot(0.5 * stacked, restrict).reshape(4, 8, 128)

    def octants(k):
        return pltpu.make_async_remote_copy(
            src_ref=oct_rows.at[s],
            dst_ref=oct_rows.at[s],
            send_sem=c_send.at[k],
            recv_sem=c_recv.at[k],
            device_id=(r, (s + k) % subs),
            device_id_type=MESH,
        )

    order = (8, 2, 10, 6, 14, 7, 9, 5, 11, 3, 13, 4, 12, 1, 15)
    for k in order:
        octants(k).start()

    pl.semaphore_wait(tok.at[1], 2)
    greet(2, 8)

    leaf_parent = []
    leaf_octant = []
    flat = numbers((8, 512), 1) * 8 + numbers((8, 512), 0)
    leaf_ids = chv[...]
    for b in range(LEAVES_HERE):
        found = jnp.sum(jnp.where(leaf_ids == here * 8 + b, flat, 0)) - mine * 8
        found = jnp.clip(found, 0, 127)
        leaf_parent.append(found >> 3)
        leaf_octant.append(found & 7)
    slot_parent = [jnp.int32(0)] * 3
    slot_filled = [jnp.int32(0)] * 3
    seen = jnp.int32(0)
    for p in range(PARENTS_HERE):
        owned = ow[mine + p] == s
        for k in range(3):
            take = jnp.logical_and(owned, seen == k)
            slot_parent[k] = jnp.where(take, p, slot_parent[k])
            slot_filled[k] = jnp.where(take, 1, slot_filled[k])
        seen = seen + jnp.where(owned, 1, 0)

    for k in order:
        octants(k).wait_recv()

    for p in range(PARENTS_HERE):
        for oz in range(2):
            for oy in range(2):
                parts = []
                for ox in range(2):
                    n = jnp.clip(ch[4 * oz + 2 * oy + ox, mine + p] - mine * 8, 0, 127)
                    tile = oct_rows[n >> 3, n & 3]
                    wanted = ((n >> 2) & 1) == ox
                    parts.append(jnp.where(wanted, tile, lane_roll(tile, 8 if ox else -8)))
                src[oy, p, oz * 8 : oz * 8 + 8, :] = jnp.where(
                    column8 < 8, parts[0], parts[1]
                )

    for layer in range(2):
        for i in range(2):
            hsend[0, layer, :, i * 128 : i * 128 + 128] = src[i, :, layer, :]
            hsend[1, layer, :, i * 128 : i * 128 + 128] = src[i, :, 15 - layer, :]

    def halo_copy(direction):
        step = -1 if direction == 0 else 1
        return pltpu.make_async_remote_copy(
            src_ref=hsend.at[direction],
            dst_ref=hrecv.at[1 - direction],
            send_sem=d_send.at[direction],
            recv_sem=d_recv.at[direction],
            device_id=((r + step + ranges) % ranges, s),
            device_id_type=MESH,
        )

    halos = (
        (r > 0, r < ranges - 1, halo_copy(0)),
        (r < ranges - 1, r > 0, halo_copy(1)),
    )
    start_all(halos)

    total = jnp.zeros((16, 128), jnp.float32)
    for p in range(PARENTS_HERE):
        g = both(geo, p)
        v = both(src, p)
        total = total + g[0] * v[0] + g[1] * v[1]
    msend[0] = jnp.sum(total, axis=0, keepdims=True)
    pair_device = (r + 1 - 2 * (r % 2), s)

    def mean_copy(k):
        return pltpu.make_async_remote_copy(
            src_ref=msend.at[0 if k == 0 else 1],
            dst_ref=mrecv.at[k],
            send_sem=m_send.at[k],
            recv_sem=m_recv.at[k],
            device_id=pair_device if k == 0 else ((r + 2 * k) % ranges, s),
            device_id_type=MESH,
        )

    mean_copy(0).start()
    for p in range(PARENTS_HERE):
        put(pv1, p, [FACTOR * v for v in both(src, p)])
    pl.semaphore_wait(tok.at[2], 2)
    mean_copy(0).wait_recv()
    msend[1] = msend[0] + mrecv[0]
    for k in range(1, 16):
        mean_copy(k).start()

    root_row = numbers((24, 128), 0)
    root_lane = numbers((24, 128), 1)
    depth = root_row + 4 * r - 8
    domain = (depth >= 0) & (depth < 4 * ranges) & (root_row < 20)

    def root_sweeps(source):
        w = [FACTOR * v for v in source]
        for _ in range(SWEEPS - 1):
            up = [lane_roll(v, 32) for v in w]
            down = [lane_roll(v, -32) for v in w]
            ysum = [
                jnp.where(root_lane < 32, 0.0, up[0])
                + jnp.where(root_lane >= 96, down[1], down[0]),
                jnp.where(root_lane < 32, up[0], up[1])
                + jnp.where(root_lane >= 96, 0.0, down[1]),
            ]
            fresh = []
            for i in range(2):
                xsum = jnp.where(root_lane % 32 == 0, 0.0, lane_roll(w[i], 1)) + jnp.where(
                    root_lane % 32 == 31, 0.0, lane_roll(w[i], -1)
                )
                zsum = row_roll(w[i], 1) + row_roll(w[i], -1)
                fresh.append(
                    jnp.where(
                        domain,
                        w[i]
                        + FACTOR * (source[i] - (6.0 * w[i] - (xsum + ysum[i] + zsum))),
                        0.0,
                    )
                )
            w = fresh
        return w

    ones = jnp.where(domain, 1.0, 0.0).astype(jnp.float32)
    flat_root = root_sweeps([ones, ones])

    wait_arrivals(halos)

    def gather(ref, index_of):
        for q in range(PARENTS_HERE):
            rows_tmp[q : q + 1, :] = ref[index_of(q)]
        return flat_pair(rows_tmp, slice(0, 16))

    def spread(ref, side, pair):
        put_flat(rows_tmp, slice(0, 16), pair)
        for q in range(PARENTS_HERE):
            ref[side * 17 + q] = rows_tmp[q : q + 1, :]

    for side in range(2):
        spread(hv, side, [FACTOR * hrecv[side, 0, :, i * 128 : i * 128 + 128] for i in range(2)])
    for p in range(PARENTS_HERE):
        put_row(own_rows, p, [pv1[i, p, 0:1, :] for i in range(2)])
        put_row(own_rows, 17 + p, [pv1[i, p, 15:16, :] for i in range(2)])
    for side in range(2):
        near = [hrecv[side, 0, :, i * 128 : i * 128 + 128] for i in range(2)]
        deep = [hrecv[side, 1, :, i * 128 : i * 128 + 128] for i in range(2)]
        h = [FACTOR * v for v in near]
        ghost = halo_ghost[side]
        low = [lane_roll(v, -15) for v in gather(hv, lambda q: ghost[q][0] + side * 17)]
        high = [lane_roll(v, 15) for v in gather(hv, lambda q: ghost[q][1] + side * 17)]
        xsum = x_sum(lane, h, low, high)
        below = gather(hv, lambda q: ghost[q][2] + side * 17)[1]
        above = gather(hv, lambda q: ghost[q][3] + side * 17)[0]
        ysum = y_sum(lane, h, below, above)
        touching = gather(own_rows, lambda q: halo_own[side][q] + side * 17)
        beside = [xsum[i] + ysum[i] + FACTOR * deep[i] + touching[i] for i in range(2)]
        put_flat(halo_two, slice(side * 16, side * 16 + 16), relaxed(h, beside, near))
        spread(h2, side, flat_pair(halo_two, slice(side * 16, side * 16 + 16)))

    for p in range(PARENTS_HERE):
        h, beside = parent_beside(pv1, hv, p)
        put(pv2, p, relaxed(h, beside, both(src, p)))
    for p in range(PARENTS_HERE):
        h, beside = parent_beside(pv2, h2, p)
        put(pv4, p, rest(h, beside, both(src, p)))
    for p in range(PARENTS_HERE):
        for i in range(2):
            quad = pv4[i, p, pl.ds(0, 4, stride=4), :]
            for t in range(1, 4):
                quad = quad + pv4[i, p, pl.ds(t, 4, stride=4), :]
            zq[p * 4 : p * 4 + 4, i * 128 : i * 128 + 128] = 0.25 * quad
    zq[...] = split_dot(zq[...], coarse_table)
    place_lane = [numbers((4, 128), 1) % 32 // 4 + 8 * i for i in range(2)]
    pair = [jnp.zeros((4, 128), jnp.float32) for _ in range(2)]
    for p in range(PARENTS_HERE):
        place = places[mine + p] - mine
        for i in range(2):
            pair[i] = jnp.where(
                place_lane[i] == place, zq[p * 4 : p * 4 + 4, i * 128 : i * 128 + 128], pair[i]
            )
    slab[:, 0:128] = pair[0]
    slab[:, 128:256] = pair[1]

    shifts = (1, -1, 2, -2)

    def slab_copy(k):
        return pltpu.make_async_remote_copy(
            src_ref=slab,
            dst_ref=rbuf.at[2 - shifts[k]],
            send_sem=f_send.at[k],
            recv_sem=f_recv.at[k],
            device_id=((r + shifts[k] + ranges) % ranges, s),
            device_id_type=MESH,
        )

    slabs = tuple(
        (
            (r + d < ranges) if d > 0 else (r + d >= 0),
            (r - d >= 0) if d > 0 else (r - d < ranges),
            slab_copy(k),
        )
        for k, d in enumerate(shifts)
    )
    start_all(slabs)
    wait_arrivals(slabs)
    for slot in range(5):
        rw[slot * 4 : slot * 4 + 4, :] = slab[...] if slot == 2 else rbuf[slot]
    rw[20:24, :] = jnp.zeros((4, 256), jnp.float32)
    root = root_sweeps([jnp.where(domain, v, 0.0) for v in flat_pair(rw, slice(0, 24))])
    for k in range(1, 16):
        mean_copy(k).wait_recv()
    sums = msend[1]
    for k in range(1, 16):
        sums = sums + mrecv[k]
    mean = jnp.sum(sums) * (0.25 / (1024.0 * ranges))
    put_flat(rw, slice(0, 24), [root[i] - mean * flat_root[i] for i in range(2)])

    wide_lane = [numbers((4, 128), 1) % 32 // 4 + 8 * i for i in range(2)]
    for p in range(PARENTS_HERE):
        for i in range(2):
            lanes = slice(i * 128, i * 128 + 128)
            wm[p * 4 : p * 4 + 4, lanes] = jnp.where(
                wide_lane[i] == places[mine + p] - mine, rw[8:12, lanes], 0.0
            )
            wm[64 + p : 65 + p, lanes] = jnp.where(
                wide_lane[i][0:1] == places[lower + p] - lower, rw[7:8, lanes], 0.0
            )
            wm[80 + p : 81 + p, lanes] = jnp.where(
                wide_lane[i][0:1] == places[upper + p] - upper, rw[12:13, lanes], 0.0
            )
    we[...] = split_dot(wm[...], widen_table)
    for side in range(2):
        base = 64 + 16 * side
        rows = slice(side * 16, side * 16 + 16)
        grown = flat_pair(we, slice(base, base + 16))
        spread(h2, side, [v + grown[i] for i, v in enumerate(flat_pair(halo_two, rows))])
    for p in range(PARENTS_HERE):
        pair = []
        for i in range(2):
            lanes = slice(i * 128, i * 128 + 128)
            grown = jnp.where(
                row < 8,
                jnp.where(row < 4, we[p * 4 : p * 4 + 1, lanes], we[p * 4 + 1 : p * 4 + 2, lanes]),
                jnp.where(
                    row < 12, we[p * 4 + 2 : p * 4 + 3, lanes], we[p * 4 + 3 : p * 4 + 4, lanes]
                ),
            )
            pair.append(pv2[i, p] + grown)
        put(pv3, p, pair)
    for p in range(PARENTS_HERE):
        h, beside = parent_beside(pv3, h2, p)
        put(pv4, p, relaxed(h, beside, both(src, p)))

    tiles = []
    for b in range(LEAVES_HERE):
        own = both(pv4, leaf_parent[b])
        side = jnp.where(((leaf_octant[b] >> 1) & 1) == 1, own[1], own[0])
        tiles.append(jnp.where((leaf_octant[b] >> 2) == 1, side[8:16], side[0:8]))
    lw[...] = split_dot(jnp.concatenate(tiles, axis=0), leaf_table)
    for b in range(LEAVES_HERE):
        piece = lw[b * 8 : b * 8 + 8, :]
        for t in range(2):
            rows = pl.ds(t, 8, stride=2)
            for i in range(2):
                lv3[i, b, rows, :] = lv2[i, b, rows, :] + piece[:, i * 128 : i * 128 + 128]
    pack_faces(lv3, xs3, zb3)
    third = exchange(2, xs3, xr3, zb3)
    start_all(third)
    for k in range(3):
        own = both(pv4, slot_parent[k])
        for i in range(2):
            parent_out[k, :, i * 128 : i * 128 + 128] = jnp.where(
                slot_filled[k] == 1, own[i], 0.0
            )
    wait_arrivals(third)
    unpack_x(xr3)
    for b in range(LEAVES_HERE):
        h, beside = leaf_beside(lv3, zb3, b)
        pair = relaxed(h, beside, lanes_of(rhs, b))
        for i in range(2):
            leaf_out[b, :, i * 128 : i * 128 + 128] = pair[i]

    for copies in (first, second, third, halos, slabs):
        wait_departures(copies)
    for k in range(1, 16):
        octants(k).wait_send()
    for k in range(16):
        mean_copy(k).wait_send()


def local(rhs, leaf_neighbors, parent_neighbors, children, owners, parent_places):
    f32 = jnp.float32
    vmem = pl.BlockSpec(memory_space=pltpu.VMEM)
    smem = pl.BlockSpec(memory_space=pltpu.SMEM)
    kids = children.T
    return pl.pallas_call(
        kernel,
        out_shape=(
            jax.ShapeDtypeStruct((8, 16, 256), f32),
            jax.ShapeDtypeStruct((3, 16, 256), f32),
        ),
        in_specs=[vmem, smem, smem, smem, smem, smem, vmem],
        out_specs=(vmem, vmem),
        scratch_shapes=[
            pltpu.VMEM((2, 9, 16, 128), f32),
            pltpu.VMEM((2, 9, 16, 128), f32),
            pltpu.VMEM((2, 9, 16, 128), f32),
            pltpu.VMEM((2, 8, 256), f32),
            pltpu.VMEM((2, 8, 256), f32),
            pltpu.VMEM((2, 8, 256), f32),
            pltpu.VMEM((2, 8, 256), f32),
            pltpu.VMEM((2, 8, 256), f32),
            pltpu.VMEM((2, 8, 256), f32),
            pltpu.VMEM((2, 2, 9, 16, 128), f32),
            pltpu.VMEM((33, 1, 256), f32),
            pltpu.VMEM((33, 1, 256), f32),
            pltpu.VMEM((33, 1, 256), f32),
            pltpu.VMEM((2, 8, 16, 128), f32),
            pltpu.VMEM((16, 4, 8, 128), f32),
            pltpu.VMEM((2, 16, 16, 128), f32),
            pltpu.VMEM((2, 17, 16, 128), f32),
            pltpu.VMEM((2, 17, 16, 128), f32),
            pltpu.VMEM((2, 17, 16, 128), f32),
            pltpu.VMEM((2, 16, 16, 128), f32),
            pltpu.VMEM((2, 17, 16, 128), f32),
            pltpu.VMEM((2, 2, 16, 256), f32),
            pltpu.VMEM((2, 2, 16, 256), f32),
            pltpu.VMEM((34, 1, 256), f32),
            pltpu.VMEM((34, 1, 256), f32),
            pltpu.VMEM((34, 1, 256), f32),
            pltpu.VMEM((32, 256), f32),
            pltpu.VMEM((16, 256), f32),
            pltpu.VMEM((64, 256), f32),
            pltpu.VMEM((4, 256), f32),
            pltpu.VMEM((5, 4, 256), f32),
            pltpu.VMEM((24, 256), f32),
            pltpu.VMEM((96, 256), f32),
            pltpu.VMEM((96, 256), f32),
            pltpu.VMEM((2, 1, 128), f32),
            pltpu.VMEM((16, 1, 128), f32),
            pltpu.VMEM((64, 256), f32),
            pltpu.SemaphoreType.DMA((3, 4)),
            pltpu.SemaphoreType.DMA((3, 4)),
            pltpu.SemaphoreType.DMA((16,)),
            pltpu.SemaphoreType.DMA((16,)),
            pltpu.SemaphoreType.DMA((2,)),
            pltpu.SemaphoreType.DMA((2,)),
            pltpu.SemaphoreType.DMA((4,)),
            pltpu.SemaphoreType.DMA((4,)),
            pltpu.SemaphoreType.DMA((16,)),
            pltpu.SemaphoreType.DMA((16,)),
            pltpu.SemaphoreType.REGULAR((3,)),
        ],
        compiler_params=pltpu.CompilerParams(collective_id=0, has_side_effects=True),
        name="vcycle",
    )(
        rhs,
        leaf_neighbors,
        parent_neighbors.T,
        kids,
        owners,
        parent_places,
        kids,
    )


def solution(mesh):
    in_specs = (P(("blk", "sub"), None, None), P(("blk", "sub"), None), P(), P(), P(), P())
    out_specs = (P(("blk", "sub"), None, None), P(("blk", "sub"), None, None))
    return jax.shard_map(local, mesh=mesh, in_specs=in_specs, out_specs=out_specs, check_vma=False)
```

```python
import jax
import jax.numpy as jnp
from jax import lax
from jax.experimental import pallas as pl
from jax.experimental.pallas import tpu as pltpu
from jax.sharding import PartitionSpec as P

FACTOR = 0.8 / 6.0
SWEEPS = 8
MESH = pl.DeviceIdType.MESH
LEAVES_HERE = 8
PARENTS_HERE = 16


def lane_roll(half, shift):
    return pltpu.roll(half, shift % 128, 1)


def row_roll(half, shift):
    return pltpu.roll(half, shift % half.shape[0], 0)


def both(ref, index):
    return [ref[0, index], ref[1, index]]


def lanes_of(ref, index):
    return [ref[index, :, 0:128], ref[index, :, 128:256]]


def flat_pair(ref, rows):
    return [ref[rows, 0:128], ref[rows, 128:256]]


def row_pair(ref, index):
    return [ref[index, :, 0:128], ref[index, :, 128:256]]


def put_row(ref, index, pair):
    ref[index, :, 0:128] = pair[0]
    ref[index, :, 128:256] = pair[1]


def put(ref, index, pair):
    ref[0, index] = pair[0]
    ref[1, index] = pair[1]


def put_flat(ref, rows, pair):
    ref[rows, 0:128] = pair[0]
    ref[rows, 128:256] = pair[1]


def split_dot(left, table):
    high = left.astype(jnp.bfloat16)
    low = (left - high.astype(jnp.float32)).astype(jnp.bfloat16)
    return jnp.dot(high, table, preferred_element_type=jnp.float32) + jnp.dot(
        low, table, preferred_element_type=jnp.float32
    )


def y_sum(lane, h, below, above):
    up = [lane_roll(h[0], 16), lane_roll(h[1], 16)]
    down = [lane_roll(h[0], -16), lane_roll(h[1], -16)]
    first = jnp.where(lane < 16, lane_roll(below, 16), up[0]) + jnp.where(
        lane >= 112, down[1], down[0]
    )
    second = jnp.where(lane < 16, up[0], up[1]) + jnp.where(
        lane >= 112, lane_roll(above, -16), down[1]
    )
    return [first, second]


def x_sum(lane, h, low, high):
    column = lane % 16
    return [
        jnp.where(column == 0, low[i], lane_roll(h[i], 1))
        + jnp.where(column == 15, high[i], lane_roll(h[i], -1))
        for i in range(2)
    ]


def z_sum(row, h, low, high):
    return [
        jnp.where(row == 0, low[i], row_roll(h[i], 1))
        + jnp.where(row == 15, high[i], row_roll(h[i], -1))
        for i in range(2)
    ]


def kernel(
    rhs_in,
    ln_in,
    pn_in,
    ch_in,
    ow_in,
    places_in,
    leaf_out,
    parent_out,
    rhs,
    ln,
    pn,
    ch,
    ow,
    places,
    chv,
    load_sem,
    ghost_table,
    pe3,
    pe4,
    le3,
    le4,
    xs4,
    xr4,
    zb4,
    lv1,
    lv2,
    lv3,
    xs1,
    xs2,
    xs3,
    xr1,
    xr2,
    xr3,
    xt,
    zb1,
    zb2,
    zb3,
    res,
    oct_rows,
    src,
    pv1,
    pv2,
    pv3,
    pv4,
    geo,
    hsend,
    hrecv,
    hv,
    h2,
    own_rows,
    halo_two,
    rows_tmp,
    zq,
    slab,
    rbuf,
    rw,
    wm,
    we,
    msend,
    mrecv,
    precv,
    lw,
    a_send,
    a_recv,
    c_send,
    c_recv,
    d_send,
    d_recv,
    f_send,
    f_recv,
    m_send,
    m_recv,
    p_send,
    p_recv,
    tok,
):
    ranges = lax.axis_size("blk")
    subs = lax.axis_size("sub")
    r = lax.axis_index("blk")
    s = lax.axis_index("sub")
    pairs = (
        (rhs_in, rhs),
        (ln_in, ln),
        (pn_in, pn),
        (ch_in, ch),
        (ch_in, chv),
        (ow_in, ow),
        (places_in, places),
    )
    loads = [
        pltpu.make_async_copy(source, target, load_sem.at[k])
        for k, (source, target) in enumerate(pairs)
    ]
    for load in loads:
        load.start()

    barrier = pltpu.get_barrier_semaphore()

    def exists(d):
        return (r + d < ranges) if d > 0 else (r + d >= 0)

    def signal_range(semaphore, distances):
        for d in distances:

            @pl.when(exists(d))
            def _():
                pl.semaphore_signal(
                    semaphore,
                    inc=1,
                    device_id=((r + d + ranges) % ranges, s),
                    device_id_type=MESH,
                )

    def signal_sub(semaphore, distances):
        for d in distances:
            pl.semaphore_signal(
                semaphore,
                inc=1,
                device_id=(r, (s + d + subs) % subs),
                device_id_type=MESH,
            )

    signal_range(barrier, (1, -1, 2, -2))
    signal_sub(barrier, (1, -1, 4, -4))
    middle = ranges // 2
    for k in range(2, 16):

        @pl.when((r < middle) & (r + 2 * k < ranges))
        def _():
            pl.semaphore_signal(
                barrier,
                inc=1,
                device_id=((r + 2 * k) % ranges, s),
                device_id_type=MESH,
            )

    greetings = 4 + sum(exists(d).astype(jnp.int32) for d in (1, -1, 2, -2))
    greetings = greetings + sum(
        ((r - 2 * k >= 0) & (r - 2 * k < middle)).astype(jnp.int32) for k in range(2, 16)
    )

    lane = lax.broadcasted_iota(jnp.int32, (16, 128), 1)
    row = lax.broadcasted_iota(jnp.int32, (16, 128), 0)
    column = lane % 16
    column8 = column[0:8]
    zero_half = jnp.zeros((16, 128), jnp.float32)
    zeros = [zero_half, zero_half]

    def pack_faces(values, xs, zb):
        for h in range(2):
            low = jnp.zeros((8, 128), jnp.float32)
            high = jnp.zeros((8, 128), jnp.float32)
            for b in range(LEAVES_HERE):
                for part in range(2):
                    v = values[h, b, part * 8 : part * 8 + 8, :]
                    k = part * 8 + b
                    low = jnp.where(column8 == k, lane_roll(v, k), low)
                    high = jnp.where(column8 == k, lane_roll(v, k - 15), high)
            xs[0, :, h * 128 : h * 128 + 128] = low
            xs[1, :, h * 128 : h * 128 + 128] = high
        for b in range(LEAVES_HERE):
            put_row(zb, b, [values[i, b, 0:1, :] for i in range(2)])
            put_row(zb, 8 + b, [values[i, b, 15:16, :] for i in range(2)])
        zb[32] = jnp.zeros((1, 256), jnp.float32)

    def exchange(step, xs, xr, zb):
        def remote(source, target, slot, device):
            return pltpu.make_async_remote_copy(
                src_ref=source,
                dst_ref=target,
                send_sem=a_send.at[step, slot],
                recv_sem=a_recv.at[step, slot],
                device_id=device,
                device_id_type=MESH,
            )

        return (
            (s > 0, s < subs - 1, remote(xs.at[0], xr.at[1], 0, (r, (s + subs - 1) % subs))),
            (s < subs - 1, s > 0, remote(xs.at[1], xr.at[0], 1, (r, (s + 1) % subs))),
            (
                r > 0,
                r < ranges - 1,
                remote(zb.at[0:8], zb.at[24:32], 2, ((r + ranges - 1) % ranges, s)),
            ),
            (
                r < ranges - 1,
                r > 0,
                remote(zb.at[8:16], zb.at[16:24], 3, ((r + 1) % ranges, s)),
            ),
        )

    def start_all(copies):
        for sends, _, copy in copies:

            @pl.when(sends)
            def _():
                copy.start()

    def wait_arrivals(copies):
        for _, arrives, copy in copies:

            @pl.when(arrives)
            def _():
                copy.wait_recv()

    def wait_departures(copies):
        for sends, _, copy in copies:

            @pl.when(sends)
            def _():
                copy.wait_send()

    def unpack_x(xr):
        for h in range(2):
            lanes = slice(h * 128, h * 128 + 128)
            below = xr[0, :, lanes]
            above = xr[1, :, lanes]
            for j in range(LEAVES_HERE):
                for part in range(2):
                    k = part * 8 + j
                    rows = slice(part * 8, part * 8 + 8)
                    xt[0, h, j, rows, :] = lane_roll(below, -k)
                    xt[1, h, j, rows, :] = lane_roll(above, 15 - k)

    def leaf_beside(values, zb, b):
        h = both(values, b)
        low = [xt[0, i, leaf_x[b][0]] for i in range(2)]
        high = [xt[1, i, leaf_x[b][1]] for i in range(2)]
        xsum = x_sum(lane, h, low, high)
        ysum = y_sum(
            lane,
            h,
            values[1, leaf_y[b][0]],
            values[0, leaf_y[b][1]],
        )
        zsum = z_sum(
            row,
            h,
            row_pair(zb, leaf_z[b][0]),
            row_pair(zb, leaf_z[b][1]),
        )
        return h, [xsum[i] + ysum[i] + zsum[i] for i in range(2)]

    def relaxed(h, beside, forcing):
        return [h[i] + FACTOR * (forcing[i] - (6.0 * h[i] - beside[i])) for i in range(2)]

    def rest(h, beside, forcing):
        return [forcing[i] - (6.0 * h[i] - beside[i]) for i in range(2)]

    for ref in (lv1, lv2, lv3, le3):
        put(ref, 8, zeros)
    for ref in (pv1, pv2, pv3, pe3):
        put(ref, 16, zeros)
    for side in range(2):
        xt[side, 0, 8] = zero_half
        xt[side, 1, 8] = zero_half
    for side in range(2):
        for ref in (hv, h2, own_rows):
            ref[side * 17 + 16] = jnp.zeros((1, 256), jnp.float32)

    loads[0].wait()
    for b in range(LEAVES_HERE):
        put(lv1, b, [FACTOR * v for v in lanes_of(rhs, b)])
    pack_faces(lv1, xs1, zb1)
    pl.semaphore_wait(barrier, greetings)
    first = exchange(0, xs1, xr1, zb1)
    start_all(first)

    def tell(stage):
        distance = 2 << stage

        @pl.when((r >= middle) & (r + distance < ranges))
        def _():
            pl.semaphore_signal(
                tok.at[stage],
                inc=1,
                device_id=((r + distance) % ranges, s),
                device_id_type=MESH,
            )

        @pl.when(r - distance >= middle)
        def _():
            pl.semaphore_signal(
                tok.at[stage],
                inc=1,
                device_id=((r - distance + ranges) % ranges, s),
                device_id_type=MESH,
            )

    def hear(stage):
        distance = 2 << stage
        peers = ((r >= middle) & (r + distance < ranges)).astype(jnp.int32)
        peers = peers + (r - distance >= middle).astype(jnp.int32)

        @pl.when(peers > 0)
        def _():
            pl.semaphore_wait(tok.at[stage], peers)

    tell(0)
    signal_sub(tok.at[4], (1, -1, 4, -4))

    loads[1].wait()
    here = r * subs + s
    leaf_y = [[None, None] for _ in range(LEAVES_HERE)]
    leaf_x = [[None, None] for _ in range(LEAVES_HERE)]
    leaf_z = [[None, None] for _ in range(LEAVES_HERE)]
    for b in range(LEAVES_HERE):
        for f in range(6):
            n = ln[b, f]
            local = jnp.where(n >= 0, n & 7, 8)
            if f < 2:
                leaf_x[b][f] = local
            elif f < 4:
                leaf_y[b][f - 2] = local
            else:
                remote = (n >> 3) != here
                own_base, far_base = (8, 16) if f == 4 else (0, 24)
                leaf_z[b][f - 4] = jnp.where(
                    n >= 0, (n & 7) + jnp.where(remote, far_base, own_base), 32
                )

    def numbers(shape, dim):
        return lax.broadcasted_iota(jnp.int32, shape, dim)

    def table(hit):
        return jnp.where(hit, 1.0, 0.0).astype(jnp.bfloat16)

    source_id = numbers((512, 128), 0)
    target_id = numbers((512, 128), 1)
    restrict = table(
        ((source_id % 256) // 32 == target_id // 16)
        & ((source_id % 16) // 2 + (source_id // 256) * 8 == target_id % 16)
    )
    fine = numbers((256, 256), 0)
    grid = numbers((256, 256), 1)
    coarse_table = table(
        (fine // 64 == (grid // 32) % 4) & ((fine % 16) // 4 == grid % 4)
    )
    grid_in = numbers((256, 256), 0)
    fine_out = numbers((256, 256), 1)
    widen_table = table(
        (fine_out // 64 == (grid_in // 32) % 4) & ((fine_out % 16) // 4 == grid_in % 4)
    )
    octant_in = numbers((128, 256), 0)
    leaf_cell = numbers((128, 256), 1)
    leaf_table = table(
        (octant_in // 16 == leaf_cell // 32)
        & (octant_in % 16 == (leaf_cell % 16) // 2 + (s % 2) * 8)
    )

    for load in loads[2:]:
        load.wait()
    def inside(n, base):
        return jnp.where(n >= 0, jnp.clip(n - base, 0, 15), 16)

    mine = r * 16
    lower = jnp.maximum(r - 1, 0) * 16
    upper = jnp.minimum(r + 1, ranges - 1) * 16
    own_ghost = [
        [
            inside(pn[f, mine + p], mine if f < 4 else (lower if f == 4 else upper))
            for f in range(6)
        ]
        for p in range(PARENTS_HERE)
    ]
    for p in range(PARENTS_HERE):
        for f in range(6):
            ghost_table[p * 6 + f] = own_ghost[p][f]
    halo_base = (lower, upper)
    halo_ghost = [
        [[inside(pn[f, base + q], base) for f in range(4)] for q in range(PARENTS_HERE)]
        for base in halo_base
    ]
    halo_own = [
        [
            inside(pn[5 - side, halo_base[side] + q], mine)
            for q in range(PARENTS_HERE)
        ]
        for side in range(2)
    ]

    hear(0)
    tell(1)
    wait_arrivals(first)
    hear(1)
    tell(2)
    pl.semaphore_wait(tok.at[4], 4)
    signal_sub(tok.at[5], (2, -2))
    unpack_x(xr1)
    for b in range(LEAVES_HERE):
        h, beside = leaf_beside(lv1, zb1, b)
        put(lv2, b, relaxed(h, beside, lanes_of(rhs, b)))
    pack_faces(lv2, xs2, zb2)
    second = exchange(1, xs2, xr2, zb2)
    start_all(second)

    def missing(base, p, f):
        return jnp.where(pn[f, base + p] < 0, FACTOR, 0.0).astype(jnp.float32)

    def edge_weight(base, p, shape, with_z):
        lanes = lax.broadcasted_iota(jnp.int32, shape, 1)
        rows = lax.broadcasted_iota(jnp.int32, shape, 0)
        pair = []
        for i in range(2):
            w = jnp.ones(shape, jnp.float32)
            w = w - jnp.where(lanes % 16 == 0, missing(base, p, 0), 0.0)
            w = w - jnp.where(lanes % 16 == 15, missing(base, p, 1), 0.0)
            if i == 0:
                w = w - jnp.where(lanes < 16, missing(base, p, 2), 0.0)
            else:
                w = w - jnp.where(lanes >= 112, missing(base, p, 3), 0.0)
            if with_z is None:
                w = w - jnp.where(rows == 0, missing(base, p, 4), 0.0)
                w = w - jnp.where(rows == 15, missing(base, p, 5), 0.0)
            else:
                w = w - missing(base, p, with_z)
            pair.append(w)
        return pair

    def parent_beside(values, halo, p):
        h = both(values, p)
        g = own_ghost[p] if isinstance(p, int) else [ghost_table[p * 6 + f] for f in range(6)]
        low = [lane_roll(v, -15) for v in both(values, g[0])]
        high = [lane_roll(v, 15) for v in both(values, g[1])]
        xsum = x_sum(lane, h, low, high)
        ysum = y_sum(lane, h, values[1, g[2]], values[0, g[3]])
        zsum = z_sum(
            row,
            h,
            row_pair(halo, g[4]),
            row_pair(halo, g[5] + 17),
        )
        return h, [xsum[i] + ysum[i] + zsum[i] for i in range(2)]

    for p in range(PARENTS_HERE):
        put(pv1, p, edge_weight(mine, p, (16, 128), None))
        for side in range(2):
            pair = edge_weight(halo_base[side], p, (1, 128), 5 - side)
            hv[side * 17 + p, :, 0:128] = pair[0]
            hv[side * 17 + p, :, 128:256] = pair[1]
    for p in range(PARENTS_HERE):
        h, beside = parent_beside(pv1, hv, p)
        put(geo, p, relaxed(h, beside, [0.0, 0.0]))

    leaf_parent = []
    leaf_octant = []
    flat = numbers((8, 512), 1) * 8 + numbers((8, 512), 0)
    leaf_ids = chv[...]
    for b in range(LEAVES_HERE):
        found = jnp.sum(jnp.where(leaf_ids == here * 8 + b, flat, 0)) - mine * 8
        found = jnp.clip(found, 0, 127)
        leaf_parent.append(found >> 3)
        leaf_octant.append(found & 7)

    first_parent = leaf_parent[0]
    last_parent = leaf_parent[0]
    for n in leaf_parent[1:]:
        first_parent = jnp.minimum(first_parent, n)
        last_parent = jnp.maximum(last_parent, n)
    leaf_slot = [jnp.where(n == last_parent, 1, 0) for n in leaf_parent]

    def widen_leaves(parents, where_from, base, target):
        tiles = []
        for b in range(LEAVES_HERE):
            own = both(parents, where_from[b])
            side = jnp.where(((leaf_octant[b] >> 1) & 1) == 1, own[1], own[0])
            tiles.append(jnp.where((leaf_octant[b] >> 2) == 1, side[8:16], side[0:8]))
        lw[...] = split_dot(jnp.concatenate(tiles, axis=0), leaf_table)
        for b in range(LEAVES_HERE):
            piece = flat_pair(lw, slice(b * 8, b * 8 + 8))
            for t in range(2):
                rows = pl.ds(t, 8, stride=2)
                for i in range(2):
                    target[i, b, rows, :] = (
                        piece[i] if base is None else base[i, b, rows, :] + piece[i]
                    )

    widen_leaves(geo, leaf_parent, None, lv3)

    wait_arrivals(second)
    unpack_x(xr2)
    for b in range(LEAVES_HERE):
        h, beside = leaf_beside(lv2, zb2, b)
        put(res, b, rest(h, beside, lanes_of(rhs, b)))
    pieces = []
    for b in range(LEAVES_HERE):
        pieces.append(
            jnp.concatenate(
                [
                    res[i, b, pl.ds(0, 8, stride=2), :] + res[i, b, pl.ds(1, 8, stride=2), :]
                    for i in range(2)
                ],
                axis=1,
            )
        )
    stacked = jnp.concatenate(
        [jnp.concatenate(pieces[0:4], axis=0), jnp.concatenate(pieces[4:8], axis=0)], axis=1
    )
    oct_rows[s] = split_dot(0.5 * stacked, restrict).reshape(4, 8, 128)

    def octants(k):
        return pltpu.make_async_remote_copy(
            src_ref=oct_rows.at[s],
            dst_ref=oct_rows.at[s],
            send_sem=c_send.at[k],
            recv_sem=c_recv.at[k],
            device_id=(r, (s + k) % subs),
            device_id_type=MESH,
        )

    order = (8, 2, 10, 6, 14, 7, 9, 5, 11, 3, 13, 4, 12, 1, 15)
    hear(2)
    pl.semaphore_wait(tok.at[5], 2)
    for k in order:
        octants(k).start()

    pair_device = (r + 1 - 2 * (r % 2), s)

    def mean_copy(k, distance=0):
        return pltpu.make_async_remote_copy(
            src_ref=msend.at[2 if k == 0 else 0],
            dst_ref=mrecv.at[k],
            send_sem=m_send.at[k],
            recv_sem=m_recv.at[k],
            device_id=pair_device if k == 0 else ((r + distance + ranges) % ranges, s),
            device_id_type=MESH,
        )

    lower_sums = tuple(
        (r >= 2 * k, r + 2 * k < ranges, mean_copy(k, -2 * k)) for k in range(1, 16)
    )
    upper_sums = tuple(
        (r + 2 * k < ranges, r >= 2 * k, mean_copy(15 + k, 2 * k)) for k in range(1, 16)
    )
    total = jnp.zeros((16, 128), jnp.float32)
    for b in range(LEAVES_HERE):
        q = both(lv3, b)
        v = both(res, b)
        total = total + q[0] * v[0] + q[1] * v[1]
    msend[0] = 0.5 * jnp.sum(total, axis=0, keepdims=True)
    start_all(lower_sums)

    @pl.when(r >= middle)
    def _():
        start_all(upper_sums)

    slot_parent = [jnp.int32(0)] * 3
    slot_filled = [jnp.int32(0)] * 3
    seen = jnp.int32(0)
    for p in range(PARENTS_HERE):
        owned = ow[mine + p] == s
        for k in range(3):
            take = jnp.logical_and(owned, seen == k)
            slot_parent[k] = jnp.where(take, p, slot_parent[k])
            slot_filled[k] = jnp.where(take, 1, slot_filled[k])
        seen = seen + jnp.where(owned, 1, 0)

    kids = [
        [jnp.clip(ch[o, mine + p] - mine * 8, 0, 127) for o in range(8)]
        for p in range(PARENTS_HERE)
    ]
    kid_dev = [[n >> 3 for n in line] for line in kids]
    kid_tile = [[n & 3 for n in line] for line in kids]
    kid_half = [[(n >> 2) & 1 for n in line] for line in kids]

    root_row = numbers((24, 128), 0)
    root_lane = numbers((24, 128), 1)
    depth = root_row + 4 * r - 8
    domain = (depth >= 0) & (depth < 4 * ranges) & (root_row < 20)

    def root_sweeps(source):
        w = [FACTOR * v for v in source]
        for _ in range(SWEEPS - 1):
            up = [lane_roll(v, 32) for v in w]
            down = [lane_roll(v, -32) for v in w]
            ysum = [
                jnp.where(root_lane < 32, 0.0, up[0])
                + jnp.where(root_lane >= 96, down[1], down[0]),
                jnp.where(root_lane < 32, up[0], up[1])
                + jnp.where(root_lane >= 96, 0.0, down[1]),
            ]
            fresh = []
            for i in range(2):
                xsum = jnp.where(root_lane % 32 == 0, 0.0, lane_roll(w[i], 1)) + jnp.where(
                    root_lane % 32 == 31, 0.0, lane_roll(w[i], -1)
                )
                zsum = row_roll(w[i], 1) + row_roll(w[i], -1)
                fresh.append(
                    jnp.where(
                        domain,
                        w[i]
                        + FACTOR * (source[i] - (6.0 * w[i] - (xsum + ysum[i] + zsum))),
                        0.0,
                    )
                )
            w = fresh
        return w

    ones = jnp.where(domain, 1.0, 0.0).astype(jnp.float32)
    flat_root = root_sweeps([ones, ones])

    wide_lane = [numbers((4, 128), 1) % 32 // 4 + 8 * i for i in range(2)]
    place_own = [places[mine + p] - mine for p in range(PARENTS_HERE)]
    place_halo = [[places[base + p] - base for p in range(PARENTS_HERE)] for base in halo_base]

    def widen_root(pair):
        put_flat(rw, slice(0, 24), pair)
        for p in range(PARENTS_HERE):
            for i in range(2):
                lanes = slice(i * 128, i * 128 + 128)
                wm[p * 4 : p * 4 + 4, lanes] = jnp.where(
                    wide_lane[i] == place_own[p], rw[8:12, lanes], 0.0
                )
                wm[64 + p : 65 + p, lanes] = jnp.where(
                    wide_lane[i][0:1] == place_halo[0][p], rw[7:8, lanes], 0.0
                )
                wm[80 + p : 81 + p, lanes] = jnp.where(
                    wide_lane[i][0:1] == place_halo[1][p], rw[12:13, lanes], 0.0
                )
        we[...] = split_dot(wm[...], widen_table)

    def widened(p):
        pair = []
        for i in range(2):
            lanes = slice(i * 128, i * 128 + 128)
            lines = [we[p * 4 + k : p * 4 + k + 1, lanes] for k in range(4)]
            pair.append(
                jnp.where(
                    row < 8,
                    jnp.where(row < 4, lines[0], lines[1]),
                    jnp.where(row < 12, lines[2], lines[3]),
                )
            )
        return pair

    def spread(ref, side, pair):
        put_flat(rows_tmp, slice(0, 16), pair)
        for q in range(PARENTS_HERE):
            ref[side * 17 + q] = rows_tmp[q : q + 1, :]

    def column_copy(k):
        return pltpu.make_async_remote_copy(
            src_ref=msend.at[1],
            dst_ref=precv.at[k],
            send_sem=p_send.at[k],
            recv_sem=p_recv.at[k],
            device_id=(r, (s + k) % subs),
            device_id_type=MESH,
        )


    def column_sums(now):
        @pl.when(now)
        def _():
            wait_arrivals(lower_sums)

            @pl.when(r < middle)
            def _():
                start_all(upper_sums)

            wait_arrivals(upper_sums)
            sums = msend[0]
            for k in range(1, 16):
                sums = sums + jnp.where(r + 2 * k < ranges, mrecv[k], 0.0)
                sums = sums + jnp.where(r >= 2 * k, mrecv[15 + k], 0.0)
            msend[1] = sums
            for k in order:
                column_copy(k).start()

    def plane_sums(now):
        @pl.when(now)
        def _():
            for k in order:
                column_copy(k).wait_recv()
            sums = msend[1]
            for k in range(1, 16):
                sums = sums + precv[k]
            msend[2] = sums
            mean_copy(0).start()


    widen_root(flat_root)
    for side in range(2):
        spread(h2, side, flat_pair(we, slice(64 + 16 * side, 80 + 16 * side)))
    for p in range(PARENTS_HERE):
        put(pe3, p, widened(p))
    for p in range(PARENTS_HERE):
        h, beside = parent_beside(pe3, h2, p)
        put(pe4, p, relaxed(h, beside, [0.0, 0.0]))
    widen_leaves(pe4, leaf_parent, None, le3)
    pack_faces(le3, xs4, zb4)
    fourth = exchange(3, xs4, xr4, zb4)
    start_all(fourth)

    for k in order:
        octants(k).wait_recv()

    for p in range(PARENTS_HERE):
        for oz in range(2):
            for oy in range(2):
                parts = []
                for ox in range(2):
                    o = 4 * oz + 2 * oy + ox
                    tile = oct_rows[kid_dev[p][o], kid_tile[p][o]]
                    wanted = kid_half[p][o] == ox
                    parts.append(jnp.where(wanted, tile, lane_roll(tile, 8 if ox else -8)))
                src[oy, p, oz * 8 : oz * 8 + 8, :] = jnp.where(
                    column8 < 8, parts[0], parts[1]
                )

    for layer in range(2):
        for i in range(2):
            hsend[0, layer, :, i * 128 : i * 128 + 128] = src[i, :, layer, :]
            hsend[1, layer, :, i * 128 : i * 128 + 128] = src[i, :, 15 - layer, :]

    def halo_copy(direction):
        step = -1 if direction == 0 else 1
        return pltpu.make_async_remote_copy(
            src_ref=hsend.at[direction],
            dst_ref=hrecv.at[1 - direction],
            send_sem=d_send.at[direction],
            recv_sem=d_recv.at[direction],
            device_id=((r + step + ranges) % ranges, s),
            device_id_type=MESH,
        )

    halos = (
        (r > 0, r < ranges - 1, halo_copy(0)),
        (r < ranges - 1, r > 0, halo_copy(1)),
    )
    start_all(halos)

    for p in range(PARENTS_HERE):
        put(pv1, p, [FACTOR * v for v in both(src, p)])

    wait_arrivals(halos)

    def gather(ref, index_of):
        for q in range(PARENTS_HERE):
            rows_tmp[q : q + 1, :] = ref[index_of(q)]
        return flat_pair(rows_tmp, slice(0, 16))

    for side in range(2):
        spread(hv, side, [FACTOR * hrecv[side, 0, :, i * 128 : i * 128 + 128] for i in range(2)])
    for p in range(PARENTS_HERE):
        put_row(own_rows, p, [pv1[i, p, 0:1, :] for i in range(2)])
        put_row(own_rows, 17 + p, [pv1[i, p, 15:16, :] for i in range(2)])
    for side in range(2):
        near = [hrecv[side, 0, :, i * 128 : i * 128 + 128] for i in range(2)]
        deep = [hrecv[side, 1, :, i * 128 : i * 128 + 128] for i in range(2)]
        h = [FACTOR * v for v in near]
        ghost = halo_ghost[side]
        low = [lane_roll(v, -15) for v in gather(hv, lambda q: ghost[q][0] + side * 17)]
        high = [lane_roll(v, 15) for v in gather(hv, lambda q: ghost[q][1] + side * 17)]
        xsum = x_sum(lane, h, low, high)
        below = gather(hv, lambda q: ghost[q][2] + side * 17)[1]
        above = gather(hv, lambda q: ghost[q][3] + side * 17)[0]
        ysum = y_sum(lane, h, below, above)
        touching = gather(own_rows, lambda q: halo_own[side][q] + side * 17)
        beside = [xsum[i] + ysum[i] + FACTOR * deep[i] + touching[i] for i in range(2)]
        put_flat(halo_two, slice(side * 16, side * 16 + 16), relaxed(h, beside, near))
        spread(h2, side, flat_pair(halo_two, slice(side * 16, side * 16 + 16)))

    for p in range(PARENTS_HERE):
        h, beside = parent_beside(pv1, hv, p)
        put(pv2, p, relaxed(h, beside, both(src, p)))
    for p in range(PARENTS_HERE):
        h, beside = parent_beside(pv2, h2, p)
        put(pv4, p, rest(h, beside, both(src, p)))
    for p in range(PARENTS_HERE):
        for i in range(2):
            quad = pv4[i, p, pl.ds(0, 4, stride=4), :]
            for t in range(1, 4):
                quad = quad + pv4[i, p, pl.ds(t, 4, stride=4), :]
            zq[p * 4 : p * 4 + 4, i * 128 : i * 128 + 128] = 0.25 * quad
    zq[...] = split_dot(zq[...], coarse_table)
    place_lane = [numbers((4, 128), 1) % 32 // 4 + 8 * i for i in range(2)]
    pair = [jnp.zeros((4, 128), jnp.float32) for _ in range(2)]
    for p in range(PARENTS_HERE):
        place = places[mine + p] - mine
        for i in range(2):
            pair[i] = jnp.where(
                place_lane[i] == place, zq[p * 4 : p * 4 + 4, i * 128 : i * 128 + 128], pair[i]
            )
    slab[:, 0:128] = pair[0]
    slab[:, 128:256] = pair[1]

    shifts = (1, -1, 2, -2)

    def slab_copy(k):
        return pltpu.make_async_remote_copy(
            src_ref=slab,
            dst_ref=rbuf.at[2 - shifts[k]],
            send_sem=f_send.at[k],
            recv_sem=f_recv.at[k],
            device_id=((r + shifts[k] + ranges) % ranges, s),
            device_id_type=MESH,
        )

    slabs = tuple(
        (
            (r + d < ranges) if d > 0 else (r + d >= 0),
            (r - d >= 0) if d > 0 else (r - d < ranges),
            slab_copy(k),
        )
        for k, d in enumerate(shifts)
    )
    start_all(slabs)
    wait_arrivals(fourth)
    unpack_x(xr4)
    for b in range(LEAVES_HERE):
        h, beside = leaf_beside(le3, zb4, b)
        put(le4, b, relaxed(h, beside, [0.0, 0.0]))

    column_sums(r < middle)
    wait_arrivals(slabs)
    for slot in range(5):
        rw[slot * 4 : slot * 4 + 4, :] = slab[...] if slot == 2 else rbuf[slot]
    rw[20:24, :] = jnp.zeros((4, 256), jnp.float32)
    root = root_sweeps([jnp.where(domain, v, 0.0) for v in flat_pair(rw, slice(0, 24))])
    widen_root(root)
    for side in range(2):
        base = 64 + 16 * side
        rows = slice(side * 16, side * 16 + 16)
        grown = flat_pair(we, slice(base, base + 16))
        spread(h2, side, [v + grown[i] for i, v in enumerate(flat_pair(halo_two, rows))])
    for p in range(PARENTS_HERE):
        grown = widened(p)
        put(pv3, p, [pv2[i, p] + grown[i] for i in range(2)])

    def parent_final(slot, p):
        h, beside = parent_beside(pv3, h2, p)
        put(pv4, slot, relaxed(h, beside, both(src, p)))

    parent_final(0, first_parent)
    parent_final(1, last_parent)

    widen_leaves(pv4, leaf_slot, lv2, lv3)
    pack_faces(lv3, xs3, zb3)
    third = exchange(2, xs3, xr3, zb3)
    start_all(third)
    for k in range(3):
        parent_final(2 + k, slot_parent[k])
    column_sums(r >= middle)
    plane_sums(r < middle)
    wait_arrivals(third)
    unpack_x(xr3)
    for b in range(LEAVES_HERE):
        h, beside = leaf_beside(lv3, zb3, b)
        put(lv1, b, relaxed(h, beside, lanes_of(rhs, b)))
    plane_sums(r >= middle)
    mean_copy(0).wait_recv()
    sums = msend[2] + mrecv[0]
    mean = jnp.sum(sums) * (0.25 / (1024.0 * ranges))
    for b in range(LEAVES_HERE):
        for i in range(2):
            leaf_out[b, :, i * 128 : i * 128 + 128] = lv1[i, b] - mean * le4[i, b]
    for k in range(3):
        own = both(pv4, 2 + k)
        flat = both(pe4, slot_parent[k])
        for i in range(2):
            parent_out[k, :, i * 128 : i * 128 + 128] = jnp.where(
                slot_filled[k] == 1, own[i] - mean * flat[i], 0.0
            )

    for copies in (first, second, third, fourth, halos, slabs):
        wait_departures(copies)
    for k in range(1, 16):
        octants(k).wait_send()
    mean_copy(0).wait_send()
    wait_departures(lower_sums)
    wait_departures(upper_sums)
    for k in order:
        column_copy(k).wait_send()


def local(rhs, leaf_neighbors, parent_neighbors, children, owners, parent_places):
    f32 = jnp.float32
    vmem = pl.BlockSpec(memory_space=pltpu.VMEM)
    hbm = pl.BlockSpec(memory_space=pltpu.HBM)
    return pl.pallas_call(
        kernel,
        out_shape=(
            jax.ShapeDtypeStruct((8, 16, 256), f32),
            jax.ShapeDtypeStruct((3, 16, 256), f32),
        ),
        in_specs=[hbm] * 6,
        out_specs=(vmem, vmem),
        scratch_shapes=[
            pltpu.VMEM((8, 16, 256), f32),
            pltpu.SMEM((8, 6), jnp.int32),
            pltpu.SMEM((6, 512), jnp.int32),
            pltpu.SMEM((8, 512), jnp.int32),
            pltpu.SMEM((512,), jnp.int32),
            pltpu.SMEM((512,), jnp.int32),
            pltpu.VMEM((8, 512), jnp.int32),
            pltpu.SemaphoreType.DMA((7,)),
            pltpu.SMEM((96,), jnp.int32),
            pltpu.VMEM((2, 17, 16, 128), f32),
            pltpu.VMEM((2, 16, 16, 128), f32),
            pltpu.VMEM((2, 9, 16, 128), f32),
            pltpu.VMEM((2, 8, 16, 128), f32),
            pltpu.VMEM((2, 8, 256), f32),
            pltpu.VMEM((2, 8, 256), f32),
            pltpu.VMEM((33, 1, 256), f32),
            pltpu.VMEM((2, 9, 16, 128), f32),
            pltpu.VMEM((2, 9, 16, 128), f32),
            pltpu.VMEM((2, 9, 16, 128), f32),
            pltpu.VMEM((2, 8, 256), f32),
            pltpu.VMEM((2, 8, 256), f32),
            pltpu.VMEM((2, 8, 256), f32),
            pltpu.VMEM((2, 8, 256), f32),
            pltpu.VMEM((2, 8, 256), f32),
            pltpu.VMEM((2, 8, 256), f32),
            pltpu.VMEM((2, 2, 9, 16, 128), f32),
            pltpu.VMEM((33, 1, 256), f32),
            pltpu.VMEM((33, 1, 256), f32),
            pltpu.VMEM((33, 1, 256), f32),
            pltpu.VMEM((2, 8, 16, 128), f32),
            pltpu.VMEM((16, 4, 8, 128), f32),
            pltpu.VMEM((2, 16, 16, 128), f32),
            pltpu.VMEM((2, 17, 16, 128), f32),
            pltpu.VMEM((2, 17, 16, 128), f32),
            pltpu.VMEM((2, 17, 16, 128), f32),
            pltpu.VMEM((2, 16, 16, 128), f32),
            pltpu.VMEM((2, 17, 16, 128), f32),
            pltpu.VMEM((2, 2, 16, 256), f32),
            pltpu.VMEM((2, 2, 16, 256), f32),
            pltpu.VMEM((34, 1, 256), f32),
            pltpu.VMEM((34, 1, 256), f32),
            pltpu.VMEM((34, 1, 256), f32),
            pltpu.VMEM((32, 256), f32),
            pltpu.VMEM((16, 256), f32),
            pltpu.VMEM((64, 256), f32),
            pltpu.VMEM((4, 256), f32),
            pltpu.VMEM((5, 4, 256), f32),
            pltpu.VMEM((24, 256), f32),
            pltpu.VMEM((96, 256), f32),
            pltpu.VMEM((96, 256), f32),
            pltpu.VMEM((3, 1, 128), f32),
            pltpu.VMEM((31, 1, 128), f32),
            pltpu.VMEM((16, 1, 128), f32),
            pltpu.VMEM((64, 256), f32),
            pltpu.SemaphoreType.DMA((4, 4)),
            pltpu.SemaphoreType.DMA((4, 4)),
            pltpu.SemaphoreType.DMA((16,)),
            pltpu.SemaphoreType.DMA((16,)),
            pltpu.SemaphoreType.DMA((2,)),
            pltpu.SemaphoreType.DMA((2,)),
            pltpu.SemaphoreType.DMA((4,)),
            pltpu.SemaphoreType.DMA((4,)),
            pltpu.SemaphoreType.DMA((31,)),
            pltpu.SemaphoreType.DMA((31,)),
            pltpu.SemaphoreType.DMA((16,)),
            pltpu.SemaphoreType.DMA((16,)),
            pltpu.SemaphoreType.REGULAR((6,)),
        ],
        compiler_params=pltpu.CompilerParams(collective_id=0, has_side_effects=True, vmem_limit_bytes=10 * 1024 * 1024),
        name="vcycle",
    )(
        *(
            pltpu.with_memory_space_constraint(v, pltpu.HBM)
            for v in (
                rhs,
                leaf_neighbors,
                parent_neighbors.T,
                children.T,
                owners,
                parent_places,
            )
        )
    )


def solution(mesh):
    in_specs = (P(("blk", "sub"), None, None), P(("blk", "sub"), None), P(), P(), P(), P())
    out_specs = (P(("blk", "sub"), None, None), P(("blk", "sub"), None, None))
    return jax.shard_map(local, mesh=mesh, in_specs=in_specs, out_specs=out_specs, check_vma=False)
```

```python
import jax
import jax.numpy as jnp
from jax import lax
from jax.experimental import pallas as pl
from jax.experimental.pallas import tpu as pltpu
from jax.sharding import PartitionSpec as P

FACTOR = 0.8 / 6.0
SWEEPS = 8
MESH = pl.DeviceIdType.MESH
LEAVES_HERE = 8
PARENTS_HERE = 16


def lane_roll(half, shift):
    return pltpu.roll(half, shift % 128, 1)


def row_roll(half, shift):
    return pltpu.roll(half, shift % half.shape[0], 0)


def both(ref, index):
    return [ref[0, index], ref[1, index]]


def lanes_of(ref, index):
    return [ref[index, :, 0:128], ref[index, :, 128:256]]


def flat_pair(ref, rows):
    return [ref[rows, 0:128], ref[rows, 128:256]]


def row_pair(ref, index):
    return [ref[index, :, 0:128], ref[index, :, 128:256]]


def put_row(ref, index, pair):
    ref[index, :, 0:128] = pair[0]
    ref[index, :, 128:256] = pair[1]


def put(ref, index, pair):
    ref[0, index] = pair[0]
    ref[1, index] = pair[1]


def put_flat(ref, rows, pair):
    ref[rows, 0:128] = pair[0]
    ref[rows, 128:256] = pair[1]


def split_dot(left, table):
    high = left.astype(jnp.bfloat16)
    low = (left - high.astype(jnp.float32)).astype(jnp.bfloat16)
    return jnp.dot(high, table, preferred_element_type=jnp.float32) + jnp.dot(
        low, table, preferred_element_type=jnp.float32
    )


def y_sum(lane, h, below, above):
    up = [lane_roll(h[0], 16), lane_roll(h[1], 16)]
    down = [lane_roll(h[0], -16), lane_roll(h[1], -16)]
    first = jnp.where(lane < 16, lane_roll(below, 16), up[0]) + jnp.where(
        lane >= 112, down[1], down[0]
    )
    second = jnp.where(lane < 16, up[0], up[1]) + jnp.where(
        lane >= 112, lane_roll(above, -16), down[1]
    )
    return [first, second]


def x_sum(lane, h, low, high):
    column = lane % 16
    return [
        jnp.where(column == 0, low[i], lane_roll(h[i], 1))
        + jnp.where(column == 15, high[i], lane_roll(h[i], -1))
        for i in range(2)
    ]


def z_sum(row, h, low, high):
    return [
        jnp.where(row == 0, low[i], row_roll(h[i], 1))
        + jnp.where(row == 15, high[i], row_roll(h[i], -1))
        for i in range(2)
    ]


def kernel(
    rhs_in,
    ln_in,
    pn_in,
    ch_in,
    ow_in,
    places_in,
    leaf_out,
    parent_out,
    rhs,
    ln,
    pn,
    ch,
    ow,
    places,
    chv,
    load_sem,
    ghost_table,
    pe3,
    pe4,
    le3,
    le4,
    xs4,
    xr4,
    zb4,
    lv1,
    lv2,
    lv3,
    xs3,
    xr3,
    xsm,
    xrm,
    zsm,
    zrm,
    line_send,
    lines,
    xt,
    zb1,
    zb2,
    zb3,
    res,
    oct_rows,
    src,
    pv1,
    pv2,
    pv3,
    pv4,
    geo,
    hsend,
    hrecv,
    hv,
    h2,
    own_rows,
    halo_two,
    rows_tmp,
    zq,
    slab,
    rbuf,
    rw,
    wm,
    we,
    msend,
    mrecv,
    precv,
    lw,
    a_send,
    a_recv,
    c_send,
    c_recv,
    d_send,
    d_recv,
    f_send,
    f_recv,
    m_send,
    m_recv,
    p_send,
    p_recv,
    tok,
):
    ranges = lax.axis_size("blk")
    subs = lax.axis_size("sub")
    r = lax.axis_index("blk")
    s = lax.axis_index("sub")
    pairs = (
        (rhs_in, rhs),
        (ln_in, ln),
        (pn_in, pn),
        (ch_in, ch),
        (ch_in, chv),
        (ow_in, ow),
        (places_in, places),
    )
    loads = [
        pltpu.make_async_copy(source, target, load_sem.at[k])
        for k, (source, target) in enumerate(pairs)
    ]
    for load in loads:
        load.start()

    barrier = pltpu.get_barrier_semaphore()

    def exists(d):
        return (r + d < ranges) if d > 0 else (r + d >= 0)

    def signal_range(semaphore, distances):
        for d in distances:

            @pl.when(exists(d))
            def _():
                pl.semaphore_signal(
                    semaphore,
                    inc=1,
                    device_id=((r + d + ranges) % ranges, s),
                    device_id_type=MESH,
                )

    def signal_sub(semaphore, distances):
        for d in distances:
            pl.semaphore_signal(
                semaphore,
                inc=1,
                device_id=(r, (s + d + subs) % subs),
                device_id_type=MESH,
            )

    signal_range(barrier, (1, -1, 2, -2))
    signal_sub(barrier, (1, -1, 4, -4))
    middle = ranges // 2
    for k in range(2, 16):

        @pl.when((r < middle) & (r + 2 * k < ranges))
        def _():
            pl.semaphore_signal(
                barrier,
                inc=1,
                device_id=((r + 2 * k) % ranges, s),
                device_id_type=MESH,
            )

    corners = tuple(
        ((r + dz >= 0) & (r + dz < ranges) & (s + dx >= 0) & (s + dx < subs), dz, dx)
        for dz in (-1, 1)
        for dx in (-1, 1)
    )
    for there, dz, dx in corners:

        @pl.when(there)
        def _():
            pl.semaphore_signal(
                barrier,
                inc=1,
                device_id=((r + dz + ranges) % ranges, (s + dx + subs) % subs),
                device_id_type=MESH,
            )

    greetings = 4 + sum(there.astype(jnp.int32) for there, _, _ in corners)
    greetings = greetings + sum(exists(d).astype(jnp.int32) for d in (1, -1, 2, -2))
    greetings = greetings + sum(
        ((r - 2 * k >= 0) & (r - 2 * k < middle)).astype(jnp.int32) for k in range(2, 16)
    )

    lane = lax.broadcasted_iota(jnp.int32, (16, 128), 1)
    row = lax.broadcasted_iota(jnp.int32, (16, 128), 0)
    column = lane % 16
    column8 = column[0:8]
    zero_half = jnp.zeros((16, 128), jnp.float32)
    zeros = [zero_half, zero_half]

    def pack_x(values, store):
        for h in range(2):
            low = jnp.zeros((8, 128), jnp.float32)
            high = jnp.zeros((8, 128), jnp.float32)
            for b in range(LEAVES_HERE):
                for part in range(2):
                    v = values[h, b, part * 8 : part * 8 + 8, :]
                    k = part * 8 + b
                    low = jnp.where(column8 == k, lane_roll(v, k), low)
                    high = jnp.where(column8 == k, lane_roll(v, k - 15), high)
            store(0, h, low)
            store(1, h, high)

    def local_rows(values, zb):
        for b in range(LEAVES_HERE):
            put_row(zb, b, [values[i, b, 0:1, :] for i in range(2)])
            put_row(zb, 8 + b, [values[i, b, 15:16, :] for i in range(2)])
        zb[32] = jnp.zeros((1, 256), jnp.float32)

    def pack_faces(values, xs, zb):
        def store(side, h, value):
            xs[side, :, h * 128 : h * 128 + 128] = value

        pack_x(values, store)
        local_rows(values, zb)

    def exchange(step, xs, xr, zb):
        def remote(source, target, slot, device):
            return pltpu.make_async_remote_copy(
                src_ref=source,
                dst_ref=target,
                send_sem=a_send.at[step, slot],
                recv_sem=a_recv.at[step, slot],
                device_id=device,
                device_id_type=MESH,
            )

        return (
            (s > 0, s < subs - 1, remote(xs.at[0], xr.at[1], 0, (r, (s + subs - 1) % subs))),
            (s < subs - 1, s > 0, remote(xs.at[1], xr.at[0], 1, (r, (s + 1) % subs))),
            (
                r > 0,
                r < ranges - 1,
                remote(zb.at[0:8], zb.at[24:32], 2, ((r + ranges - 1) % ranges, s)),
            ),
            (
                r < ranges - 1,
                r > 0,
                remote(zb.at[8:16], zb.at[16:24], 3, ((r + 1) % ranges, s)),
            ),
        )

    def start_all(copies):
        for sends, _, copy in copies:

            @pl.when(sends)
            def _():
                copy.start()

    def wait_arrivals(copies):
        for _, arrives, copy in copies:

            @pl.when(arrives)
            def _():
                copy.wait_recv()

    def wait_departures(copies):
        for sends, _, copy in copies:

            @pl.when(sends)
            def _():
                copy.wait_send()

    def unpack_faces(face_of):
        for h in range(2):
            below = face_of(0, h)
            above = face_of(1, h)
            for j in range(LEAVES_HERE):
                for part in range(2):
                    k = part * 8 + j
                    rows = slice(part * 8, part * 8 + 8)
                    xt[0, h, j, rows, :] = lane_roll(below, -k)
                    xt[1, h, j, rows, :] = lane_roll(above, 15 - k)

    def unpack_x(xr):
        unpack_faces(lambda side, h: xr[side, :, h * 128 : h * 128 + 128])

    def leaf_beside(values, zb, b):
        h = both(values, b)
        low = [xt[0, i, leaf_x[b][0]] for i in range(2)]
        high = [xt[1, i, leaf_x[b][1]] for i in range(2)]
        xsum = x_sum(lane, h, low, high)
        ysum = y_sum(
            lane,
            h,
            values[1, leaf_y[b][0]],
            values[0, leaf_y[b][1]],
        )
        zsum = z_sum(
            row,
            h,
            row_pair(zb, leaf_z[b][0]),
            row_pair(zb, leaf_z[b][1]),
        )
        return h, [xsum[i] + ysum[i] + zsum[i] for i in range(2)]

    def relaxed(h, beside, forcing):
        return [h[i] + FACTOR * (forcing[i] - (6.0 * h[i] - beside[i])) for i in range(2)]

    def rest(h, beside, forcing):
        return [forcing[i] - (6.0 * h[i] - beside[i]) for i in range(2)]

    for ref in (lv1, lv2, lv3, le3):
        put(ref, 8, zeros)
    for ref in (pv1, pv2, pv3, pe3):
        put(ref, 16, zeros)
    for side in range(2):
        xt[side, 0, 8] = zero_half
        xt[side, 1, 8] = zero_half
    for side in range(2):
        for ref in (hv, h2, own_rows):
            ref[side * 17 + 16] = jnp.zeros((1, 256), jnp.float32)

    loads[1].wait()
    here = r * subs + s
    leaf_y = [[None, None] for _ in range(LEAVES_HERE)]
    leaf_x = [[None, None] for _ in range(LEAVES_HERE)]
    leaf_z = [[None, None] for _ in range(LEAVES_HERE)]
    for b in range(LEAVES_HERE):
        for f in range(6):
            n = ln[b, f]
            local = jnp.where(n >= 0, n & 7, 8)
            if f < 2:
                leaf_x[b][f] = local
            elif f < 4:
                leaf_y[b][f - 2] = local
            else:
                remote = (n >> 3) != here
                own_base, far_base = (8, 16) if f == 4 else (0, 24)
                leaf_z[b][f - 4] = jnp.where(
                    n >= 0, (n & 7) + jnp.where(remote, far_base, own_base), 32
                )

    leaf_near = []
    leaf_far = []
    for b in range(LEAVES_HERE):
        far = [leaf_z[b][f] >= 16 for f in range(2)]
        leaf_near.append([jnp.where(far[f], 32, leaf_z[b][f]) for f in range(2)])
        leaf_far.append([jnp.where(far[f], leaf_z[b][f], 32) for f in range(2)])
    loads[0].wait()
    for b in range(LEAVES_HERE):
        put(lv1, b, [FACTOR * v for v in lanes_of(rhs, b)])
    local_rows(lv1, zb1)
    for b in range(LEAVES_HERE):
        h = both(lv1, b)
        xsum = x_sum(lane, h, [0.0, 0.0], [0.0, 0.0])
        ysum = y_sum(lane, h, lv1[1, leaf_y[b][0]], lv1[0, leaf_y[b][1]])
        zsum = z_sum(row, h, row_pair(zb1, leaf_near[b][0]), row_pair(zb1, leaf_near[b][1]))
        beside = [xsum[i] + ysum[i] + zsum[i] for i in range(2)]
        put(res, b, relaxed(h, beside, lanes_of(rhs, b)))
    row8 = row[0:8]
    for field, values in ((0, lv1), (1, res)):

        def store(side, h, value):
            xsm[side, field, :, h * 128 : h * 128 + 128] = value

        pack_x(values, store)
        for b in range(LEAVES_HERE):
            for i in range(2):
                lanes = slice(i * 128, i * 128 + 128)
                zsm[0, field, b : b + 1, lanes] = values[i, b, 0:1, :]
                zsm[1, field, b : b + 1, lanes] = values[i, b, 15:16, :]
    x_lines = jnp.full((8, 128), -100.0, jnp.float32)
    z_lines = jnp.full((8, 128), -100.0, jnp.float32)
    for b in range(LEAVES_HERE):
        down = jnp.where(leaf_z[b][0] >= 16, leaf_z[b][0] - 8, -100).astype(jnp.float32)
        up = jnp.where(leaf_far[b][1] < 32, leaf_z[b][1] - 24, -100).astype(jnp.float32)
        down = jnp.where(leaf_z[b][0] < 32, down, -100.0)
        x_lines = jnp.where((row8 == 0) & (column8 == b), down, x_lines)
        x_lines = jnp.where((row8 == 7) & (column8 == 8 + b), up, x_lines)
        left = jnp.where(leaf_x[b][0] < 8, leaf_x[b][0], -100).astype(jnp.float32)
        right = jnp.where(leaf_x[b][1] < 8, leaf_x[b][1], -100).astype(jnp.float32)
        z_lines = jnp.where((row8 == b) & (column8 == 0), left, z_lines)
        z_lines = jnp.where((row8 == b) & (column8 == 15), right, z_lines)
    for side in range(2):
        for i in range(2):
            lanes = slice(i * 128, i * 128 + 128)
            xsm[side, 2, :, lanes] = x_lines
            zsm[side, 2, :, lanes] = z_lines
            for zi in range(2):
                at = 0 if zi == 0 else 7
                line_send[2 * zi + side, :, lanes] = xsm[side, 0, at : at + 1, lanes]

    def first_copy(step, slot, source, target, device):
        return pltpu.make_async_remote_copy(
            src_ref=source,
            dst_ref=target,
            send_sem=a_send.at[step, slot],
            recv_sem=a_recv.at[step, slot],
            device_id=device,
            device_id_type=MESH,
        )

    pl.semaphore_wait(barrier, greetings)
    first = (
        (
            s > 0,
            s < subs - 1,
            first_copy(0, 0, xsm.at[0], xrm.at[1], (r, (s + subs - 1) % subs)),
        ),
        (s < subs - 1, s > 0, first_copy(0, 1, xsm.at[1], xrm.at[0], (r, (s + 1) % subs))),
        (
            r > 0,
            r < ranges - 1,
            first_copy(0, 2, zsm.at[0], zrm.at[1], ((r + ranges - 1) % ranges, s)),
        ),
        (r < ranges - 1, r > 0, first_copy(0, 3, zsm.at[1], zrm.at[0], ((r + 1) % ranges, s))),
    )
    first = first + tuple(
        (
            there,
            corners[3 - k][0],
            first_copy(
                1,
                k,
                line_send.at[k],
                lines.at[3 - k],
                ((r + dz + ranges) % ranges, (s + dx + subs) % subs),
            ),
        )
        for k, (there, dz, dx) in enumerate(corners)
    )
    start_all(first)

    def tell(stage):
        distance = 2 << stage

        @pl.when((r >= middle) & (r + distance < ranges))
        def _():
            pl.semaphore_signal(
                tok.at[stage],
                inc=1,
                device_id=((r + distance) % ranges, s),
                device_id_type=MESH,
            )

        @pl.when(r - distance >= middle)
        def _():
            pl.semaphore_signal(
                tok.at[stage],
                inc=1,
                device_id=((r - distance + ranges) % ranges, s),
                device_id_type=MESH,
            )

    def hear(stage):
        distance = 2 << stage
        peers = ((r >= middle) & (r + distance < ranges)).astype(jnp.int32)
        peers = peers + (r - distance >= middle).astype(jnp.int32)

        @pl.when(peers > 0)
        def _():
            pl.semaphore_wait(tok.at[stage], peers)

    tell(0)
    signal_sub(tok.at[4], (1, -1, 4, -4))

    def numbers(shape, dim):
        return lax.broadcasted_iota(jnp.int32, shape, dim)

    def table(hit):
        return jnp.where(hit, 1.0, 0.0).astype(jnp.bfloat16)

    source_id = numbers((512, 128), 0)
    target_id = numbers((512, 128), 1)
    restrict = table(
        ((source_id % 256) // 32 == target_id // 16)
        & ((source_id % 16) // 2 + (source_id // 256) * 8 == target_id % 16)
    )
    octant_in = numbers((128, 256), 0)
    leaf_cell = numbers((128, 256), 1)
    leaf_table = table(
        (octant_in // 16 == leaf_cell // 32)
        & (octant_in % 16 == (leaf_cell % 16) // 2 + (s % 2) * 8)
    )

    for load in loads[2:]:
        load.wait()
    def inside(n, base):
        return jnp.where(n >= 0, jnp.clip(n - base, 0, 15), 16)

    mine = r * 16
    lower = jnp.maximum(r - 1, 0) * 16
    upper = jnp.minimum(r + 1, ranges - 1) * 16
    own_ghost = [
        [
            inside(pn[f, mine + p], mine if f < 4 else (lower if f == 4 else upper))
            for f in range(6)
        ]
        for p in range(PARENTS_HERE)
    ]
    for p in range(PARENTS_HERE):
        for f in range(6):
            ghost_table[p * 6 + f] = own_ghost[p][f]
    halo_base = (lower, upper)
    halo_ghost = [
        [[inside(pn[f, base + q], base) for f in range(4)] for q in range(PARENTS_HERE)]
        for base in halo_base
    ]
    halo_own = [
        [
            inside(pn[5 - side, halo_base[side] + q], mine)
            for q in range(PARENTS_HERE)
        ]
        for side in range(2)
    ]


    def missing(base, p, f):
        return jnp.where(pn[f, base + p] < 0, FACTOR, 0.0).astype(jnp.float32)

    def edge_weight(base, p, shape, with_z):
        lanes = lax.broadcasted_iota(jnp.int32, shape, 1)
        rows = lax.broadcasted_iota(jnp.int32, shape, 0)
        pair = []
        for i in range(2):
            w = jnp.ones(shape, jnp.float32)
            w = w - jnp.where(lanes % 16 == 0, missing(base, p, 0), 0.0)
            w = w - jnp.where(lanes % 16 == 15, missing(base, p, 1), 0.0)
            if i == 0:
                w = w - jnp.where(lanes < 16, missing(base, p, 2), 0.0)
            else:
                w = w - jnp.where(lanes >= 112, missing(base, p, 3), 0.0)
            if with_z is None:
                w = w - jnp.where(rows == 0, missing(base, p, 4), 0.0)
                w = w - jnp.where(rows == 15, missing(base, p, 5), 0.0)
            else:
                w = w - missing(base, p, with_z)
            pair.append(w)
        return pair

    def parent_beside(values, halo, p):
        h = both(values, p)
        g = own_ghost[p] if isinstance(p, int) else [ghost_table[p * 6 + f] for f in range(6)]
        low = [lane_roll(v, -15) for v in both(values, g[0])]
        high = [lane_roll(v, 15) for v in both(values, g[1])]
        xsum = x_sum(lane, h, low, high)
        ysum = y_sum(lane, h, values[1, g[2]], values[0, g[3]])
        zsum = z_sum(
            row,
            h,
            row_pair(halo, g[4]),
            row_pair(halo, g[5] + 17),
        )
        return h, [xsum[i] + ysum[i] + zsum[i] for i in range(2)]

    for p in range(PARENTS_HERE):
        put(pv1, p, edge_weight(mine, p, (16, 128), None))
        for side in range(2):
            pair = edge_weight(halo_base[side], p, (1, 128), 5 - side)
            hv[side * 17 + p, :, 0:128] = pair[0]
            hv[side * 17 + p, :, 128:256] = pair[1]
    for p in range(PARENTS_HERE):
        h, beside = parent_beside(pv1, hv, p)
        put(geo, p, relaxed(h, beside, [0.0, 0.0]))

    leaf_parent = []
    leaf_octant = []
    flat = numbers((8, 512), 1) * 8 + numbers((8, 512), 0)
    leaf_ids = chv[...]
    for b in range(LEAVES_HERE):
        found = jnp.sum(jnp.where(leaf_ids == here * 8 + b, flat, 0)) - mine * 8
        found = jnp.clip(found, 0, 127)
        leaf_parent.append(found >> 3)
        leaf_octant.append(found & 7)

    first_parent = leaf_parent[0]
    last_parent = leaf_parent[0]
    for n in leaf_parent[1:]:
        first_parent = jnp.minimum(first_parent, n)
        last_parent = jnp.maximum(last_parent, n)
    leaf_slot = [jnp.where(n == last_parent, 1, 0) for n in leaf_parent]

    def widen_leaves(parents, where_from, base, target):
        tiles = []
        for b in range(LEAVES_HERE):
            own = both(parents, where_from[b])
            side = jnp.where(((leaf_octant[b] >> 1) & 1) == 1, own[1], own[0])
            tiles.append(jnp.where((leaf_octant[b] >> 2) == 1, side[8:16], side[0:8]))
        lw[...] = split_dot(jnp.concatenate(tiles, axis=0), leaf_table)
        for b in range(LEAVES_HERE):
            piece = flat_pair(lw, slice(b * 8, b * 8 + 8))
            for t in range(2):
                rows = pl.ds(t, 8, stride=2)
                for i in range(2):
                    target[i, b, rows, :] = (
                        piece[i] if base is None else base[i, b, rows, :] + piece[i]
                    )

    widen_leaves(geo, leaf_parent, None, lv3)

    hear(0)
    tell(1)
    pl.semaphore_wait(tok.at[4], 4)
    signal_sub(tok.at[5], (2, -2))
    wait_arrivals(first)
    hear(1)
    tell(2)
    unpack_faces(lambda side, h: xrm[side, 0, :, h * 128 : h * 128 + 128])
    for side in range(2):
        for n in range(LEAVES_HERE):
            zb1[16 + 8 * side + n] = zrm[side, 0, n : n + 1, :]
    for b in range(LEAVES_HERE):
        low = [xt[0, i, leaf_x[b][0]] for i in range(2)]
        high = [xt[1, i, leaf_x[b][1]] for i in range(2)]
        below = row_pair(zb1, leaf_far[b][0])
        above = row_pair(zb1, leaf_far[b][1])
        pair = []
        for i in range(2):
            more = jnp.where(column == 0, low[i], 0.0) + jnp.where(column == 15, high[i], 0.0)
            more = more + jnp.where(row == 0, below[i], 0.0) + jnp.where(row == 15, above[i], 0.0)
            pair.append(res[i, b] + FACTOR * more)
        put(lv2, b, pair)
    local_rows(lv2, zb2)

    def x_face(side, h):
        lanes = slice(h * 128, h * 128 + 128)
        hit = xrm[side, 2, :, lanes] - column8.astype(jnp.float32)
        more = jnp.zeros((8, 128), jnp.float32)
        for zi in range(2):
            line = jnp.broadcast_to(lines[2 * zi + side, :, lanes], (8, 128))
            for d in range(1, 16):
                shift = d if zi == 0 else -d
                wanted = (row8 == (0 if zi == 0 else 7)) & (hit == shift)
                more = jnp.where(wanted, lane_roll(line, -shift), more)
        return xrm[side, 1, :, lanes] + FACTOR * more

    unpack_faces(x_face)
    for zi in range(2):
        for h in range(2):
            lanes = slice(h * 128, h * 128 + 128)
            wanted = zrm[zi, 2, :, lanes]
            left = jnp.broadcast_to(lines[2 * zi, :, lanes], (8, 128))
            right = jnp.broadcast_to(lines[2 * zi + 1, :, lanes], (8, 128))
            more = jnp.zeros((8, 128), jnp.float32)
            for k in range(8):
                at = k + 8 if zi == 0 else k
                moved = jnp.where(column8 == 0, lane_roll(left, -at), lane_roll(right, 15 - at))
                more = jnp.where(wanted == k, moved, more)
            rows_tmp[zi * 8 : zi * 8 + 8, lanes] = zrm[zi, 1, :, lanes] + FACTOR * more
    for n in range(16):
        zb2[16 + n] = rows_tmp[n : n + 1, :]
    for b in range(LEAVES_HERE):
        v = both(lv1, b)
        h = both(lv2, b)
        side_gain = [jnp.where(leaf_x[b][f] < 8, FACTOR, 0.0).astype(jnp.float32) for f in range(2)]
        far_gain = [
            jnp.where(leaf_far[b][f] < 32, FACTOR, 0.0).astype(jnp.float32) for f in range(2)
        ]
        low = [xt[0, i, leaf_x[b][0]] + side_gain[0] * v[i] for i in range(2)]
        high = [xt[1, i, leaf_x[b][1]] + side_gain[1] * v[i] for i in range(2)]
        below = row_pair(zb2, leaf_z[b][0])
        above = row_pair(zb2, leaf_z[b][1])
        below = [below[i] + far_gain[0] * v[i][0:1] for i in range(2)]
        above = [above[i] + far_gain[1] * v[i][15:16] for i in range(2)]
        xsum = x_sum(lane, h, low, high)
        ysum = y_sum(lane, h, lv2[1, leaf_y[b][0]], lv2[0, leaf_y[b][1]])
        zsum = z_sum(row, h, below, above)
        put(res, b, rest(h, [xsum[i] + ysum[i] + zsum[i] for i in range(2)], lanes_of(rhs, b)))
    pieces = []
    for b in range(LEAVES_HERE):
        pieces.append(
            jnp.concatenate(
                [
                    res[i, b, pl.ds(0, 8, stride=2), :] + res[i, b, pl.ds(1, 8, stride=2), :]
                    for i in range(2)
                ],
                axis=1,
            )
        )
    stacked = jnp.concatenate(
        [jnp.concatenate(pieces[0:4], axis=0), jnp.concatenate(pieces[4:8], axis=0)], axis=1
    )
    oct_rows[s] = split_dot(0.5 * stacked, restrict).reshape(4, 8, 128)

    def octants(k):
        return pltpu.make_async_remote_copy(
            src_ref=oct_rows.at[s],
            dst_ref=oct_rows.at[s],
            send_sem=c_send.at[k],
            recv_sem=c_recv.at[k],
            device_id=(r, (s + k) % subs),
            device_id_type=MESH,
        )

    order = (8, 2, 10, 6, 14, 7, 9, 5, 11, 3, 13, 4, 12, 1, 15)
    pl.semaphore_wait(tok.at[5], 2)
    for k in order:
        octants(k).start()

    pair_device = (r + 1 - 2 * (r % 2), s)

    def mean_copy(k, distance=0):
        return pltpu.make_async_remote_copy(
            src_ref=msend.at[2 if k == 0 else 0],
            dst_ref=mrecv.at[k],
            send_sem=m_send.at[k],
            recv_sem=m_recv.at[k],
            device_id=pair_device if k == 0 else ((r + distance + ranges) % ranges, s),
            device_id_type=MESH,
        )

    lower_sums = tuple(
        (r >= 2 * k, r + 2 * k < ranges, mean_copy(k, -2 * k)) for k in range(1, 16)
    )
    upper_sums = tuple(
        (r + 2 * k < ranges, r >= 2 * k, mean_copy(15 + k, 2 * k)) for k in range(1, 16)
    )
    total = jnp.zeros((16, 128), jnp.float32)
    for b in range(LEAVES_HERE):
        q = both(lv3, b)
        v = both(res, b)
        total = total + q[0] * v[0] + q[1] * v[1]
    msend[0] = 0.5 * jnp.sum(total, axis=0, keepdims=True)
    hear(2)
    start_all(lower_sums)

    @pl.when(r >= middle)
    def _():
        start_all(upper_sums)

    fine = numbers((256, 256), 0)
    grid = numbers((256, 256), 1)
    coarse_table = table(
        (fine // 64 == (grid // 32) % 4) & ((fine % 16) // 4 == grid % 4)
    )
    grid_in = numbers((256, 256), 0)
    fine_out = numbers((256, 256), 1)
    widen_table = table(
        (fine_out // 64 == (grid_in // 32) % 4) & ((fine_out % 16) // 4 == grid_in % 4)
    )
    slot_parent = [jnp.int32(0)] * 3
    slot_filled = [jnp.int32(0)] * 3
    seen = jnp.int32(0)
    for p in range(PARENTS_HERE):
        owned = ow[mine + p] == s
        for k in range(3):
            take = jnp.logical_and(owned, seen == k)
            slot_parent[k] = jnp.where(take, p, slot_parent[k])
            slot_filled[k] = jnp.where(take, 1, slot_filled[k])
        seen = seen + jnp.where(owned, 1, 0)

    kids = [
        [jnp.clip(ch[o, mine + p] - mine * 8, 0, 127) for o in range(8)]
        for p in range(PARENTS_HERE)
    ]
    kid_dev = [[n >> 3 for n in line] for line in kids]
    kid_tile = [[n & 3 for n in line] for line in kids]
    kid_half = [[(n >> 2) & 1 for n in line] for line in kids]

    root_row = numbers((24, 128), 0)
    root_lane = numbers((24, 128), 1)
    depth = root_row + 4 * r - 8
    domain = (depth >= 0) & (depth < 4 * ranges) & (root_row < 20)

    def root_sweeps(source):
        w = [FACTOR * v for v in source]
        for _ in range(SWEEPS - 1):
            up = [lane_roll(v, 32) for v in w]
            down = [lane_roll(v, -32) for v in w]
            ysum = [
                jnp.where(root_lane < 32, 0.0, up[0])
                + jnp.where(root_lane >= 96, down[1], down[0]),
                jnp.where(root_lane < 32, up[0], up[1])
                + jnp.where(root_lane >= 96, 0.0, down[1]),
            ]
            fresh = []
            for i in range(2):
                xsum = jnp.where(root_lane % 32 == 0, 0.0, lane_roll(w[i], 1)) + jnp.where(
                    root_lane % 32 == 31, 0.0, lane_roll(w[i], -1)
                )
                zsum = row_roll(w[i], 1) + row_roll(w[i], -1)
                fresh.append(
                    jnp.where(
                        domain,
                        w[i]
                        + FACTOR * (source[i] - (6.0 * w[i] - (xsum + ysum[i] + zsum))),
                        0.0,
                    )
                )
            w = fresh
        return w

    ones = jnp.where(domain, 1.0, 0.0).astype(jnp.float32)
    flat_root = root_sweeps([ones, ones])

    wide_lane = [numbers((4, 128), 1) % 32 // 4 + 8 * i for i in range(2)]
    place_own = [places[mine + p] - mine for p in range(PARENTS_HERE)]
    place_halo = [[places[base + p] - base for p in range(PARENTS_HERE)] for base in halo_base]

    def widen_root(pair):
        put_flat(rw, slice(0, 24), pair)
        for p in range(PARENTS_HERE):
            for i in range(2):
                lanes = slice(i * 128, i * 128 + 128)
                wm[p * 4 : p * 4 + 4, lanes] = jnp.where(
                    wide_lane[i] == place_own[p], rw[8:12, lanes], 0.0
                )
                wm[64 + p : 65 + p, lanes] = jnp.where(
                    wide_lane[i][0:1] == place_halo[0][p], rw[7:8, lanes], 0.0
                )
                wm[80 + p : 81 + p, lanes] = jnp.where(
                    wide_lane[i][0:1] == place_halo[1][p], rw[12:13, lanes], 0.0
                )
        we[...] = split_dot(wm[...], widen_table)

    def widened(p):
        pair = []
        for i in range(2):
            lanes = slice(i * 128, i * 128 + 128)
            lines = [we[p * 4 + k : p * 4 + k + 1, lanes] for k in range(4)]
            pair.append(
                jnp.where(
                    row < 8,
                    jnp.where(row < 4, lines[0], lines[1]),
                    jnp.where(row < 12, lines[2], lines[3]),
                )
            )
        return pair

    def spread(ref, side, pair):
        put_flat(rows_tmp, slice(0, 16), pair)
        for q in range(PARENTS_HERE):
            ref[side * 17 + q] = rows_tmp[q : q + 1, :]

    def column_copy(k):
        return pltpu.make_async_remote_copy(
            src_ref=msend.at[1],
            dst_ref=precv.at[k],
            send_sem=p_send.at[k],
            recv_sem=p_recv.at[k],
            device_id=(r, (s + k) % subs),
            device_id_type=MESH,
        )


    def column_sums(now):
        @pl.when(now)
        def _():
            wait_arrivals(lower_sums)

            @pl.when(r < middle)
            def _():
                start_all(upper_sums)

            wait_arrivals(upper_sums)
            sums = msend[0]
            for k in range(1, 16):
                sums = sums + jnp.where(r + 2 * k < ranges, mrecv[k], 0.0)
                sums = sums + jnp.where(r >= 2 * k, mrecv[15 + k], 0.0)
            msend[1] = sums
            for k in order:
                column_copy(k).start()

    def plane_sums(now):
        @pl.when(now)
        def _():
            for k in order:
                column_copy(k).wait_recv()
            sums = msend[1]
            for k in range(1, 16):
                sums = sums + precv[k]
            msend[2] = sums
            mean_copy(0).start()


    widen_root(flat_root)
    for side in range(2):
        spread(h2, side, flat_pair(we, slice(64 + 16 * side, 80 + 16 * side)))
    for p in range(PARENTS_HERE):
        put(pe3, p, widened(p))
    for p in range(PARENTS_HERE):
        h, beside = parent_beside(pe3, h2, p)
        put(pe4, p, relaxed(h, beside, [0.0, 0.0]))
    widen_leaves(pe4, leaf_parent, None, le3)
    pack_faces(le3, xs4, zb4)
    fourth = exchange(3, xs4, xr4, zb4)
    start_all(fourth)

    for k in order:
        octants(k).wait_recv()

    for p in range(PARENTS_HERE):
        for oz in range(2):
            for oy in range(2):
                parts = []
                for ox in range(2):
                    o = 4 * oz + 2 * oy + ox
                    tile = oct_rows[kid_dev[p][o], kid_tile[p][o]]
                    wanted = kid_half[p][o] == ox
                    parts.append(jnp.where(wanted, tile, lane_roll(tile, 8 if ox else -8)))
                src[oy, p, oz * 8 : oz * 8 + 8, :] = jnp.where(
                    column8 < 8, parts[0], parts[1]
                )

    for layer in range(2):
        for i in range(2):
            hsend[0, layer, :, i * 128 : i * 128 + 128] = src[i, :, layer, :]
            hsend[1, layer, :, i * 128 : i * 128 + 128] = src[i, :, 15 - layer, :]

    def halo_copy(direction):
        step = -1 if direction == 0 else 1
        return pltpu.make_async_remote_copy(
            src_ref=hsend.at[direction],
            dst_ref=hrecv.at[1 - direction],
            send_sem=d_send.at[direction],
            recv_sem=d_recv.at[direction],
            device_id=((r + step + ranges) % ranges, s),
            device_id_type=MESH,
        )

    halos = (
        (r > 0, r < ranges - 1, halo_copy(0)),
        (r < ranges - 1, r > 0, halo_copy(1)),
    )
    start_all(halos)

    for p in range(PARENTS_HERE):
        put(pv1, p, [FACTOR * v for v in both(src, p)])

    wait_arrivals(halos)

    def gather(ref, index_of):
        for q in range(PARENTS_HERE):
            rows_tmp[q : q + 1, :] = ref[index_of(q)]
        return flat_pair(rows_tmp, slice(0, 16))

    for side in range(2):
        spread(hv, side, [FACTOR * hrecv[side, 0, :, i * 128 : i * 128 + 128] for i in range(2)])
    for p in range(PARENTS_HERE):
        put_row(own_rows, p, [pv1[i, p, 0:1, :] for i in range(2)])
        put_row(own_rows, 17 + p, [pv1[i, p, 15:16, :] for i in range(2)])
    for side in range(2):
        near = [hrecv[side, 0, :, i * 128 : i * 128 + 128] for i in range(2)]
        deep = [hrecv[side, 1, :, i * 128 : i * 128 + 128] for i in range(2)]
        h = [FACTOR * v for v in near]
        ghost = halo_ghost[side]
        low = [lane_roll(v, -15) for v in gather(hv, lambda q: ghost[q][0] + side * 17)]
        high = [lane_roll(v, 15) for v in gather(hv, lambda q: ghost[q][1] + side * 17)]
        xsum = x_sum(lane, h, low, high)
        below = gather(hv, lambda q: ghost[q][2] + side * 17)[1]
        above = gather(hv, lambda q: ghost[q][3] + side * 17)[0]
        ysum = y_sum(lane, h, below, above)
        touching = gather(own_rows, lambda q: halo_own[side][q] + side * 17)
        beside = [xsum[i] + ysum[i] + FACTOR * deep[i] + touching[i] for i in range(2)]
        put_flat(halo_two, slice(side * 16, side * 16 + 16), relaxed(h, beside, near))
        spread(h2, side, flat_pair(halo_two, slice(side * 16, side * 16 + 16)))

    for p in range(PARENTS_HERE):
        h, beside = parent_beside(pv1, hv, p)
        put(pv2, p, relaxed(h, beside, both(src, p)))
    for p in range(PARENTS_HERE):
        h, beside = parent_beside(pv2, h2, p)
        put(pv4, p, rest(h, beside, both(src, p)))
    for p in range(PARENTS_HERE):
        for i in range(2):
            quad = pv4[i, p, pl.ds(0, 4, stride=4), :]
            for t in range(1, 4):
                quad = quad + pv4[i, p, pl.ds(t, 4, stride=4), :]
            zq[p * 4 : p * 4 + 4, i * 128 : i * 128 + 128] = 0.25 * quad
    zq[...] = split_dot(zq[...], coarse_table)
    place_lane = [numbers((4, 128), 1) % 32 // 4 + 8 * i for i in range(2)]
    pair = [jnp.zeros((4, 128), jnp.float32) for _ in range(2)]
    for p in range(PARENTS_HERE):
        place = places[mine + p] - mine
        for i in range(2):
            pair[i] = jnp.where(
                place_lane[i] == place, zq[p * 4 : p * 4 + 4, i * 128 : i * 128 + 128], pair[i]
            )
    slab[:, 0:128] = pair[0]
    slab[:, 128:256] = pair[1]

    shifts = (1, -1, 2, -2)

    def slab_copy(k):
        return pltpu.make_async_remote_copy(
            src_ref=slab,
            dst_ref=rbuf.at[2 - shifts[k]],
            send_sem=f_send.at[k],
            recv_sem=f_recv.at[k],
            device_id=((r + shifts[k] + ranges) % ranges, s),
            device_id_type=MESH,
        )

    slabs = tuple(
        (
            (r + d < ranges) if d > 0 else (r + d >= 0),
            (r - d >= 0) if d > 0 else (r - d < ranges),
            slab_copy(k),
        )
        for k, d in enumerate(shifts)
    )
    start_all(slabs)
    wait_arrivals(fourth)
    unpack_x(xr4)
    for b in range(LEAVES_HERE):
        h, beside = leaf_beside(le3, zb4, b)
        put(le4, b, relaxed(h, beside, [0.0, 0.0]))

    column_sums(r < middle)
    wait_arrivals(slabs)
    for slot in range(5):
        rw[slot * 4 : slot * 4 + 4, :] = slab[...] if slot == 2 else rbuf[slot]
    rw[20:24, :] = jnp.zeros((4, 256), jnp.float32)
    root = root_sweeps([jnp.where(domain, v, 0.0) for v in flat_pair(rw, slice(0, 24))])
    widen_root(root)
    for side in range(2):
        base = 64 + 16 * side
        rows = slice(side * 16, side * 16 + 16)
        grown = flat_pair(we, slice(base, base + 16))
        spread(h2, side, [v + grown[i] for i, v in enumerate(flat_pair(halo_two, rows))])
    for p in range(PARENTS_HERE):
        grown = widened(p)
        put(pv3, p, [pv2[i, p] + grown[i] for i in range(2)])

    def parent_final(slot, p):
        h, beside = parent_beside(pv3, h2, p)
        put(pv4, slot, relaxed(h, beside, both(src, p)))

    parent_final(0, first_parent)
    parent_final(1, last_parent)

    widen_leaves(pv4, leaf_slot, lv2, lv3)
    pack_faces(lv3, xs3, zb3)
    third = exchange(2, xs3, xr3, zb3)
    start_all(third)
    for k in range(3):
        parent_final(2 + k, slot_parent[k])
    column_sums(r >= middle)
    plane_sums(r < middle)
    wait_arrivals(third)
    unpack_x(xr3)
    for b in range(LEAVES_HERE):
        h, beside = leaf_beside(lv3, zb3, b)
        put(lv1, b, relaxed(h, beside, lanes_of(rhs, b)))
    plane_sums(r >= middle)
    mean_copy(0).wait_recv()
    sums = msend[2] + mrecv[0]
    mean = jnp.sum(sums) * (0.25 / (1024.0 * ranges))
    for b in range(LEAVES_HERE):
        for i in range(2):
            leaf_out[b, :, i * 128 : i * 128 + 128] = lv1[i, b] - mean * le4[i, b]
    for k in range(3):
        own = both(pv4, 2 + k)
        flat = both(pe4, slot_parent[k])
        for i in range(2):
            parent_out[k, :, i * 128 : i * 128 + 128] = jnp.where(
                slot_filled[k] == 1, own[i] - mean * flat[i], 0.0
            )

    for copies in (first, third, fourth, halos, slabs):
        wait_departures(copies)
    for k in range(1, 16):
        octants(k).wait_send()
    mean_copy(0).wait_send()
    wait_departures(lower_sums)
    wait_departures(upper_sums)
    for k in order:
        column_copy(k).wait_send()


def local(rhs, leaf_neighbors, parent_neighbors, children, owners, parent_places):
    f32 = jnp.float32
    vmem = pl.BlockSpec(memory_space=pltpu.VMEM)
    hbm = pl.BlockSpec(memory_space=pltpu.HBM)
    return pl.pallas_call(
        kernel,
        out_shape=(
            jax.ShapeDtypeStruct((8, 16, 256), f32),
            jax.ShapeDtypeStruct((3, 16, 256), f32),
        ),
        in_specs=[hbm] * 6,
        out_specs=(vmem, vmem),
        scratch_shapes=[
            pltpu.VMEM((8, 16, 256), f32),
            pltpu.SMEM((8, 6), jnp.int32),
            pltpu.SMEM((6, 512), jnp.int32),
            pltpu.SMEM((8, 512), jnp.int32),
            pltpu.SMEM((512,), jnp.int32),
            pltpu.SMEM((512,), jnp.int32),
            pltpu.VMEM((8, 512), jnp.int32),
            pltpu.SemaphoreType.DMA((7,)),
            pltpu.SMEM((96,), jnp.int32),
            pltpu.VMEM((2, 17, 16, 128), f32),
            pltpu.VMEM((2, 16, 16, 128), f32),
            pltpu.VMEM((2, 9, 16, 128), f32),
            pltpu.VMEM((2, 8, 16, 128), f32),
            pltpu.VMEM((2, 8, 256), f32),
            pltpu.VMEM((2, 8, 256), f32),
            pltpu.VMEM((33, 1, 256), f32),
            pltpu.VMEM((2, 9, 16, 128), f32),
            pltpu.VMEM((2, 9, 16, 128), f32),
            pltpu.VMEM((2, 9, 16, 128), f32),
            pltpu.VMEM((2, 8, 256), f32),
            pltpu.VMEM((2, 8, 256), f32),
            pltpu.VMEM((2, 3, 8, 256), f32),
            pltpu.VMEM((2, 3, 8, 256), f32),
            pltpu.VMEM((2, 3, 8, 256), f32),
            pltpu.VMEM((2, 3, 8, 256), f32),
            pltpu.VMEM((4, 1, 256), f32),
            pltpu.VMEM((4, 1, 256), f32),
            pltpu.VMEM((2, 2, 9, 16, 128), f32),
            pltpu.VMEM((33, 1, 256), f32),
            pltpu.VMEM((33, 1, 256), f32),
            pltpu.VMEM((33, 1, 256), f32),
            pltpu.VMEM((2, 8, 16, 128), f32),
            pltpu.VMEM((16, 4, 8, 128), f32),
            pltpu.VMEM((2, 16, 16, 128), f32),
            pltpu.VMEM((2, 17, 16, 128), f32),
            pltpu.VMEM((2, 17, 16, 128), f32),
            pltpu.VMEM((2, 17, 16, 128), f32),
            pltpu.VMEM((2, 16, 16, 128), f32),
            pltpu.VMEM((2, 17, 16, 128), f32),
            pltpu.VMEM((2, 2, 16, 256), f32),
            pltpu.VMEM((2, 2, 16, 256), f32),
            pltpu.VMEM((34, 1, 256), f32),
            pltpu.VMEM((34, 1, 256), f32),
            pltpu.VMEM((34, 1, 256), f32),
            pltpu.VMEM((32, 256), f32),
            pltpu.VMEM((16, 256), f32),
            pltpu.VMEM((64, 256), f32),
            pltpu.VMEM((4, 256), f32),
            pltpu.VMEM((5, 4, 256), f32),
            pltpu.VMEM((24, 256), f32),
            pltpu.VMEM((96, 256), f32),
            pltpu.VMEM((96, 256), f32),
            pltpu.VMEM((3, 1, 128), f32),
            pltpu.VMEM((31, 1, 128), f32),
            pltpu.VMEM((16, 1, 128), f32),
            pltpu.VMEM((64, 256), f32),
            pltpu.SemaphoreType.DMA((4, 4)),
            pltpu.SemaphoreType.DMA((4, 4)),
            pltpu.SemaphoreType.DMA((16,)),
            pltpu.SemaphoreType.DMA((16,)),
            pltpu.SemaphoreType.DMA((2,)),
            pltpu.SemaphoreType.DMA((2,)),
            pltpu.SemaphoreType.DMA((4,)),
            pltpu.SemaphoreType.DMA((4,)),
            pltpu.SemaphoreType.DMA((31,)),
            pltpu.SemaphoreType.DMA((31,)),
            pltpu.SemaphoreType.DMA((16,)),
            pltpu.SemaphoreType.DMA((16,)),
            pltpu.SemaphoreType.REGULAR((6,)),
        ],
        compiler_params=pltpu.CompilerParams(collective_id=0, has_side_effects=True, vmem_limit_bytes=10 * 1024 * 1024),
        name="vcycle",
    )(
        *(
            pltpu.with_memory_space_constraint(v, pltpu.HBM)
            for v in (
                rhs,
                leaf_neighbors,
                parent_neighbors.T,
                children.T,
                owners,
                parent_places,
            )
        )
    )


def solution(mesh):
    in_specs = (P(("blk", "sub"), None, None), P(("blk", "sub"), None), P(), P(), P(), P())
    out_specs = (P(("blk", "sub"), None, None), P(("blk", "sub"), None, None))
    return jax.shard_map(local, mesh=mesh, in_specs=in_specs, out_specs=out_specs, check_vma=False)
```

```python
import jax
import jax.numpy as jnp
from jax import lax
from jax.experimental import pallas as pl
from jax.experimental.pallas import tpu as pltpu
from jax.sharding import PartitionSpec as P

FACTOR = 0.8 / 6.0
SWEEPS = 8
MESH = pl.DeviceIdType.MESH
LEAVES_HERE = 8
PARENTS_HERE = 16


def lane_roll(half, shift):
    return pltpu.roll(half, shift % 128, 1)


def row_roll(half, shift):
    return pltpu.roll(half, shift % half.shape[0], 0)


def both(ref, index):
    return [ref[0, index], ref[1, index]]


def lanes_of(ref, index):
    return [ref[index, :, 0:128], ref[index, :, 128:256]]


def flat_pair(ref, rows):
    return [ref[rows, 0:128], ref[rows, 128:256]]


def row_pair(ref, index):
    return [ref[index, :, 0:128], ref[index, :, 128:256]]


def put_row(ref, index, pair):
    ref[index, :, 0:128] = pair[0]
    ref[index, :, 128:256] = pair[1]


def put(ref, index, pair):
    ref[0, index] = pair[0]
    ref[1, index] = pair[1]


def put_flat(ref, rows, pair):
    ref[rows, 0:128] = pair[0]
    ref[rows, 128:256] = pair[1]


def split_dot(left, table):
    high = left.astype(jnp.bfloat16)
    low = (left - high.astype(jnp.float32)).astype(jnp.bfloat16)
    return jnp.dot(high, table, preferred_element_type=jnp.float32) + jnp.dot(
        low, table, preferred_element_type=jnp.float32
    )


def y_sum(lane, h, below, above):
    up = [lane_roll(h[0], 16), lane_roll(h[1], 16)]
    down = [lane_roll(h[0], -16), lane_roll(h[1], -16)]
    first = jnp.where(lane < 16, lane_roll(below, 16), up[0]) + jnp.where(
        lane >= 112, down[1], down[0]
    )
    second = jnp.where(lane < 16, up[0], up[1]) + jnp.where(
        lane >= 112, lane_roll(above, -16), down[1]
    )
    return [first, second]


def x_sum(lane, h, low, high):
    column = lane % 16
    return [
        jnp.where(column == 0, low[i], lane_roll(h[i], 1))
        + jnp.where(column == 15, high[i], lane_roll(h[i], -1))
        for i in range(2)
    ]


def z_sum(row, h, low, high):
    return [
        jnp.where(row == 0, low[i], row_roll(h[i], 1))
        + jnp.where(row == 15, high[i], row_roll(h[i], -1))
        for i in range(2)
    ]


def kernel(
    rhs_in,
    ln_in,
    pn_in,
    ch_in,
    ow_in,
    places_in,
    leaf_out,
    parent_out,
    rhs,
    ln,
    pn,
    ch,
    ow,
    places,
    chv,
    load_sem,
    ghost_table,
    pe3,
    pe4,
    le3,
    le4,
    xs4,
    xr4,
    zb4,
    lv1,
    lv2,
    lv3,
    xs3,
    xr3,
    xsm,
    xrm,
    zsm,
    zrm,
    line_send,
    lines,
    xt,
    zb1,
    zb2,
    zb3,
    res,
    oct_rows,
    src,
    pv1,
    pv2,
    pv3,
    pv4,
    geo,
    hsend,
    hrecv,
    hv,
    h2,
    own_rows,
    halo_two,
    rows_tmp,
    zq,
    slab,
    rbuf,
    rw,
    wm,
    we,
    msend,
    mrecv,
    precv,
    lw,
    a_send,
    a_recv,
    c_send,
    c_recv,
    d_send,
    d_recv,
    f_send,
    f_recv,
    m_send,
    m_recv,
    p_send,
    p_recv,
    tok,
):
    ranges = lax.axis_size("blk")
    subs = lax.axis_size("sub")
    r = lax.axis_index("blk")
    s = lax.axis_index("sub")
    pairs = (
        (rhs_in, rhs),
        (ln_in, ln),
        (pn_in, pn),
        (ch_in, ch),
        (ch_in, chv),
        (ow_in, ow),
        (places_in, places),
    )
    loads = [
        pltpu.make_async_copy(source, target, load_sem.at[k])
        for k, (source, target) in enumerate(pairs)
    ]
    for load in loads:
        load.start()

    barrier = pltpu.get_barrier_semaphore()

    def exists(d):
        return (r + d < ranges) if d > 0 else (r + d >= 0)

    def signal_range(semaphore, distances):
        for d in distances:

            @pl.when(exists(d))
            def _():
                pl.semaphore_signal(
                    semaphore,
                    inc=1,
                    device_id=((r + d + ranges) % ranges, s),
                    device_id_type=MESH,
                )

    def signal_sub(semaphore, distances):
        for d in distances:
            pl.semaphore_signal(
                semaphore,
                inc=1,
                device_id=(r, (s + d + subs) % subs),
                device_id_type=MESH,
            )

    signal_range(barrier, (1, -1, 2, -2))
    signal_sub(barrier, (1, -1, 4, -4))
    middle = ranges // 2
    for k in range(2, 16):

        @pl.when((r < middle) & (r + 2 * k < ranges))
        def _():
            pl.semaphore_signal(
                barrier,
                inc=1,
                device_id=((r + 2 * k) % ranges, s),
                device_id_type=MESH,
            )

    corners = tuple(
        ((r + dz >= 0) & (r + dz < ranges) & (s + dx >= 0) & (s + dx < subs), dz, dx)
        for dz in (-1, 1)
        for dx in (-1, 1)
    )
    for there, dz, dx in corners:

        @pl.when(there)
        def _():
            pl.semaphore_signal(
                barrier,
                inc=1,
                device_id=((r + dz + ranges) % ranges, (s + dx + subs) % subs),
                device_id_type=MESH,
            )

    greetings = 4 + sum(there.astype(jnp.int32) for there, _, _ in corners)
    greetings = greetings + sum(exists(d).astype(jnp.int32) for d in (1, -1, 2, -2))
    greetings = greetings + sum(
        ((r - 2 * k >= 0) & (r - 2 * k < middle)).astype(jnp.int32) for k in range(2, 16)
    )

    lane = lax.broadcasted_iota(jnp.int32, (16, 128), 1)
    row = lax.broadcasted_iota(jnp.int32, (16, 128), 0)
    column = lane % 16
    column8 = column[0:8]
    zero_half = jnp.zeros((16, 128), jnp.float32)
    zeros = [zero_half, zero_half]

    def pack_x(values, store):
        for h in range(2):
            low = jnp.zeros((8, 128), jnp.float32)
            high = jnp.zeros((8, 128), jnp.float32)
            for b in range(LEAVES_HERE):
                for part in range(2):
                    v = values[h, b, part * 8 : part * 8 + 8, :]
                    k = part * 8 + b
                    low = jnp.where(column8 == k, lane_roll(v, k), low)
                    high = jnp.where(column8 == k, lane_roll(v, k - 15), high)
            store(0, h, low)
            store(1, h, high)

    def local_rows(values, zb):
        for b in range(LEAVES_HERE):
            put_row(zb, b, [values[i, b, 0:1, :] for i in range(2)])
            put_row(zb, 8 + b, [values[i, b, 15:16, :] for i in range(2)])
        zb[32] = jnp.zeros((1, 256), jnp.float32)

    def pack_faces(values, xs, zb):
        def store(side, h, value):
            xs[side, :, h * 128 : h * 128 + 128] = value

        pack_x(values, store)
        local_rows(values, zb)

    def exchange(step, xs, xr, zb):
        def remote(source, target, slot, device):
            return pltpu.make_async_remote_copy(
                src_ref=source,
                dst_ref=target,
                send_sem=a_send.at[step, slot],
                recv_sem=a_recv.at[step, slot],
                device_id=device,
                device_id_type=MESH,
            )

        return (
            (s > 0, s < subs - 1, remote(xs.at[0], xr.at[1], 0, (r, (s + subs - 1) % subs))),
            (s < subs - 1, s > 0, remote(xs.at[1], xr.at[0], 1, (r, (s + 1) % subs))),
            (
                r > 0,
                r < ranges - 1,
                remote(zb.at[0:8], zb.at[24:32], 2, ((r + ranges - 1) % ranges, s)),
            ),
            (
                r < ranges - 1,
                r > 0,
                remote(zb.at[8:16], zb.at[16:24], 3, ((r + 1) % ranges, s)),
            ),
        )

    def start_all(copies):
        for sends, _, copy in copies:

            @pl.when(sends)
            def _():
                copy.start()

    def wait_arrivals(copies):
        for _, arrives, copy in copies:

            @pl.when(arrives)
            def _():
                copy.wait_recv()

    def wait_departures(copies):
        for sends, _, copy in copies:

            @pl.when(sends)
            def _():
                copy.wait_send()

    def unpack_faces(face_of):
        for h in range(2):
            below = face_of(0, h)
            above = face_of(1, h)
            for j in range(LEAVES_HERE):
                for part in range(2):
                    k = part * 8 + j
                    rows = slice(part * 8, part * 8 + 8)
                    xt[0, h, j, rows, :] = lane_roll(below, -k)
                    xt[1, h, j, rows, :] = lane_roll(above, 15 - k)

    def unpack_x(xr):
        unpack_faces(lambda side, h: xr[side, :, h * 128 : h * 128 + 128])

    def leaf_beside(values, zb, b):
        h = both(values, b)
        low = [xt[0, i, leaf_x[b][0]] for i in range(2)]
        high = [xt[1, i, leaf_x[b][1]] for i in range(2)]
        xsum = x_sum(lane, h, low, high)
        ysum = y_sum(
            lane,
            h,
            values[1, leaf_y[b][0]],
            values[0, leaf_y[b][1]],
        )
        zsum = z_sum(
            row,
            h,
            row_pair(zb, leaf_z[b][0]),
            row_pair(zb, leaf_z[b][1]),
        )
        return h, [xsum[i] + ysum[i] + zsum[i] for i in range(2)]

    def relaxed(h, beside, forcing):
        return [h[i] + FACTOR * (forcing[i] - (6.0 * h[i] - beside[i])) for i in range(2)]

    def rest(h, beside, forcing):
        return [forcing[i] - (6.0 * h[i] - beside[i]) for i in range(2)]

    for ref in (lv1, lv2, lv3, le3):
        put(ref, 8, zeros)
    for ref in (pv1, pv2, pv3, pe3):
        put(ref, 16, zeros)
    for side in range(2):
        xt[side, 0, 8] = zero_half
        xt[side, 1, 8] = zero_half
    for side in range(2):
        for ref in (hv, h2, own_rows):
            ref[side * 17 + 16] = jnp.zeros((1, 256), jnp.float32)

    loads[1].wait()
    here = r * subs + s
    leaf_y = [[None, None] for _ in range(LEAVES_HERE)]
    leaf_x = [[None, None] for _ in range(LEAVES_HERE)]
    leaf_z = [[None, None] for _ in range(LEAVES_HERE)]
    for b in range(LEAVES_HERE):
        for f in range(6):
            n = ln[b, f]
            local = jnp.where(n >= 0, n & 7, 8)
            if f < 2:
                leaf_x[b][f] = local
            elif f < 4:
                leaf_y[b][f - 2] = local
            else:
                remote = (n >> 3) != here
                own_base, far_base = (8, 16) if f == 4 else (0, 24)
                leaf_z[b][f - 4] = jnp.where(
                    n >= 0, (n & 7) + jnp.where(remote, far_base, own_base), 32
                )

    leaf_near = []
    leaf_far = []
    for b in range(LEAVES_HERE):
        far = [leaf_z[b][f] >= 16 for f in range(2)]
        leaf_near.append([jnp.where(far[f], 32, leaf_z[b][f]) for f in range(2)])
        leaf_far.append([jnp.where(far[f], leaf_z[b][f], 32) for f in range(2)])
    loads[0].wait()
    for b in range(LEAVES_HERE):
        put(lv1, b, [FACTOR * v for v in lanes_of(rhs, b)])
    local_rows(lv1, zb1)
    for b in range(LEAVES_HERE):
        h = both(lv1, b)
        xsum = x_sum(lane, h, [0.0, 0.0], [0.0, 0.0])
        ysum = y_sum(lane, h, lv1[1, leaf_y[b][0]], lv1[0, leaf_y[b][1]])
        zsum = z_sum(row, h, row_pair(zb1, leaf_near[b][0]), row_pair(zb1, leaf_near[b][1]))
        beside = [xsum[i] + ysum[i] + zsum[i] for i in range(2)]
        put(res, b, relaxed(h, beside, lanes_of(rhs, b)))
    row8 = row[0:8]
    for field, values in ((0, lv1), (1, res)):

        def store(side, h, value):
            xsm[side, field, :, h * 128 : h * 128 + 128] = value

        pack_x(values, store)
        for b in range(LEAVES_HERE):
            for i in range(2):
                lanes = slice(i * 128, i * 128 + 128)
                zsm[0, field, b : b + 1, lanes] = values[i, b, 0:1, :]
                zsm[1, field, b : b + 1, lanes] = values[i, b, 15:16, :]
    x_lines = jnp.full((8, 128), -100.0, jnp.float32)
    z_lines = jnp.full((8, 128), -100.0, jnp.float32)
    for b in range(LEAVES_HERE):
        down = jnp.where(leaf_z[b][0] >= 16, leaf_z[b][0] - 8, -100).astype(jnp.float32)
        up = jnp.where(leaf_far[b][1] < 32, leaf_z[b][1] - 24, -100).astype(jnp.float32)
        down = jnp.where(leaf_z[b][0] < 32, down, -100.0)
        x_lines = jnp.where((row8 == 0) & (column8 == b), down, x_lines)
        x_lines = jnp.where((row8 == 7) & (column8 == 8 + b), up, x_lines)
        left = jnp.where(leaf_x[b][0] < 8, leaf_x[b][0], -100).astype(jnp.float32)
        right = jnp.where(leaf_x[b][1] < 8, leaf_x[b][1], -100).astype(jnp.float32)
        z_lines = jnp.where((row8 == b) & (column8 == 0), left, z_lines)
        z_lines = jnp.where((row8 == b) & (column8 == 15), right, z_lines)
    for side in range(2):
        for i in range(2):
            lanes = slice(i * 128, i * 128 + 128)
            xsm[side, 2, :, lanes] = x_lines
            zsm[side, 2, :, lanes] = z_lines
            for zi in range(2):
                at = 0 if zi == 0 else 7
                line_send[2 * zi + side, :, lanes] = xsm[side, 0, at : at + 1, lanes]

    def first_copy(step, slot, source, target, device):
        return pltpu.make_async_remote_copy(
            src_ref=source,
            dst_ref=target,
            send_sem=a_send.at[step, slot],
            recv_sem=a_recv.at[step, slot],
            device_id=device,
            device_id_type=MESH,
        )

    pl.semaphore_wait(barrier, greetings)
    first = (
        (
            s > 0,
            s < subs - 1,
            first_copy(0, 0, xsm.at[0], xrm.at[1], (r, (s + subs - 1) % subs)),
        ),
        (s < subs - 1, s > 0, first_copy(0, 1, xsm.at[1], xrm.at[0], (r, (s + 1) % subs))),
        (
            r > 0,
            r < ranges - 1,
            first_copy(0, 2, zsm.at[0], zrm.at[1], ((r + ranges - 1) % ranges, s)),
        ),
        (r < ranges - 1, r > 0, first_copy(0, 3, zsm.at[1], zrm.at[0], ((r + 1) % ranges, s))),
    )
    first = first + tuple(
        (
            there,
            corners[3 - k][0],
            first_copy(
                1,
                k,
                line_send.at[k],
                lines.at[3 - k],
                ((r + dz + ranges) % ranges, (s + dx + subs) % subs),
            ),
        )
        for k, (there, dz, dx) in enumerate(corners)
    )
    start_all(first)

    def tell(stage):
        distance = 2 << stage

        @pl.when((r >= middle) & (r + distance < ranges))
        def _():
            pl.semaphore_signal(
                tok.at[stage],
                inc=1,
                device_id=((r + distance) % ranges, s),
                device_id_type=MESH,
            )

        @pl.when(r - distance >= middle)
        def _():
            pl.semaphore_signal(
                tok.at[stage],
                inc=1,
                device_id=((r - distance + ranges) % ranges, s),
                device_id_type=MESH,
            )

    def hear(stage):
        distance = 2 << stage
        peers = ((r >= middle) & (r + distance < ranges)).astype(jnp.int32)
        peers = peers + (r - distance >= middle).astype(jnp.int32)

        @pl.when(peers > 0)
        def _():
            pl.semaphore_wait(tok.at[stage], peers)

    tell(0)
    signal_sub(tok.at[4], (1, -1, 4, -4))

    def numbers(shape, dim):
        return lax.broadcasted_iota(jnp.int32, shape, dim)

    def table(hit):
        return jnp.where(hit, 1.0, 0.0).astype(jnp.bfloat16)

    source_id = numbers((512, 128), 0)
    target_id = numbers((512, 128), 1)
    restrict = table(
        ((source_id % 256) // 32 == target_id // 16)
        & ((source_id % 16) // 2 + (source_id // 256) * 8 == target_id % 16)
    )
    octant_in = numbers((128, 256), 0)
    leaf_cell = numbers((128, 256), 1)
    leaf_table = table(
        (octant_in // 16 == leaf_cell // 32)
        & (octant_in % 16 == (leaf_cell % 16) // 2 + (s % 2) * 8)
    )

    for load in loads[2:]:
        load.wait()
    def inside(n, base):
        return jnp.where(n >= 0, jnp.clip(n - base, 0, 15), 16)

    mine = r * 16
    lower = jnp.maximum(r - 1, 0) * 16
    upper = jnp.minimum(r + 1, ranges - 1) * 16
    own_ghost = [
        [
            inside(pn[f, mine + p], mine if f < 4 else (lower if f == 4 else upper))
            for f in range(6)
        ]
        for p in range(PARENTS_HERE)
    ]
    for p in range(PARENTS_HERE):
        for f in range(6):
            ghost_table[p * 6 + f] = own_ghost[p][f]
    halo_base = (lower, upper)
    halo_ghost = [
        [[inside(pn[f, base + q], base) for f in range(4)] for q in range(PARENTS_HERE)]
        for base in halo_base
    ]
    halo_own = [
        [
            inside(pn[5 - side, halo_base[side] + q], mine)
            for q in range(PARENTS_HERE)
        ]
        for side in range(2)
    ]


    hear(0)
    tell(1)

    def missing(base, p, f):
        return jnp.where(pn[f, base + p] < 0, FACTOR, 0.0).astype(jnp.float32)

    def edge_weight(base, p, shape, with_z):
        lanes = lax.broadcasted_iota(jnp.int32, shape, 1)
        rows = lax.broadcasted_iota(jnp.int32, shape, 0)
        pair = []
        for i in range(2):
            w = jnp.ones(shape, jnp.float32)
            w = w - jnp.where(lanes % 16 == 0, missing(base, p, 0), 0.0)
            w = w - jnp.where(lanes % 16 == 15, missing(base, p, 1), 0.0)
            if i == 0:
                w = w - jnp.where(lanes < 16, missing(base, p, 2), 0.0)
            else:
                w = w - jnp.where(lanes >= 112, missing(base, p, 3), 0.0)
            if with_z is None:
                w = w - jnp.where(rows == 0, missing(base, p, 4), 0.0)
                w = w - jnp.where(rows == 15, missing(base, p, 5), 0.0)
            else:
                w = w - missing(base, p, with_z)
            pair.append(w)
        return pair

    def parent_beside(values, halo, p):
        h = both(values, p)
        g = own_ghost[p] if isinstance(p, int) else [ghost_table[p * 6 + f] for f in range(6)]
        low = [lane_roll(v, -15) for v in both(values, g[0])]
        high = [lane_roll(v, 15) for v in both(values, g[1])]
        xsum = x_sum(lane, h, low, high)
        ysum = y_sum(lane, h, values[1, g[2]], values[0, g[3]])
        zsum = z_sum(
            row,
            h,
            row_pair(halo, g[4]),
            row_pair(halo, g[5] + 17),
        )
        return h, [xsum[i] + ysum[i] + zsum[i] for i in range(2)]

    for p in range(PARENTS_HERE):
        put(pv1, p, edge_weight(mine, p, (16, 128), None))
        for side in range(2):
            pair = edge_weight(halo_base[side], p, (1, 128), 5 - side)
            hv[side * 17 + p, :, 0:128] = pair[0]
            hv[side * 17 + p, :, 128:256] = pair[1]
    for p in range(PARENTS_HERE):
        h, beside = parent_beside(pv1, hv, p)
        put(geo, p, relaxed(h, beside, [0.0, 0.0]))

    leaf_parent = []
    leaf_octant = []
    flat = numbers((8, 512), 1) * 8 + numbers((8, 512), 0)
    leaf_ids = chv[...]
    for b in range(LEAVES_HERE):
        found = jnp.sum(jnp.where(leaf_ids == here * 8 + b, flat, 0)) - mine * 8
        found = jnp.clip(found, 0, 127)
        leaf_parent.append(found >> 3)
        leaf_octant.append(found & 7)

    first_parent = leaf_parent[0]
    last_parent = leaf_parent[0]
    for n in leaf_parent[1:]:
        first_parent = jnp.minimum(first_parent, n)
        last_parent = jnp.maximum(last_parent, n)
    leaf_slot = [jnp.where(n == last_parent, 1, 0) for n in leaf_parent]

    def widen_leaves(parents, where_from, base, target):
        tiles = []
        for b in range(LEAVES_HERE):
            own = both(parents, where_from[b])
            side = jnp.where(((leaf_octant[b] >> 1) & 1) == 1, own[1], own[0])
            tiles.append(jnp.where((leaf_octant[b] >> 2) == 1, side[8:16], side[0:8]))
        lw[...] = split_dot(jnp.concatenate(tiles, axis=0), leaf_table)
        for b in range(LEAVES_HERE):
            piece = flat_pair(lw, slice(b * 8, b * 8 + 8))
            for t in range(2):
                rows = pl.ds(t, 8, stride=2)
                for i in range(2):
                    target[i, b, rows, :] = (
                        piece[i] if base is None else base[i, b, rows, :] + piece[i]
                    )

    widen_leaves(geo, leaf_parent, None, lv3)

    hear(1)
    tell(2)
    pl.semaphore_wait(tok.at[4], 4)
    signal_sub(tok.at[5], (2, -2))
    wait_arrivals(first)
    unpack_faces(lambda side, h: xrm[side, 0, :, h * 128 : h * 128 + 128])
    for side in range(2):
        for n in range(LEAVES_HERE):
            zb1[16 + 8 * side + n] = zrm[side, 0, n : n + 1, :]
    for b in range(LEAVES_HERE):
        low = [xt[0, i, leaf_x[b][0]] for i in range(2)]
        high = [xt[1, i, leaf_x[b][1]] for i in range(2)]
        below = row_pair(zb1, leaf_far[b][0])
        above = row_pair(zb1, leaf_far[b][1])
        pair = []
        for i in range(2):
            more = jnp.where(column == 0, low[i], 0.0) + jnp.where(column == 15, high[i], 0.0)
            more = more + jnp.where(row == 0, below[i], 0.0) + jnp.where(row == 15, above[i], 0.0)
            pair.append(res[i, b] + FACTOR * more)
        put(lv2, b, pair)
    local_rows(lv2, zb2)

    def x_face(side, h):
        lanes = slice(h * 128, h * 128 + 128)
        hit = xrm[side, 2, :, lanes] - column8.astype(jnp.float32)
        more = jnp.zeros((8, 128), jnp.float32)
        for zi in range(2):
            line = jnp.broadcast_to(lines[2 * zi + side, :, lanes], (8, 128))
            for d in range(1, 16):
                shift = d if zi == 0 else -d
                wanted = (row8 == (0 if zi == 0 else 7)) & (hit == shift)
                more = jnp.where(wanted, lane_roll(line, -shift), more)
        return xrm[side, 1, :, lanes] + FACTOR * more

    unpack_faces(x_face)
    for zi in range(2):
        for h in range(2):
            lanes = slice(h * 128, h * 128 + 128)
            wanted = zrm[zi, 2, :, lanes]
            left = jnp.broadcast_to(lines[2 * zi, :, lanes], (8, 128))
            right = jnp.broadcast_to(lines[2 * zi + 1, :, lanes], (8, 128))
            more = jnp.zeros((8, 128), jnp.float32)
            for k in range(8):
                at = k + 8 if zi == 0 else k
                moved = jnp.where(column8 == 0, lane_roll(left, -at), lane_roll(right, 15 - at))
                more = jnp.where(wanted == k, moved, more)
            rows_tmp[zi * 8 : zi * 8 + 8, lanes] = zrm[zi, 1, :, lanes] + FACTOR * more
    for n in range(16):
        zb2[16 + n] = rows_tmp[n : n + 1, :]
    for b in range(LEAVES_HERE):
        v = both(lv1, b)
        h = both(lv2, b)
        side_gain = [jnp.where(leaf_x[b][f] < 8, FACTOR, 0.0).astype(jnp.float32) for f in range(2)]
        far_gain = [
            jnp.where(leaf_far[b][f] < 32, FACTOR, 0.0).astype(jnp.float32) for f in range(2)
        ]
        low = [xt[0, i, leaf_x[b][0]] + side_gain[0] * v[i] for i in range(2)]
        high = [xt[1, i, leaf_x[b][1]] + side_gain[1] * v[i] for i in range(2)]
        below = row_pair(zb2, leaf_z[b][0])
        above = row_pair(zb2, leaf_z[b][1])
        below = [below[i] + far_gain[0] * v[i][0:1] for i in range(2)]
        above = [above[i] + far_gain[1] * v[i][15:16] for i in range(2)]
        xsum = x_sum(lane, h, low, high)
        ysum = y_sum(lane, h, lv2[1, leaf_y[b][0]], lv2[0, leaf_y[b][1]])
        zsum = z_sum(row, h, below, above)
        put(res, b, rest(h, [xsum[i] + ysum[i] + zsum[i] for i in range(2)], lanes_of(rhs, b)))
    pieces = []
    for b in range(LEAVES_HERE):
        pieces.append(
            jnp.concatenate(
                [
                    res[i, b, pl.ds(0, 8, stride=2), :] + res[i, b, pl.ds(1, 8, stride=2), :]
                    for i in range(2)
                ],
                axis=1,
            )
        )
    stacked = jnp.concatenate(
        [jnp.concatenate(pieces[0:4], axis=0), jnp.concatenate(pieces[4:8], axis=0)], axis=1
    )
    oct_rows[s] = split_dot(0.5 * stacked, restrict).reshape(4, 8, 128)

    def octants(k):
        return pltpu.make_async_remote_copy(
            src_ref=oct_rows.at[s],
            dst_ref=oct_rows.at[s],
            send_sem=c_send.at[k],
            recv_sem=c_recv.at[k],
            device_id=(r, (s + k) % subs),
            device_id_type=MESH,
        )

    order = (8, 2, 10, 6, 14, 7, 9, 5, 11, 3, 13, 4, 12, 1, 15)
    pl.semaphore_wait(tok.at[5], 2)
    for k in order:
        octants(k).start()

    pair_device = (r + 1 - 2 * (r % 2), s)

    def mean_copy(k, distance=0):
        return pltpu.make_async_remote_copy(
            src_ref=msend.at[2 if k == 0 else 0],
            dst_ref=mrecv.at[k],
            send_sem=m_send.at[k],
            recv_sem=m_recv.at[k],
            device_id=pair_device if k == 0 else ((r + distance + ranges) % ranges, s),
            device_id_type=MESH,
        )

    lower_sums = tuple(
        (r >= 2 * k, r + 2 * k < ranges, mean_copy(k, -2 * k)) for k in range(1, 16)
    )
    upper_sums = tuple(
        (r + 2 * k < ranges, r >= 2 * k, mean_copy(15 + k, 2 * k)) for k in range(1, 16)
    )
    total = jnp.zeros((16, 128), jnp.float32)
    for b in range(LEAVES_HERE):
        q = both(lv3, b)
        v = both(res, b)
        total = total + q[0] * v[0] + q[1] * v[1]
    msend[0] = 0.5 * jnp.sum(total, axis=0, keepdims=True)
    start_all(
        tuple((sends & (r - 2 * k < middle), None, c) for k, (sends, _, c) in enumerate(lower_sums, 1))
    )
    hear(2)
    start_all(
        tuple((sends & (r - 2 * k >= middle), None, c) for k, (sends, _, c) in enumerate(lower_sums, 1))
    )

    @pl.when(r >= middle)
    def _():
        start_all(upper_sums)

    fine = numbers((256, 256), 0)
    grid = numbers((256, 256), 1)
    coarse_table = table(
        (fine // 64 == (grid // 32) % 4) & ((fine % 16) // 4 == grid % 4)
    )
    grid_in = numbers((256, 256), 0)
    fine_out = numbers((256, 256), 1)
    widen_table = table(
        (fine_out // 64 == (grid_in // 32) % 4) & ((fine_out % 16) // 4 == grid_in % 4)
    )
    slot_parent = [jnp.int32(0)] * 3
    slot_filled = [jnp.int32(0)] * 3
    seen = jnp.int32(0)
    for p in range(PARENTS_HERE):
        owned = ow[mine + p] == s
        for k in range(3):
            take = jnp.logical_and(owned, seen == k)
            slot_parent[k] = jnp.where(take, p, slot_parent[k])
            slot_filled[k] = jnp.where(take, 1, slot_filled[k])
        seen = seen + jnp.where(owned, 1, 0)

    kids = [
        [jnp.clip(ch[o, mine + p] - mine * 8, 0, 127) for o in range(8)]
        for p in range(PARENTS_HERE)
    ]
    kid_dev = [[n >> 3 for n in line] for line in kids]
    kid_tile = [[n & 3 for n in line] for line in kids]
    kid_half = [[(n >> 2) & 1 for n in line] for line in kids]

    root_row = numbers((24, 128), 0)
    root_lane = numbers((24, 128), 1)
    depth = root_row + 4 * r - 8
    domain = (depth >= 0) & (depth < 4 * ranges) & (root_row < 20)

    def root_sweeps(source):
        w = [FACTOR * v for v in source]
        for _ in range(SWEEPS - 1):
            up = [lane_roll(v, 32) for v in w]
            down = [lane_roll(v, -32) for v in w]
            ysum = [
                jnp.where(root_lane < 32, 0.0, up[0])
                + jnp.where(root_lane >= 96, down[1], down[0]),
                jnp.where(root_lane < 32, up[0], up[1])
                + jnp.where(root_lane >= 96, 0.0, down[1]),
            ]
            fresh = []
            for i in range(2):
                xsum = jnp.where(root_lane % 32 == 0, 0.0, lane_roll(w[i], 1)) + jnp.where(
                    root_lane % 32 == 31, 0.0, lane_roll(w[i], -1)
                )
                zsum = row_roll(w[i], 1) + row_roll(w[i], -1)
                fresh.append(
                    jnp.where(
                        domain,
                        w[i]
                        + FACTOR * (source[i] - (6.0 * w[i] - (xsum + ysum[i] + zsum))),
                        0.0,
                    )
                )
            w = fresh
        return w

    ones = jnp.where(domain, 1.0, 0.0).astype(jnp.float32)
    flat_root = root_sweeps([ones, ones])

    wide_lane = [numbers((4, 128), 1) % 32 // 4 + 8 * i for i in range(2)]
    place_own = [places[mine + p] - mine for p in range(PARENTS_HERE)]
    place_halo = [[places[base + p] - base for p in range(PARENTS_HERE)] for base in halo_base]

    def widen_root(pair):
        put_flat(rw, slice(0, 24), pair)
        for p in range(PARENTS_HERE):
            for i in range(2):
                lanes = slice(i * 128, i * 128 + 128)
                wm[p * 4 : p * 4 + 4, lanes] = jnp.where(
                    wide_lane[i] == place_own[p], rw[8:12, lanes], 0.0
                )
                wm[64 + p : 65 + p, lanes] = jnp.where(
                    wide_lane[i][0:1] == place_halo[0][p], rw[7:8, lanes], 0.0
                )
                wm[80 + p : 81 + p, lanes] = jnp.where(
                    wide_lane[i][0:1] == place_halo[1][p], rw[12:13, lanes], 0.0
                )
        we[...] = split_dot(wm[...], widen_table)

    def widened(p):
        pair = []
        for i in range(2):
            lanes = slice(i * 128, i * 128 + 128)
            lines = [we[p * 4 + k : p * 4 + k + 1, lanes] for k in range(4)]
            pair.append(
                jnp.where(
                    row < 8,
                    jnp.where(row < 4, lines[0], lines[1]),
                    jnp.where(row < 12, lines[2], lines[3]),
                )
            )
        return pair

    def spread(ref, side, pair):
        put_flat(rows_tmp, slice(0, 16), pair)
        for q in range(PARENTS_HERE):
            ref[side * 17 + q] = rows_tmp[q : q + 1, :]

    def column_copy(k):
        return pltpu.make_async_remote_copy(
            src_ref=msend.at[1],
            dst_ref=precv.at[k],
            send_sem=p_send.at[k],
            recv_sem=p_recv.at[k],
            device_id=(r, (s + k) % subs),
            device_id_type=MESH,
        )


    def column_sums(now):
        @pl.when(now)
        def _():
            wait_arrivals(lower_sums)

            @pl.when(r < middle)
            def _():
                start_all(upper_sums)

            wait_arrivals(upper_sums)
            sums = msend[0]
            for k in range(1, 16):
                sums = sums + jnp.where(r + 2 * k < ranges, mrecv[k], 0.0)
                sums = sums + jnp.where(r >= 2 * k, mrecv[15 + k], 0.0)
            msend[1] = sums
            for k in order:
                column_copy(k).start()

    def plane_sums(now):
        @pl.when(now)
        def _():
            for k in order:
                column_copy(k).wait_recv()
            sums = msend[1]
            for k in range(1, 16):
                sums = sums + precv[k]
            msend[2] = sums
            mean_copy(0).start()


    widen_root(flat_root)
    for side in range(2):
        spread(h2, side, flat_pair(we, slice(64 + 16 * side, 80 + 16 * side)))
    for p in range(PARENTS_HERE):
        put(pe3, p, widened(p))
    for p in range(PARENTS_HERE):
        h, beside = parent_beside(pe3, h2, p)
        put(pe4, p, relaxed(h, beside, [0.0, 0.0]))
    widen_leaves(pe4, leaf_parent, None, le3)
    pack_faces(le3, xs4, zb4)
    fourth = exchange(3, xs4, xr4, zb4)
    start_all(fourth)

    for k in order:
        octants(k).wait_recv()

    for p in range(PARENTS_HERE):
        for oz in range(2):
            for oy in range(2):
                parts = []
                for ox in range(2):
                    o = 4 * oz + 2 * oy + ox
                    tile = oct_rows[kid_dev[p][o], kid_tile[p][o]]
                    wanted = kid_half[p][o] == ox
                    parts.append(jnp.where(wanted, tile, lane_roll(tile, 8 if ox else -8)))
                src[oy, p, oz * 8 : oz * 8 + 8, :] = jnp.where(
                    column8 < 8, parts[0], parts[1]
                )

    for layer in range(2):
        for i in range(2):
            hsend[0, layer, :, i * 128 : i * 128 + 128] = src[i, :, layer, :]
            hsend[1, layer, :, i * 128 : i * 128 + 128] = src[i, :, 15 - layer, :]

    def halo_copy(direction):
        step = -1 if direction == 0 else 1
        return pltpu.make_async_remote_copy(
            src_ref=hsend.at[direction],
            dst_ref=hrecv.at[1 - direction],
            send_sem=d_send.at[direction],
            recv_sem=d_recv.at[direction],
            device_id=((r + step + ranges) % ranges, s),
            device_id_type=MESH,
        )

    halos = (
        (r > 0, r < ranges - 1, halo_copy(0)),
        (r < ranges - 1, r > 0, halo_copy(1)),
    )
    start_all(halos)

    for p in range(PARENTS_HERE):
        put(pv1, p, [FACTOR * v for v in both(src, p)])

    wait_arrivals(halos)

    def gather(ref, index_of):
        for q in range(PARENTS_HERE):
            rows_tmp[q : q + 1, :] = ref[index_of(q)]
        return flat_pair(rows_tmp, slice(0, 16))

    for side in range(2):
        spread(hv, side, [FACTOR * hrecv[side, 0, :, i * 128 : i * 128 + 128] for i in range(2)])
    for p in range(PARENTS_HERE):
        put_row(own_rows, p, [pv1[i, p, 0:1, :] for i in range(2)])
        put_row(own_rows, 17 + p, [pv1[i, p, 15:16, :] for i in range(2)])
    for side in range(2):
        near = [hrecv[side, 0, :, i * 128 : i * 128 + 128] for i in range(2)]
        deep = [hrecv[side, 1, :, i * 128 : i * 128 + 128] for i in range(2)]
        h = [FACTOR * v for v in near]
        ghost = halo_ghost[side]
        low = [lane_roll(v, -15) for v in gather(hv, lambda q: ghost[q][0] + side * 17)]
        high = [lane_roll(v, 15) for v in gather(hv, lambda q: ghost[q][1] + side * 17)]
        xsum = x_sum(lane, h, low, high)
        below = gather(hv, lambda q: ghost[q][2] + side * 17)[1]
        above = gather(hv, lambda q: ghost[q][3] + side * 17)[0]
        ysum = y_sum(lane, h, below, above)
        touching = gather(own_rows, lambda q: halo_own[side][q] + side * 17)
        beside = [xsum[i] + ysum[i] + FACTOR * deep[i] + touching[i] for i in range(2)]
        put_flat(halo_two, slice(side * 16, side * 16 + 16), relaxed(h, beside, near))
        spread(h2, side, flat_pair(halo_two, slice(side * 16, side * 16 + 16)))

    for p in range(PARENTS_HERE):
        h, beside = parent_beside(pv1, hv, p)
        put(pv2, p, relaxed(h, beside, both(src, p)))
    for p in range(PARENTS_HERE):
        h, beside = parent_beside(pv2, h2, p)
        put(pv4, p, rest(h, beside, both(src, p)))
    for p in range(PARENTS_HERE):
        for i in range(2):
            quad = pv4[i, p, pl.ds(0, 4, stride=4), :]
            for t in range(1, 4):
                quad = quad + pv4[i, p, pl.ds(t, 4, stride=4), :]
            zq[p * 4 : p * 4 + 4, i * 128 : i * 128 + 128] = 0.25 * quad
    zq[...] = split_dot(zq[...], coarse_table)
    place_lane = [numbers((4, 128), 1) % 32 // 4 + 8 * i for i in range(2)]
    pair = [jnp.zeros((4, 128), jnp.float32) for _ in range(2)]
    for p in range(PARENTS_HERE):
        place = places[mine + p] - mine
        for i in range(2):
            pair[i] = jnp.where(
                place_lane[i] == place, zq[p * 4 : p * 4 + 4, i * 128 : i * 128 + 128], pair[i]
            )
    slab[:, 0:128] = pair[0]
    slab[:, 128:256] = pair[1]

    shifts = (1, -1, 2, -2)

    def slab_copy(k):
        return pltpu.make_async_remote_copy(
            src_ref=slab,
            dst_ref=rbuf.at[2 - shifts[k]],
            send_sem=f_send.at[k],
            recv_sem=f_recv.at[k],
            device_id=((r + shifts[k] + ranges) % ranges, s),
            device_id_type=MESH,
        )

    slabs = tuple(
        (
            (r + d < ranges) if d > 0 else (r + d >= 0),
            (r - d >= 0) if d > 0 else (r - d < ranges),
            slab_copy(k),
        )
        for k, d in enumerate(shifts)
    )
    start_all(slabs)
    wait_arrivals(fourth)
    unpack_x(xr4)
    for b in range(LEAVES_HERE):
        h, beside = leaf_beside(le3, zb4, b)
        put(le4, b, relaxed(h, beside, [0.0, 0.0]))

    column_sums(r < middle)
    wait_arrivals(slabs)
    for slot in range(5):
        rw[slot * 4 : slot * 4 + 4, :] = slab[...] if slot == 2 else rbuf[slot]
    rw[20:24, :] = jnp.zeros((4, 256), jnp.float32)
    root = root_sweeps([jnp.where(domain, v, 0.0) for v in flat_pair(rw, slice(0, 24))])
    widen_root(root)
    for side in range(2):
        base = 64 + 16 * side
        rows = slice(side * 16, side * 16 + 16)
        grown = flat_pair(we, slice(base, base + 16))
        spread(h2, side, [v + grown[i] for i, v in enumerate(flat_pair(halo_two, rows))])
    for p in range(PARENTS_HERE):
        grown = widened(p)
        put(pv3, p, [pv2[i, p] + grown[i] for i in range(2)])

    def parent_final(slot, p):
        h, beside = parent_beside(pv3, h2, p)
        put(pv4, slot, relaxed(h, beside, both(src, p)))

    parent_final(0, first_parent)
    parent_final(1, last_parent)

    widen_leaves(pv4, leaf_slot, lv2, lv3)
    pack_faces(lv3, xs3, zb3)
    third = exchange(2, xs3, xr3, zb3)
    start_all(third)
    for k in range(3):
        parent_final(2 + k, slot_parent[k])
    column_sums(r >= middle)
    plane_sums(r < middle)
    wait_arrivals(third)
    unpack_x(xr3)
    for b in range(LEAVES_HERE):
        h, beside = leaf_beside(lv3, zb3, b)
        put(lv1, b, relaxed(h, beside, lanes_of(rhs, b)))
    plane_sums(r >= middle)
    mean_copy(0).wait_recv()
    sums = msend[2] + mrecv[0]
    mean = jnp.sum(sums) * (0.25 / (1024.0 * ranges))
    for b in range(LEAVES_HERE):
        for i in range(2):
            leaf_out[b, :, i * 128 : i * 128 + 128] = lv1[i, b] - mean * le4[i, b]
    for k in range(3):
        own = both(pv4, 2 + k)
        flat = both(pe4, slot_parent[k])
        for i in range(2):
            parent_out[k, :, i * 128 : i * 128 + 128] = jnp.where(
                slot_filled[k] == 1, own[i] - mean * flat[i], 0.0
            )

    for copies in (first, third, fourth, halos, slabs):
        wait_departures(copies)
    for k in range(1, 16):
        octants(k).wait_send()
    mean_copy(0).wait_send()
    wait_departures(lower_sums)
    wait_departures(upper_sums)
    for k in order:
        column_copy(k).wait_send()


def local(rhs, leaf_neighbors, parent_neighbors, children, owners, parent_places):
    f32 = jnp.float32
    vmem = pl.BlockSpec(memory_space=pltpu.VMEM)
    hbm = pl.BlockSpec(memory_space=pltpu.HBM)
    return pl.pallas_call(
        kernel,
        out_shape=(
            jax.ShapeDtypeStruct((8, 16, 256), f32),
            jax.ShapeDtypeStruct((3, 16, 256), f32),
        ),
        in_specs=[hbm] * 6,
        out_specs=(vmem, vmem),
        scratch_shapes=[
            pltpu.VMEM((8, 16, 256), f32),
            pltpu.SMEM((8, 6), jnp.int32),
            pltpu.SMEM((6, 512), jnp.int32),
            pltpu.SMEM((8, 512), jnp.int32),
            pltpu.SMEM((512,), jnp.int32),
            pltpu.SMEM((512,), jnp.int32),
            pltpu.VMEM((8, 512), jnp.int32),
            pltpu.SemaphoreType.DMA((7,)),
            pltpu.SMEM((96,), jnp.int32),
            pltpu.VMEM((2, 17, 16, 128), f32),
            pltpu.VMEM((2, 16, 16, 128), f32),
            pltpu.VMEM((2, 9, 16, 128), f32),
            pltpu.VMEM((2, 8, 16, 128), f32),
            pltpu.VMEM((2, 8, 256), f32),
            pltpu.VMEM((2, 8, 256), f32),
            pltpu.VMEM((33, 1, 256), f32),
            pltpu.VMEM((2, 9, 16, 128), f32),
            pltpu.VMEM((2, 9, 16, 128), f32),
            pltpu.VMEM((2, 9, 16, 128), f32),
            pltpu.VMEM((2, 8, 256), f32),
            pltpu.VMEM((2, 8, 256), f32),
            pltpu.VMEM((2, 3, 8, 256), f32),
            pltpu.VMEM((2, 3, 8, 256), f32),
            pltpu.VMEM((2, 3, 8, 256), f32),
            pltpu.VMEM((2, 3, 8, 256), f32),
            pltpu.VMEM((4, 1, 256), f32),
            pltpu.VMEM((4, 1, 256), f32),
            pltpu.VMEM((2, 2, 9, 16, 128), f32),
            pltpu.VMEM((33, 1, 256), f32),
            pltpu.VMEM((33, 1, 256), f32),
            pltpu.VMEM((33, 1, 256), f32),
            pltpu.VMEM((2, 8, 16, 128), f32),
            pltpu.VMEM((16, 4, 8, 128), f32),
            pltpu.VMEM((2, 16, 16, 128), f32),
            pltpu.VMEM((2, 17, 16, 128), f32),
            pltpu.VMEM((2, 17, 16, 128), f32),
            pltpu.VMEM((2, 17, 16, 128), f32),
            pltpu.VMEM((2, 16, 16, 128), f32),
            pltpu.VMEM((2, 17, 16, 128), f32),
            pltpu.VMEM((2, 2, 16, 256), f32),
            pltpu.VMEM((2, 2, 16, 256), f32),
            pltpu.VMEM((34, 1, 256), f32),
            pltpu.VMEM((34, 1, 256), f32),
            pltpu.VMEM((34, 1, 256), f32),
            pltpu.VMEM((32, 256), f32),
            pltpu.VMEM((16, 256), f32),
            pltpu.VMEM((64, 256), f32),
            pltpu.VMEM((4, 256), f32),
            pltpu.VMEM((5, 4, 256), f32),
            pltpu.VMEM((24, 256), f32),
            pltpu.VMEM((96, 256), f32),
            pltpu.VMEM((96, 256), f32),
            pltpu.VMEM((3, 1, 128), f32),
            pltpu.VMEM((31, 1, 128), f32),
            pltpu.VMEM((16, 1, 128), f32),
            pltpu.VMEM((64, 256), f32),
            pltpu.SemaphoreType.DMA((4, 4)),
            pltpu.SemaphoreType.DMA((4, 4)),
            pltpu.SemaphoreType.DMA((16,)),
            pltpu.SemaphoreType.DMA((16,)),
            pltpu.SemaphoreType.DMA((2,)),
            pltpu.SemaphoreType.DMA((2,)),
            pltpu.SemaphoreType.DMA((4,)),
            pltpu.SemaphoreType.DMA((4,)),
            pltpu.SemaphoreType.DMA((31,)),
            pltpu.SemaphoreType.DMA((31,)),
            pltpu.SemaphoreType.DMA((16,)),
            pltpu.SemaphoreType.DMA((16,)),
            pltpu.SemaphoreType.REGULAR((6,)),
        ],
        compiler_params=pltpu.CompilerParams(collective_id=0, has_side_effects=True, vmem_limit_bytes=10 * 1024 * 1024),
        name="vcycle",
    )(
        *(
            pltpu.with_memory_space_constraint(v, pltpu.HBM)
            for v in (
                rhs,
                leaf_neighbors,
                parent_neighbors.T,
                children.T,
                owners,
                parent_places,
            )
        )
    )


def solution(mesh):
    in_specs = (P(("blk", "sub"), None, None), P(("blk", "sub"), None), P(), P(), P(), P())
    out_specs = (P(("blk", "sub"), None, None), P(("blk", "sub"), None, None))
    return jax.shard_map(local, mesh=mesh, in_specs=in_specs, out_specs=out_specs, check_vma=False)
```

```python
import jax
import jax.numpy as jnp
from jax import lax
from jax.experimental import pallas as pl
from jax.experimental.pallas import tpu as pltpu
from jax.sharding import PartitionSpec as P

FACTOR = 0.8 / 6.0
SWEEPS = 8
MESH = pl.DeviceIdType.MESH
LEAVES_HERE = 8
PARENTS_HERE = 16


def lane_roll(half, shift):
    return pltpu.roll(half, shift % 128, 1)


def row_roll(half, shift):
    return pltpu.roll(half, shift % half.shape[0], 0)


def both(ref, index):
    return [ref[0, index], ref[1, index]]


def lanes_of(ref, index):
    return [ref[index, :, 0:128], ref[index, :, 128:256]]


def flat_pair(ref, rows):
    return [ref[rows, 0:128], ref[rows, 128:256]]


def row_pair(ref, index):
    return [ref[index, :, 0:128], ref[index, :, 128:256]]


def put_row(ref, index, pair):
    ref[index, :, 0:128] = pair[0]
    ref[index, :, 128:256] = pair[1]


def put(ref, index, pair):
    ref[0, index] = pair[0]
    ref[1, index] = pair[1]


def put_flat(ref, rows, pair):
    ref[rows, 0:128] = pair[0]
    ref[rows, 128:256] = pair[1]


def split_dot(left, table):
    high = left.astype(jnp.bfloat16)
    low = (left - high.astype(jnp.float32)).astype(jnp.bfloat16)
    return jnp.dot(high, table, preferred_element_type=jnp.float32) + jnp.dot(
        low, table, preferred_element_type=jnp.float32
    )


def y_sum(lane, h, below, above):
    up = [lane_roll(h[0], 16), lane_roll(h[1], 16)]
    down = [lane_roll(h[0], -16), lane_roll(h[1], -16)]
    first = jnp.where(lane < 16, lane_roll(below, 16), up[0]) + jnp.where(
        lane >= 112, down[1], down[0]
    )
    second = jnp.where(lane < 16, up[0], up[1]) + jnp.where(
        lane >= 112, lane_roll(above, -16), down[1]
    )
    return [first, second]


def x_sum(lane, h, low, high):
    column = lane % 16
    return [
        jnp.where(column == 0, low[i], lane_roll(h[i], 1))
        + jnp.where(column == 15, high[i], lane_roll(h[i], -1))
        for i in range(2)
    ]


def z_sum(row, h, low, high):
    return [
        jnp.where(row == 0, low[i], row_roll(h[i], 1))
        + jnp.where(row == 15, high[i], row_roll(h[i], -1))
        for i in range(2)
    ]


def kernel(
    rhs_in,
    ln_in,
    pn_in,
    ch_in,
    ow_in,
    places_in,
    leaf_out,
    parent_out,
    rhs,
    ln,
    pn,
    ch,
    ow,
    places,
    chv,
    load_sem,
    ghost_table,
    pe3,
    pe4,
    le3,
    le4,
    xs4,
    xr4,
    zb4,
    lv1,
    lv2,
    lv3,
    xs3,
    xr3,
    xsm,
    xrm,
    zsm,
    zrm,
    line_send,
    lines,
    xt,
    zb1,
    zb2,
    zb3,
    res,
    oct_rows,
    src,
    pv1,
    pv2,
    pv3,
    pv4,
    geo,
    hsend,
    hrecv,
    hv,
    h2,
    own_rows,
    halo_two,
    rows_tmp,
    zq,
    slab,
    rbuf,
    rw,
    wm,
    we,
    msend,
    mrecv,
    precv,
    lw,
    a_send,
    a_recv,
    c_send,
    c_recv,
    d_send,
    d_recv,
    f_send,
    f_recv,
    m_send,
    m_recv,
    p_send,
    p_recv,
    tok,
):
    ranges = lax.axis_size("blk")
    subs = lax.axis_size("sub")
    r = lax.axis_index("blk")
    s = lax.axis_index("sub")
    pairs = (
        (rhs_in, rhs),
        (ln_in, ln),
        (pn_in, pn),
        (ch_in, ch),
        (ch_in, chv),
        (ow_in, ow),
        (places_in, places),
    )
    loads = [
        pltpu.make_async_copy(source, target, load_sem.at[k])
        for k, (source, target) in enumerate(pairs)
    ]
    for load in loads:
        load.start()

    barrier = pltpu.get_barrier_semaphore()

    def exists(d):
        return (r + d < ranges) if d > 0 else (r + d >= 0)

    def signal_range(semaphore, distances):
        for d in distances:

            @pl.when(exists(d))
            def _():
                pl.semaphore_signal(
                    semaphore,
                    inc=1,
                    device_id=((r + d + ranges) % ranges, s),
                    device_id_type=MESH,
                )

    def signal_sub(semaphore, distances):
        for d in distances:
            pl.semaphore_signal(
                semaphore,
                inc=1,
                device_id=(r, (s + d + subs) % subs),
                device_id_type=MESH,
            )

    signal_range(barrier, (1, -1, 2, -2))
    signal_sub(barrier, (1, -1, 4, -4))
    middle = ranges // 2
    for k in range(2, 16):

        @pl.when((r < middle) & (r + 2 * k < ranges))
        def _():
            pl.semaphore_signal(
                barrier,
                inc=1,
                device_id=((r + 2 * k) % ranges, s),
                device_id_type=MESH,
            )

    corners = tuple(
        ((r + dz >= 0) & (r + dz < ranges) & (s + dx >= 0) & (s + dx < subs), dz, dx)
        for dz in (-1, 1)
        for dx in (-1, 1)
    )
    for there, dz, dx in corners:

        @pl.when(there)
        def _():
            pl.semaphore_signal(
                barrier,
                inc=1,
                device_id=((r + dz + ranges) % ranges, (s + dx + subs) % subs),
                device_id_type=MESH,
            )

    greetings = 4 + sum(there.astype(jnp.int32) for there, _, _ in corners)
    greetings = greetings + sum(exists(d).astype(jnp.int32) for d in (1, -1, 2, -2))
    greetings = greetings + sum(
        ((r - 2 * k >= 0) & (r - 2 * k < middle)).astype(jnp.int32) for k in range(2, 16)
    )

    lane = lax.broadcasted_iota(jnp.int32, (16, 128), 1)
    row = lax.broadcasted_iota(jnp.int32, (16, 128), 0)
    column = lane % 16
    column8 = column[0:8]
    zero_half = jnp.zeros((16, 128), jnp.float32)
    zeros = [zero_half, zero_half]

    def pack_x(values, store):
        for h in range(2):
            low = jnp.zeros((8, 128), jnp.float32)
            high = jnp.zeros((8, 128), jnp.float32)
            for b in range(LEAVES_HERE):
                for part in range(2):
                    v = values[h, b, part * 8 : part * 8 + 8, :]
                    k = part * 8 + b
                    low = jnp.where(column8 == k, lane_roll(v, k), low)
                    high = jnp.where(column8 == k, lane_roll(v, k - 15), high)
            store(0, h, low)
            store(1, h, high)

    def local_rows(values, zb):
        for b in range(LEAVES_HERE):
            put_row(zb, b, [values[i, b, 0:1, :] for i in range(2)])
            put_row(zb, 8 + b, [values[i, b, 15:16, :] for i in range(2)])
        zb[32] = jnp.zeros((1, 256), jnp.float32)

    def pack_faces(values, xs, zb):
        def store(side, h, value):
            xs[side, :, h * 128 : h * 128 + 128] = value

        pack_x(values, store)
        local_rows(values, zb)

    def exchange(step, xs, xr, zb):
        def remote(source, target, slot, device):
            return pltpu.make_async_remote_copy(
                src_ref=source,
                dst_ref=target,
                send_sem=a_send.at[step, slot],
                recv_sem=a_recv.at[step, slot],
                device_id=device,
                device_id_type=MESH,
            )

        return (
            (s > 0, s < subs - 1, remote(xs.at[0], xr.at[1], 0, (r, (s + subs - 1) % subs))),
            (s < subs - 1, s > 0, remote(xs.at[1], xr.at[0], 1, (r, (s + 1) % subs))),
            (
                r > 0,
                r < ranges - 1,
                remote(zb.at[0:8], zb.at[24:32], 2, ((r + ranges - 1) % ranges, s)),
            ),
            (
                r < ranges - 1,
                r > 0,
                remote(zb.at[8:16], zb.at[16:24], 3, ((r + 1) % ranges, s)),
            ),
        )

    def start_all(copies):
        for sends, _, copy in copies:

            @pl.when(sends)
            def _():
                copy.start()

    def wait_arrivals(copies):
        for _, arrives, copy in copies:

            @pl.when(arrives)
            def _():
                copy.wait_recv()

    def wait_departures(copies):
        for sends, _, copy in copies:

            @pl.when(sends)
            def _():
                copy.wait_send()

    def unpack_faces(face_of):
        for h in range(2):
            below = face_of(0, h)
            above = face_of(1, h)
            for j in range(LEAVES_HERE):
                for part in range(2):
                    k = part * 8 + j
                    rows = slice(part * 8, part * 8 + 8)
                    xt[0, h, j, rows, :] = lane_roll(below, -k)
                    xt[1, h, j, rows, :] = lane_roll(above, 15 - k)

    def unpack_x(xr):
        unpack_faces(lambda side, h: xr[side, :, h * 128 : h * 128 + 128])

    def leaf_beside(values, zb, b):
        h = both(values, b)
        low = [xt[0, i, leaf_x[b][0]] for i in range(2)]
        high = [xt[1, i, leaf_x[b][1]] for i in range(2)]
        xsum = x_sum(lane, h, low, high)
        ysum = y_sum(
            lane,
            h,
            values[1, leaf_y[b][0]],
            values[0, leaf_y[b][1]],
        )
        zsum = z_sum(
            row,
            h,
            row_pair(zb, leaf_z[b][0]),
            row_pair(zb, leaf_z[b][1]),
        )
        return h, [xsum[i] + ysum[i] + zsum[i] for i in range(2)]

    def relaxed(h, beside, forcing):
        return [h[i] + FACTOR * (forcing[i] - (6.0 * h[i] - beside[i])) for i in range(2)]

    def rest(h, beside, forcing):
        return [forcing[i] - (6.0 * h[i] - beside[i]) for i in range(2)]

    for ref in (lv1, lv2, lv3, le3):
        put(ref, 8, zeros)
    for ref in (pv1, pv2, pv3, pe3):
        put(ref, 16, zeros)
    for side in range(2):
        xt[side, 0, 8] = zero_half
        xt[side, 1, 8] = zero_half
    for side in range(2):
        for ref in (hv, h2, own_rows):
            ref[side * 17 + 16] = jnp.zeros((1, 256), jnp.float32)

    loads[1].wait()
    here = r * subs + s
    leaf_y = [[None, None] for _ in range(LEAVES_HERE)]
    leaf_x = [[None, None] for _ in range(LEAVES_HERE)]
    leaf_z = [[None, None] for _ in range(LEAVES_HERE)]
    for b in range(LEAVES_HERE):
        for f in range(6):
            n = ln[b, f]
            local = jnp.where(n >= 0, n & 7, 8)
            if f < 2:
                leaf_x[b][f] = local
            elif f < 4:
                leaf_y[b][f - 2] = local
            else:
                remote = (n >> 3) != here
                own_base, far_base = (8, 16) if f == 4 else (0, 24)
                leaf_z[b][f - 4] = jnp.where(
                    n >= 0, (n & 7) + jnp.where(remote, far_base, own_base), 32
                )

    leaf_near = []
    leaf_far = []
    for b in range(LEAVES_HERE):
        far = [leaf_z[b][f] >= 16 for f in range(2)]
        leaf_near.append([jnp.where(far[f], 32, leaf_z[b][f]) for f in range(2)])
        leaf_far.append([jnp.where(far[f], leaf_z[b][f], 32) for f in range(2)])
    loads[0].wait()
    for b in range(LEAVES_HERE):
        put(lv1, b, [FACTOR * v for v in lanes_of(rhs, b)])
    local_rows(lv1, zb1)
    for b in range(LEAVES_HERE):
        h = both(lv1, b)
        xsum = x_sum(lane, h, [0.0, 0.0], [0.0, 0.0])
        ysum = y_sum(lane, h, lv1[1, leaf_y[b][0]], lv1[0, leaf_y[b][1]])
        zsum = z_sum(row, h, row_pair(zb1, leaf_near[b][0]), row_pair(zb1, leaf_near[b][1]))
        beside = [xsum[i] + ysum[i] + zsum[i] for i in range(2)]
        put(res, b, relaxed(h, beside, lanes_of(rhs, b)))
    row8 = row[0:8]
    for field, values in ((0, lv1), (1, res)):

        def store(side, h, value):
            xsm[side, field, :, h * 128 : h * 128 + 128] = value

        pack_x(values, store)
        for b in range(LEAVES_HERE):
            for i in range(2):
                lanes = slice(i * 128, i * 128 + 128)
                zsm[0, field, b : b + 1, lanes] = values[i, b, 0:1, :]
                zsm[1, field, b : b + 1, lanes] = values[i, b, 15:16, :]
    x_lines = jnp.full((8, 128), -100.0, jnp.float32)
    z_lines = jnp.full((8, 128), -100.0, jnp.float32)
    for b in range(LEAVES_HERE):
        down = jnp.where(leaf_z[b][0] >= 16, leaf_z[b][0] - 8, -100).astype(jnp.float32)
        up = jnp.where(leaf_far[b][1] < 32, leaf_z[b][1] - 24, -100).astype(jnp.float32)
        down = jnp.where(leaf_z[b][0] < 32, down, -100.0)
        x_lines = jnp.where((row8 == 0) & (column8 == b), down, x_lines)
        x_lines = jnp.where((row8 == 7) & (column8 == 8 + b), up, x_lines)
        left = jnp.where(leaf_x[b][0] < 8, leaf_x[b][0], -100).astype(jnp.float32)
        right = jnp.where(leaf_x[b][1] < 8, leaf_x[b][1], -100).astype(jnp.float32)
        z_lines = jnp.where((row8 == b) & (column8 == 0), left, z_lines)
        z_lines = jnp.where((row8 == b) & (column8 == 15), right, z_lines)
    for side in range(2):
        for i in range(2):
            lanes = slice(i * 128, i * 128 + 128)
            xsm[side, 2, :, lanes] = x_lines
            zsm[side, 2, :, lanes] = z_lines
            for zi in range(2):
                at = 0 if zi == 0 else 7
                line_send[2 * zi + side, :, lanes] = xsm[side, 0, at : at + 1, lanes]

    def first_copy(step, slot, source, target, device):
        return pltpu.make_async_remote_copy(
            src_ref=source,
            dst_ref=target,
            send_sem=a_send.at[step, slot],
            recv_sem=a_recv.at[step, slot],
            device_id=device,
            device_id_type=MESH,
        )

    pl.semaphore_wait(barrier, greetings)
    first = (
        (
            s > 0,
            s < subs - 1,
            first_copy(0, 0, xsm.at[0], xrm.at[1], (r, (s + subs - 1) % subs)),
        ),
        (s < subs - 1, s > 0, first_copy(0, 1, xsm.at[1], xrm.at[0], (r, (s + 1) % subs))),
        (
            r > 0,
            r < ranges - 1,
            first_copy(0, 2, zsm.at[0], zrm.at[1], ((r + ranges - 1) % ranges, s)),
        ),
        (r < ranges - 1, r > 0, first_copy(0, 3, zsm.at[1], zrm.at[0], ((r + 1) % ranges, s))),
    )
    first = first + tuple(
        (
            there,
            corners[3 - k][0],
            first_copy(
                1,
                k,
                line_send.at[k],
                lines.at[3 - k],
                ((r + dz + ranges) % ranges, (s + dx + subs) % subs),
            ),
        )
        for k, (there, dz, dx) in enumerate(corners)
    )
    start_all(first)

    def tell(stage):
        distance = 2 << stage

        @pl.when((r >= middle) & (r + distance < ranges))
        def _():
            pl.semaphore_signal(
                tok.at[stage],
                inc=1,
                device_id=((r + distance) % ranges, s),
                device_id_type=MESH,
            )

        @pl.when(r - distance >= middle)
        def _():
            pl.semaphore_signal(
                tok.at[stage],
                inc=1,
                device_id=((r - distance + ranges) % ranges, s),
                device_id_type=MESH,
            )

    def hear(stage):
        distance = 2 << stage
        peers = ((r >= middle) & (r + distance < ranges)).astype(jnp.int32)
        peers = peers + (r - distance >= middle).astype(jnp.int32)

        @pl.when(peers > 0)
        def _():
            pl.semaphore_wait(tok.at[stage], peers)

    tell(0)
    signal_sub(tok.at[4], (1, -1, 4, -4))

    def numbers(shape, dim):
        return lax.broadcasted_iota(jnp.int32, shape, dim)

    def table(hit):
        return jnp.where(hit, 1.0, 0.0).astype(jnp.bfloat16)

    source_id = numbers((512, 128), 0)
    target_id = numbers((512, 128), 1)
    restrict = table(
        ((source_id % 256) // 32 == target_id // 16)
        & ((source_id % 16) // 2 + (source_id // 256) * 8 == target_id % 16)
    )
    octant_in = numbers((128, 256), 0)
    leaf_cell = numbers((128, 256), 1)
    leaf_table = table(
        (octant_in // 16 == leaf_cell // 32)
        & (octant_in % 16 == (leaf_cell % 16) // 2 + (s % 2) * 8)
    )

    for load in loads[2:]:
        load.wait()
    def inside(n, base):
        return jnp.where(n >= 0, jnp.clip(n - base, 0, 15), 16)

    mine = r * 16
    lower = jnp.maximum(r - 1, 0) * 16
    upper = jnp.minimum(r + 1, ranges - 1) * 16
    own_ghost = [
        [
            inside(pn[f, mine + p], mine if f < 4 else (lower if f == 4 else upper))
            for f in range(6)
        ]
        for p in range(PARENTS_HERE)
    ]
    for p in range(PARENTS_HERE):
        for f in range(6):
            ghost_table[p * 6 + f] = own_ghost[p][f]
    halo_base = (lower, upper)
    halo_ghost = [
        [[inside(pn[f, base + q], base) for f in range(4)] for q in range(PARENTS_HERE)]
        for base in halo_base
    ]
    halo_own = [
        [
            inside(pn[5 - side, halo_base[side] + q], mine)
            for q in range(PARENTS_HERE)
        ]
        for side in range(2)
    ]


    hear(0)
    tell(1)

    def missing(base, p, f):
        return jnp.where(pn[f, base + p] < 0, FACTOR, 0.0).astype(jnp.float32)

    def edge_weight(base, p, shape, with_z):
        lanes = lax.broadcasted_iota(jnp.int32, shape, 1)
        rows = lax.broadcasted_iota(jnp.int32, shape, 0)
        pair = []
        for i in range(2):
            w = jnp.ones(shape, jnp.float32)
            w = w - jnp.where(lanes % 16 == 0, missing(base, p, 0), 0.0)
            w = w - jnp.where(lanes % 16 == 15, missing(base, p, 1), 0.0)
            if i == 0:
                w = w - jnp.where(lanes < 16, missing(base, p, 2), 0.0)
            else:
                w = w - jnp.where(lanes >= 112, missing(base, p, 3), 0.0)
            if with_z is None:
                w = w - jnp.where(rows == 0, missing(base, p, 4), 0.0)
                w = w - jnp.where(rows == 15, missing(base, p, 5), 0.0)
            else:
                w = w - missing(base, p, with_z)
            pair.append(w)
        return pair

    def parent_beside(values, halo, p):
        h = both(values, p)
        g = own_ghost[p] if isinstance(p, int) else [ghost_table[p * 6 + f] for f in range(6)]
        low = [lane_roll(v, -15) for v in both(values, g[0])]
        high = [lane_roll(v, 15) for v in both(values, g[1])]
        xsum = x_sum(lane, h, low, high)
        ysum = y_sum(lane, h, values[1, g[2]], values[0, g[3]])
        if halo is None:
            zsum = z_sum(row, h, [0.0, 0.0], [0.0, 0.0])
        else:
            zsum = z_sum(row, h, row_pair(halo, g[4]), row_pair(halo, g[5] + 17))
        return h, [xsum[i] + ysum[i] + zsum[i] for i in range(2)]

    for p in range(PARENTS_HERE):
        put(pv1, p, edge_weight(mine, p, (16, 128), None))
        for side in range(2):
            pair = edge_weight(halo_base[side], p, (1, 128), 5 - side)
            hv[side * 17 + p, :, 0:128] = pair[0]
            hv[side * 17 + p, :, 128:256] = pair[1]
    for p in range(PARENTS_HERE):
        h, beside = parent_beside(pv1, hv, p)
        put(geo, p, relaxed(h, beside, [0.0, 0.0]))

    leaf_parent = []
    leaf_octant = []
    flat = numbers((8, 512), 1) * 8 + numbers((8, 512), 0)
    leaf_ids = chv[...]
    for b in range(LEAVES_HERE):
        found = jnp.sum(jnp.where(leaf_ids == here * 8 + b, flat, 0)) - mine * 8
        found = jnp.clip(found, 0, 127)
        leaf_parent.append(found >> 3)
        leaf_octant.append(found & 7)

    first_parent = leaf_parent[0]
    last_parent = leaf_parent[0]
    for n in leaf_parent[1:]:
        first_parent = jnp.minimum(first_parent, n)
        last_parent = jnp.maximum(last_parent, n)
    leaf_slot = [jnp.where(n == last_parent, 1, 0) for n in leaf_parent]

    def widen_leaves(parents, where_from, base, target):
        tiles = []
        for b in range(LEAVES_HERE):
            own = both(parents, where_from[b])
            side = jnp.where(((leaf_octant[b] >> 1) & 1) == 1, own[1], own[0])
            tiles.append(jnp.where((leaf_octant[b] >> 2) == 1, side[8:16], side[0:8]))
        lw[...] = split_dot(jnp.concatenate(tiles, axis=0), leaf_table)
        for b in range(LEAVES_HERE):
            piece = flat_pair(lw, slice(b * 8, b * 8 + 8))
            for t in range(2):
                rows = pl.ds(t, 8, stride=2)
                for i in range(2):
                    target[i, b, rows, :] = (
                        piece[i] if base is None else base[i, b, rows, :] + piece[i]
                    )

    widen_leaves(geo, leaf_parent, None, lv3)

    hear(1)
    tell(2)
    pl.semaphore_wait(tok.at[4], 4)
    signal_sub(tok.at[5], (2, -2))
    wait_arrivals(first)
    unpack_faces(lambda side, h: xrm[side, 0, :, h * 128 : h * 128 + 128])
    for side in range(2):
        for n in range(LEAVES_HERE):
            zb1[16 + 8 * side + n] = zrm[side, 0, n : n + 1, :]
    for b in range(LEAVES_HERE):
        low = [xt[0, i, leaf_x[b][0]] for i in range(2)]
        high = [xt[1, i, leaf_x[b][1]] for i in range(2)]
        below = row_pair(zb1, leaf_far[b][0])
        above = row_pair(zb1, leaf_far[b][1])
        pair = []
        for i in range(2):
            more = jnp.where(column == 0, low[i], 0.0) + jnp.where(column == 15, high[i], 0.0)
            more = more + jnp.where(row == 0, below[i], 0.0) + jnp.where(row == 15, above[i], 0.0)
            pair.append(res[i, b] + FACTOR * more)
        put(lv2, b, pair)
    local_rows(lv2, zb2)

    def x_face(side, h):
        lanes = slice(h * 128, h * 128 + 128)
        hit = xrm[side, 2, :, lanes] - column8.astype(jnp.float32)
        more = jnp.zeros((8, 128), jnp.float32)
        for zi in range(2):
            line = jnp.broadcast_to(lines[2 * zi + side, :, lanes], (8, 128))
            for d in range(1, 16):
                shift = d if zi == 0 else -d
                wanted = (row8 == (0 if zi == 0 else 7)) & (hit == shift)
                more = jnp.where(wanted, lane_roll(line, -shift), more)
        return xrm[side, 1, :, lanes] + FACTOR * more

    unpack_faces(x_face)
    for zi in range(2):
        for h in range(2):
            lanes = slice(h * 128, h * 128 + 128)
            wanted = zrm[zi, 2, :, lanes]
            left = jnp.broadcast_to(lines[2 * zi, :, lanes], (8, 128))
            right = jnp.broadcast_to(lines[2 * zi + 1, :, lanes], (8, 128))
            more = jnp.zeros((8, 128), jnp.float32)
            for k in range(8):
                at = k + 8 if zi == 0 else k
                moved = jnp.where(column8 == 0, lane_roll(left, -at), lane_roll(right, 15 - at))
                more = jnp.where(wanted == k, moved, more)
            rows_tmp[zi * 8 : zi * 8 + 8, lanes] = zrm[zi, 1, :, lanes] + FACTOR * more
    for n in range(16):
        zb2[16 + n] = rows_tmp[n : n + 1, :]
    for b in range(LEAVES_HERE):
        v = both(lv1, b)
        h = both(lv2, b)
        side_gain = [jnp.where(leaf_x[b][f] < 8, FACTOR, 0.0).astype(jnp.float32) for f in range(2)]
        far_gain = [
            jnp.where(leaf_far[b][f] < 32, FACTOR, 0.0).astype(jnp.float32) for f in range(2)
        ]
        low = [xt[0, i, leaf_x[b][0]] + side_gain[0] * v[i] for i in range(2)]
        high = [xt[1, i, leaf_x[b][1]] + side_gain[1] * v[i] for i in range(2)]
        below = row_pair(zb2, leaf_z[b][0])
        above = row_pair(zb2, leaf_z[b][1])
        below = [below[i] + far_gain[0] * v[i][0:1] for i in range(2)]
        above = [above[i] + far_gain[1] * v[i][15:16] for i in range(2)]
        xsum = x_sum(lane, h, low, high)
        ysum = y_sum(lane, h, lv2[1, leaf_y[b][0]], lv2[0, leaf_y[b][1]])
        zsum = z_sum(row, h, below, above)
        put(res, b, rest(h, [xsum[i] + ysum[i] + zsum[i] for i in range(2)], lanes_of(rhs, b)))
    pieces = []
    for b in range(LEAVES_HERE):
        pieces.append(
            jnp.concatenate(
                [
                    res[i, b, pl.ds(0, 8, stride=2), :] + res[i, b, pl.ds(1, 8, stride=2), :]
                    for i in range(2)
                ],
                axis=1,
            )
        )
    stacked = jnp.concatenate(
        [jnp.concatenate(pieces[0:4], axis=0), jnp.concatenate(pieces[4:8], axis=0)], axis=1
    )
    oct_rows[s] = split_dot(0.5 * stacked, restrict).reshape(4, 8, 128)

    def octants(k):
        return pltpu.make_async_remote_copy(
            src_ref=oct_rows.at[s],
            dst_ref=oct_rows.at[s],
            send_sem=c_send.at[k],
            recv_sem=c_recv.at[k],
            device_id=(r, (s + k) % subs),
            device_id_type=MESH,
        )

    order = (8, 2, 10, 6, 14, 7, 9, 5, 11, 3, 13, 4, 12, 1, 15)
    pl.semaphore_wait(tok.at[5], 2)
    for k in order:
        octants(k).start()

    pair_device = (r + 1 - 2 * (r % 2), s)

    def mean_copy(k, distance=0):
        return pltpu.make_async_remote_copy(
            src_ref=msend.at[2 if k == 0 else 0],
            dst_ref=mrecv.at[k],
            send_sem=m_send.at[k],
            recv_sem=m_recv.at[k],
            device_id=pair_device if k == 0 else ((r + distance + ranges) % ranges, s),
            device_id_type=MESH,
        )

    lower_sums = tuple(
        (r >= 2 * k, r + 2 * k < ranges, mean_copy(k, -2 * k)) for k in range(1, 16)
    )
    upper_sums = tuple(
        (r + 2 * k < ranges, r >= 2 * k, mean_copy(15 + k, 2 * k)) for k in range(1, 16)
    )
    total = jnp.zeros((16, 128), jnp.float32)
    for b in range(LEAVES_HERE):
        q = both(lv3, b)
        v = both(res, b)
        total = total + q[0] * v[0] + q[1] * v[1]
    msend[0] = 0.5 * jnp.sum(total, axis=0, keepdims=True)
    start_all(
        tuple((sends & (r - 2 * k < middle), None, c) for k, (sends, _, c) in enumerate(lower_sums, 1))
    )
    hear(2)
    start_all(
        tuple((sends & (r - 2 * k >= middle), None, c) for k, (sends, _, c) in enumerate(lower_sums, 1))
    )

    @pl.when(r >= middle)
    def _():
        start_all(upper_sums)

    fine = numbers((256, 256), 0)
    grid = numbers((256, 256), 1)
    coarse_table = table(
        (fine // 64 == (grid // 32) % 4) & ((fine % 16) // 4 == grid % 4)
    )
    grid_in = numbers((256, 256), 0)
    fine_out = numbers((256, 256), 1)
    widen_table = table(
        (fine_out // 64 == (grid_in // 32) % 4) & ((fine_out % 16) // 4 == grid_in % 4)
    )
    slot_parent = [jnp.int32(0)] * 3
    slot_filled = [jnp.int32(0)] * 3
    seen = jnp.int32(0)
    for p in range(PARENTS_HERE):
        owned = ow[mine + p] == s
        for k in range(3):
            take = jnp.logical_and(owned, seen == k)
            slot_parent[k] = jnp.where(take, p, slot_parent[k])
            slot_filled[k] = jnp.where(take, 1, slot_filled[k])
        seen = seen + jnp.where(owned, 1, 0)

    kids = [
        [jnp.clip(ch[o, mine + p] - mine * 8, 0, 127) for o in range(8)]
        for p in range(PARENTS_HERE)
    ]
    kid_dev = [[n >> 3 for n in line] for line in kids]
    kid_tile = [[n & 3 for n in line] for line in kids]
    kid_half = [[(n >> 2) & 1 for n in line] for line in kids]

    root_row = numbers((24, 128), 0)
    root_lane = numbers((24, 128), 1)
    depth = root_row + 4 * r - 8
    domain = (depth >= 0) & (depth < 4 * ranges) & (root_row < 20)

    def root_sweeps(source):
        w = [FACTOR * v for v in source]
        for _ in range(SWEEPS - 1):
            up = [lane_roll(v, 32) for v in w]
            down = [lane_roll(v, -32) for v in w]
            ysum = [
                jnp.where(root_lane < 32, 0.0, up[0])
                + jnp.where(root_lane >= 96, down[1], down[0]),
                jnp.where(root_lane < 32, up[0], up[1])
                + jnp.where(root_lane >= 96, 0.0, down[1]),
            ]
            fresh = []
            for i in range(2):
                xsum = jnp.where(root_lane % 32 == 0, 0.0, lane_roll(w[i], 1)) + jnp.where(
                    root_lane % 32 == 31, 0.0, lane_roll(w[i], -1)
                )
                zsum = row_roll(w[i], 1) + row_roll(w[i], -1)
                fresh.append(
                    jnp.where(
                        domain,
                        w[i]
                        + FACTOR * (source[i] - (6.0 * w[i] - (xsum + ysum[i] + zsum))),
                        0.0,
                    )
                )
            w = fresh
        return w

    ones = jnp.where(domain, 1.0, 0.0).astype(jnp.float32)
    flat_root = root_sweeps([ones, ones])

    wide_lane = [numbers((4, 128), 1) % 32 // 4 + 8 * i for i in range(2)]
    place_own = [places[mine + p] - mine for p in range(PARENTS_HERE)]
    place_halo = [[places[base + p] - base for p in range(PARENTS_HERE)] for base in halo_base]

    def widen_root(pair):
        put_flat(rw, slice(0, 24), pair)
        for p in range(PARENTS_HERE):
            for i in range(2):
                lanes = slice(i * 128, i * 128 + 128)
                wm[p * 4 : p * 4 + 4, lanes] = jnp.where(
                    wide_lane[i] == place_own[p], rw[8:12, lanes], 0.0
                )
                wm[64 + p : 65 + p, lanes] = jnp.where(
                    wide_lane[i][0:1] == place_halo[0][p], rw[7:8, lanes], 0.0
                )
                wm[80 + p : 81 + p, lanes] = jnp.where(
                    wide_lane[i][0:1] == place_halo[1][p], rw[12:13, lanes], 0.0
                )
        we[...] = split_dot(wm[...], widen_table)

    def widened(p):
        pair = []
        for i in range(2):
            lanes = slice(i * 128, i * 128 + 128)
            lines = [we[p * 4 + k : p * 4 + k + 1, lanes] for k in range(4)]
            pair.append(
                jnp.where(
                    row < 8,
                    jnp.where(row < 4, lines[0], lines[1]),
                    jnp.where(row < 12, lines[2], lines[3]),
                )
            )
        return pair

    def spread(ref, side, pair):
        put_flat(rows_tmp, slice(0, 16), pair)
        for q in range(PARENTS_HERE):
            ref[side * 17 + q] = rows_tmp[q : q + 1, :]

    def column_copy(k):
        return pltpu.make_async_remote_copy(
            src_ref=msend.at[1],
            dst_ref=precv.at[k],
            send_sem=p_send.at[k],
            recv_sem=p_recv.at[k],
            device_id=(r, (s + k) % subs),
            device_id_type=MESH,
        )


    def column_sums(now):
        @pl.when(now)
        def _():
            wait_arrivals(lower_sums)

            @pl.when(r < middle)
            def _():
                start_all(upper_sums)

            wait_arrivals(upper_sums)
            sums = msend[0]
            for k in range(1, 16):
                sums = sums + jnp.where(r + 2 * k < ranges, mrecv[k], 0.0)
                sums = sums + jnp.where(r >= 2 * k, mrecv[15 + k], 0.0)
            msend[1] = sums
            for k in order:
                column_copy(k).start()

    def plane_sums(now):
        @pl.when(now)
        def _():
            for k in order:
                column_copy(k).wait_recv()
            sums = msend[1]
            for k in range(1, 16):
                sums = sums + precv[k]
            msend[2] = sums
            mean_copy(0).start()


    widen_root(flat_root)
    for side in range(2):
        spread(h2, side, flat_pair(we, slice(64 + 16 * side, 80 + 16 * side)))
    for p in range(PARENTS_HERE):
        put(pe3, p, widened(p))
    for p in range(PARENTS_HERE):
        h, beside = parent_beside(pe3, h2, p)
        put(pe4, p, relaxed(h, beside, [0.0, 0.0]))
    widen_leaves(pe4, leaf_parent, None, le3)
    pack_faces(le3, xs4, zb4)
    fourth = exchange(3, xs4, xr4, zb4)
    start_all(fourth)

    for k in order:
        octants(k).wait_recv()

    for p in range(PARENTS_HERE):
        for oz in range(2):
            for oy in range(2):
                parts = []
                for ox in range(2):
                    o = 4 * oz + 2 * oy + ox
                    tile = oct_rows[kid_dev[p][o], kid_tile[p][o]]
                    wanted = kid_half[p][o] == ox
                    parts.append(jnp.where(wanted, tile, lane_roll(tile, 8 if ox else -8)))
                src[oy, p, oz * 8 : oz * 8 + 8, :] = jnp.where(
                    column8 < 8, parts[0], parts[1]
                )

    for layer in range(2):
        for i in range(2):
            hsend[0, layer, :, i * 128 : i * 128 + 128] = src[i, :, layer, :]
            hsend[1, layer, :, i * 128 : i * 128 + 128] = src[i, :, 15 - layer, :]

    def halo_copy(direction):
        step = -1 if direction == 0 else 1
        return pltpu.make_async_remote_copy(
            src_ref=hsend.at[direction],
            dst_ref=hrecv.at[1 - direction],
            send_sem=d_send.at[direction],
            recv_sem=d_recv.at[direction],
            device_id=((r + step + ranges) % ranges, s),
            device_id_type=MESH,
        )

    halos = (
        (r > 0, r < ranges - 1, halo_copy(0)),
        (r < ranges - 1, r > 0, halo_copy(1)),
    )
    start_all(halos)

    for p in range(PARENTS_HERE):
        put(pv1, p, [FACTOR * v for v in both(src, p)])

    for p in range(PARENTS_HERE):
        put_row(own_rows, p, [pv1[i, p, 0:1, :] for i in range(2)])
        put_row(own_rows, 17 + p, [pv1[i, p, 15:16, :] for i in range(2)])
    for p in range(PARENTS_HERE):
        h, beside = parent_beside(pv1, None, p)
        put(pv2, p, relaxed(h, beside, both(src, p)))

    wait_arrivals(halos)

    def gather(ref, index_of):
        for q in range(PARENTS_HERE):
            rows_tmp[q : q + 1, :] = ref[index_of(q)]
        return flat_pair(rows_tmp, slice(0, 16))

    for side in range(2):
        spread(hv, side, [FACTOR * hrecv[side, 0, :, i * 128 : i * 128 + 128] for i in range(2)])
    for side in range(2):
        near = [hrecv[side, 0, :, i * 128 : i * 128 + 128] for i in range(2)]
        deep = [hrecv[side, 1, :, i * 128 : i * 128 + 128] for i in range(2)]
        h = [FACTOR * v for v in near]
        ghost = halo_ghost[side]
        low = [lane_roll(v, -15) for v in gather(hv, lambda q: ghost[q][0] + side * 17)]
        high = [lane_roll(v, 15) for v in gather(hv, lambda q: ghost[q][1] + side * 17)]
        xsum = x_sum(lane, h, low, high)
        below = gather(hv, lambda q: ghost[q][2] + side * 17)[1]
        above = gather(hv, lambda q: ghost[q][3] + side * 17)[0]
        ysum = y_sum(lane, h, below, above)
        touching = gather(own_rows, lambda q: halo_own[side][q] + side * 17)
        beside = [xsum[i] + ysum[i] + FACTOR * deep[i] + touching[i] for i in range(2)]
        put_flat(halo_two, slice(side * 16, side * 16 + 16), relaxed(h, beside, near))
        spread(h2, side, flat_pair(halo_two, slice(side * 16, side * 16 + 16)))

    for p in range(PARENTS_HERE):
        g = own_ghost[p]
        below = row_pair(hv, g[4])
        above = row_pair(hv, g[5] + 17)
        for i in range(2):
            pv2[i, p, 0:1, :] = pv2[i, p, 0:1, :] + FACTOR * below[i]
            pv2[i, p, 15:16, :] = pv2[i, p, 15:16, :] + FACTOR * above[i]
    for p in range(PARENTS_HERE):
        h, beside = parent_beside(pv2, h2, p)
        put(pv4, p, rest(h, beside, both(src, p)))
    for p in range(PARENTS_HERE):
        for i in range(2):
            quad = pv4[i, p, pl.ds(0, 4, stride=4), :]
            for t in range(1, 4):
                quad = quad + pv4[i, p, pl.ds(t, 4, stride=4), :]
            zq[p * 4 : p * 4 + 4, i * 128 : i * 128 + 128] = 0.25 * quad
    zq[...] = split_dot(zq[...], coarse_table)
    place_lane = [numbers((4, 128), 1) % 32 // 4 + 8 * i for i in range(2)]
    pair = [jnp.zeros((4, 128), jnp.float32) for _ in range(2)]
    for p in range(PARENTS_HERE):
        place = places[mine + p] - mine
        for i in range(2):
            pair[i] = jnp.where(
                place_lane[i] == place, zq[p * 4 : p * 4 + 4, i * 128 : i * 128 + 128], pair[i]
            )
    slab[:, 0:128] = pair[0]
    slab[:, 128:256] = pair[1]

    shifts = (1, -1, 2, -2)

    def slab_copy(k):
        return pltpu.make_async_remote_copy(
            src_ref=slab,
            dst_ref=rbuf.at[2 - shifts[k]],
            send_sem=f_send.at[k],
            recv_sem=f_recv.at[k],
            device_id=((r + shifts[k] + ranges) % ranges, s),
            device_id_type=MESH,
        )

    slabs = tuple(
        (
            (r + d < ranges) if d > 0 else (r + d >= 0),
            (r - d >= 0) if d > 0 else (r - d < ranges),
            slab_copy(k),
        )
        for k, d in enumerate(shifts)
    )
    start_all(slabs)
    wait_arrivals(fourth)
    unpack_x(xr4)
    for b in range(LEAVES_HERE):
        h, beside = leaf_beside(le3, zb4, b)
        put(le4, b, relaxed(h, beside, [0.0, 0.0]))

    column_sums(r < middle)
    wait_arrivals(slabs)
    for slot in range(5):
        rw[slot * 4 : slot * 4 + 4, :] = slab[...] if slot == 2 else rbuf[slot]
    rw[20:24, :] = jnp.zeros((4, 256), jnp.float32)
    root = root_sweeps([jnp.where(domain, v, 0.0) for v in flat_pair(rw, slice(0, 24))])
    widen_root(root)
    for side in range(2):
        base = 64 + 16 * side
        rows = slice(side * 16, side * 16 + 16)
        grown = flat_pair(we, slice(base, base + 16))
        spread(h2, side, [v + grown[i] for i, v in enumerate(flat_pair(halo_two, rows))])
    for p in range(PARENTS_HERE):
        grown = widened(p)
        put(pv3, p, [pv2[i, p] + grown[i] for i in range(2)])

    def parent_final(slot, p):
        h, beside = parent_beside(pv3, h2, p)
        put(pv4, slot, relaxed(h, beside, both(src, p)))

    parent_final(0, first_parent)
    parent_final(1, last_parent)

    widen_leaves(pv4, leaf_slot, lv2, lv3)
    pack_faces(lv3, xs3, zb3)
    third = exchange(2, xs3, xr3, zb3)
    start_all(third)
    for k in range(3):
        parent_final(2 + k, slot_parent[k])
    column_sums(r >= middle)
    plane_sums(r < middle)
    wait_arrivals(third)
    unpack_x(xr3)
    for b in range(LEAVES_HERE):
        h, beside = leaf_beside(lv3, zb3, b)
        put(lv1, b, relaxed(h, beside, lanes_of(rhs, b)))
    plane_sums(r >= middle)
    mean_copy(0).wait_recv()
    sums = msend[2] + mrecv[0]
    mean = jnp.sum(sums) * (0.25 / (1024.0 * ranges))
    for b in range(LEAVES_HERE):
        for i in range(2):
            leaf_out[b, :, i * 128 : i * 128 + 128] = lv1[i, b] - mean * le4[i, b]
    for k in range(3):
        own = both(pv4, 2 + k)
        flat = both(pe4, slot_parent[k])
        for i in range(2):
            parent_out[k, :, i * 128 : i * 128 + 128] = jnp.where(
                slot_filled[k] == 1, own[i] - mean * flat[i], 0.0
            )

    for copies in (first, third, fourth, halos, slabs):
        wait_departures(copies)
    for k in range(1, 16):
        octants(k).wait_send()
    mean_copy(0).wait_send()
    wait_departures(lower_sums)
    wait_departures(upper_sums)
    for k in order:
        column_copy(k).wait_send()


def local(rhs, leaf_neighbors, parent_neighbors, children, owners, parent_places):
    f32 = jnp.float32
    vmem = pl.BlockSpec(memory_space=pltpu.VMEM)
    hbm = pl.BlockSpec(memory_space=pltpu.HBM)
    return pl.pallas_call(
        kernel,
        out_shape=(
            jax.ShapeDtypeStruct((8, 16, 256), f32),
            jax.ShapeDtypeStruct((3, 16, 256), f32),
        ),
        in_specs=[hbm] * 6,
        out_specs=(vmem, vmem),
        scratch_shapes=[
            pltpu.VMEM((8, 16, 256), f32),
            pltpu.SMEM((8, 6), jnp.int32),
            pltpu.SMEM((6, 512), jnp.int32),
            pltpu.SMEM((8, 512), jnp.int32),
            pltpu.SMEM((512,), jnp.int32),
            pltpu.SMEM((512,), jnp.int32),
            pltpu.VMEM((8, 512), jnp.int32),
            pltpu.SemaphoreType.DMA((7,)),
            pltpu.SMEM((96,), jnp.int32),
            pltpu.VMEM((2, 17, 16, 128), f32),
            pltpu.VMEM((2, 16, 16, 128), f32),
            pltpu.VMEM((2, 9, 16, 128), f32),
            pltpu.VMEM((2, 8, 16, 128), f32),
            pltpu.VMEM((2, 8, 256), f32),
            pltpu.VMEM((2, 8, 256), f32),
            pltpu.VMEM((33, 1, 256), f32),
            pltpu.VMEM((2, 9, 16, 128), f32),
            pltpu.VMEM((2, 9, 16, 128), f32),
            pltpu.VMEM((2, 9, 16, 128), f32),
            pltpu.VMEM((2, 8, 256), f32),
            pltpu.VMEM((2, 8, 256), f32),
            pltpu.VMEM((2, 3, 8, 256), f32),
            pltpu.VMEM((2, 3, 8, 256), f32),
            pltpu.VMEM((2, 3, 8, 256), f32),
            pltpu.VMEM((2, 3, 8, 256), f32),
            pltpu.VMEM((4, 1, 256), f32),
            pltpu.VMEM((4, 1, 256), f32),
            pltpu.VMEM((2, 2, 9, 16, 128), f32),
            pltpu.VMEM((33, 1, 256), f32),
            pltpu.VMEM((33, 1, 256), f32),
            pltpu.VMEM((33, 1, 256), f32),
            pltpu.VMEM((2, 8, 16, 128), f32),
            pltpu.VMEM((16, 4, 8, 128), f32),
            pltpu.VMEM((2, 16, 16, 128), f32),
            pltpu.VMEM((2, 17, 16, 128), f32),
            pltpu.VMEM((2, 17, 16, 128), f32),
            pltpu.VMEM((2, 17, 16, 128), f32),
            pltpu.VMEM((2, 16, 16, 128), f32),
            pltpu.VMEM((2, 17, 16, 128), f32),
            pltpu.VMEM((2, 2, 16, 256), f32),
            pltpu.VMEM((2, 2, 16, 256), f32),
            pltpu.VMEM((34, 1, 256), f32),
            pltpu.VMEM((34, 1, 256), f32),
            pltpu.VMEM((34, 1, 256), f32),
            pltpu.VMEM((32, 256), f32),
            pltpu.VMEM((16, 256), f32),
            pltpu.VMEM((64, 256), f32),
            pltpu.VMEM((4, 256), f32),
            pltpu.VMEM((5, 4, 256), f32),
            pltpu.VMEM((24, 256), f32),
            pltpu.VMEM((96, 256), f32),
            pltpu.VMEM((96, 256), f32),
            pltpu.VMEM((3, 1, 128), f32),
            pltpu.VMEM((31, 1, 128), f32),
            pltpu.VMEM((16, 1, 128), f32),
            pltpu.VMEM((64, 256), f32),
            pltpu.SemaphoreType.DMA((4, 4)),
            pltpu.SemaphoreType.DMA((4, 4)),
            pltpu.SemaphoreType.DMA((16,)),
            pltpu.SemaphoreType.DMA((16,)),
            pltpu.SemaphoreType.DMA((2,)),
            pltpu.SemaphoreType.DMA((2,)),
            pltpu.SemaphoreType.DMA((4,)),
            pltpu.SemaphoreType.DMA((4,)),
            pltpu.SemaphoreType.DMA((31,)),
            pltpu.SemaphoreType.DMA((31,)),
            pltpu.SemaphoreType.DMA((16,)),
            pltpu.SemaphoreType.DMA((16,)),
            pltpu.SemaphoreType.REGULAR((6,)),
        ],
        compiler_params=pltpu.CompilerParams(collective_id=0, has_side_effects=True, vmem_limit_bytes=10 * 1024 * 1024),
        name="vcycle",
    )(
        *(
            pltpu.with_memory_space_constraint(v, pltpu.HBM)
            for v in (
                rhs,
                leaf_neighbors,
                parent_neighbors.T,
                children.T,
                owners,
                parent_places,
            )
        )
    )


def solution(mesh):
    in_specs = (P(("blk", "sub"), None, None), P(("blk", "sub"), None), P(), P(), P(), P())
    out_specs = (P(("blk", "sub"), None, None), P(("blk", "sub"), None, None))
    return jax.shard_map(local, mesh=mesh, in_specs=in_specs, out_specs=out_specs, check_vma=False)
```
